32 devices in a mesh: fsdp: 16 (over z, y, x), win: 2 (over core).
Axes of the slice: x: 2, y: 2, z: 4, core: 2. Of those that a mesh axis runs over, the one named last changes fastest.
Arguments:
- images: bfloat16 [512, 14, 14, 512], P('fsdp', 'win'), may hold values from -6 to 6
- norm1_gain: bfloat16 [512], P('fsdp'), may hold values from 0.099609375 to 1.8984375
- norm1_bias: bfloat16 [512], P('fsdp'), may hold values from -3 to 3
- qkv_weight: bfloat16 [512, 1536], P('fsdp'), may hold values from -0.25 to 0.25
- q_bias: bfloat16 [512], P('fsdp'), may hold values from -3 to 3
- v_bias: bfloat16 [512], P('fsdp'), may hold values from -3 to 3
- proj_weight: bfloat16 [512, 512], P('fsdp'), may hold values from -0.75 to 0.75
- proj_bias: bfloat16 [512], P('fsdp'), may hold values from -3 to 3
- norm2_gain: bfloat16 [512], P('fsdp'), may hold values from 0.099609375 to 1.8984375
- norm2_bias: bfloat16 [512], P('fsdp'), may hold values from -3 to 3
- fc1_weight: bfloat16 [512, 2048], P('fsdp'), may hold values from -0.25 to 0.25
- fc1_bias: bfloat16 [2048], P('fsdp'), may hold values from -3 to 3
- fc2_weight: bfloat16 [2048, 512], P('fsdp'), may hold values from -0.125 to 0.125
- fc2_bias: bfloat16 [512], P('fsdp'), may hold values from -3 to 3
- bias_table: float32 [169, 16], replicated, may hold values from -4 to 4
- regions: int32 [2, 2, 49], P('win'), may hold values from 0 to 3
- rel_index: int32 [49, 49], replicated, may hold values from 0 to 168
- cotangent: bfloat16 [512, 14, 14, 512], P('fsdp', 'win'), may hold values from -6 to 6
Outputs:
- activations: bfloat16 [512, 14, 14, 512], P('fsdp', 'win')
- input_grad: float32 [512, 14, 14, 512], P('fsdp', 'win')
- norm1_gain_grad: float32 [512], P('fsdp')
- norm1_bias_grad: float32 [512], P('fsdp')
- qkv_weight_grad: float32 [512, 1536], P('fsdp')
- q_bias_grad: float32 [512], P('fsdp')
- v_bias_grad: float32 [512], P('fsdp')
- proj_weight_grad: float32 [512, 512], P('fsdp')
- proj_bias_grad: float32 [512], P('fsdp')
- norm2_gain_grad: float32 [512], P('fsdp')
- norm2_bias_grad: float32 [512], P('fsdp')
- fc1_weight_grad: float32 [512, 2048], P('fsdp')
- fc1_bias_grad: float32 [2048], P('fsdp')
- fc2_weight_grad: float32 [2048, 512], P('fsdp')
- fc2_bias_grad: float32 [512], P('fsdp')
- bias_table_grad: float32 [169, 16], replicated
The draws below stay inside these ranges and needn't reach their ends.
All inputs are finite; a program needn't handle non-finite values.
Results may differ from the reference program's by a relative error of at most 0.014.
Values may be sent and summed in bfloat16 or wider, within the bound.
A program may use at most 320 MiB of HBM per device.

```python
import math
import jax
import jax.numpy as jnp
from jax import lax

D = 512
HEADS = 16
HD = 32
FF = 2048
WIN = 7
SHIFT = 3
HH = 14
WW = 14
HWIN = 2
WWIN = 2
WT = 49
RELS = 169
IMGS = 512


def touch_ends(values, key, smallest, top_value):
    extent = values.shape
    index_at = [jax.random.randint(jax.random.fold_in(key, axis), (), 0, extent[axis]) for axis in range(len(extent))]
    values = values.at[tuple(index_at)].set(smallest)
    longest = extent.index(max(extent))
    index_at[longest] = (index_at[longest] + 1) % extent[longest]
    return values.at[tuple(index_at)].set(top_value)


def with_spikes(entries, rng, source, target, blocks, factor):
    def block_of(position):
        return (jnp.arange(entries.shape[position]) // (entries.shape[position] // blocks)).reshape((-1,) + (1,) * (entries.ndim - 1 - position))

    first = jax.random.permutation(rng, blocks)[block_of(target)]
    other_side = (block_of(target) + blocks // 2) % blocks
    return jnp.where((block_of(source) == first) | (block_of(source) == other_side), factor * entries, entries)


def levels(key, extent, pieces, smallest, top_value):
    level, own = 1.0, jax.random.fold_in(key, 6)
    for position, shards_of in pieces:
        steps = jnp.exp(jax.random.uniform(jax.random.fold_in(own, position), (shards_of,), jnp.float32, smallest / len(pieces), top_value / len(pieces)))
        level = level * jnp.repeat(steps, extent[position] // shards_of).reshape([-1 if axis == position else 1 for axis in range(len(extent))])
    return level


def gaussian(rng, dims, spread, reach, cuts=(), dtype=jnp.bfloat16):
    array = jax.random.normal(rng, dims, jnp.float32) * spread
    if len(cuts) > 0:
        array = levels(rng, dims, cuts, -0.22, 0.18) * array
    return jnp.clip(array, min=-reach, max=reach).astype(dtype)


def heavy_noise(stream_key, shape, scale, limit, cuts, heavy, dtype=jnp.bfloat16):
    values = scale * jax.random.normal(stream_key, shape, jnp.float32)
    if cuts:
        values = values * levels(stream_key, shape, cuts, -0.22, 0.18)
    return jnp.clip(with_spikes(values, jax.random.fold_in(stream_key, 3), *heavy), -limit, limit).astype(dtype)


def setup_inputs(seed: int = 0) -> dict:
    streams_of = jax.random.split(jax.random.key(seed), 19)
    images = gaussian(streams_of[0], (IMGS, HH, WW, D), 1.0, 6.0, ((0, 16), (1, 2)))
    norm1_gain = jnp.clip(1.0 + 0.18 * jax.random.normal(streams_of[1], (D,), jnp.float32), 0.099609375, 1.8984375).astype(jnp.bfloat16)
    norm1_bias = gaussian(streams_of[2], (D,), 0.5, 3.0, ((0, 16),))
    qkv_weight = gaussian(streams_of[3], (D, 3 * D), D ** -0.5, 0.25, ((0, 16),))
    q_bias = gaussian(streams_of[4], (D,), 0.5, 3.0, ((0, 16),))
    v_bias = gaussian(streams_of[5], (D,), 0.5, 3.0, ((0, 16),))
    proj_weight = gaussian(streams_of[6], (D, D), (D // 8) ** -0.5, 0.75, ((0, 16),))
    proj_bias = gaussian(streams_of[7], (D,), 0.5, 3.0, ((0, 16),))
    norm2_gain = jnp.clip(1.0 + 0.18 * jax.random.normal(streams_of[8], (D,), jnp.float32), 0.099609375, 1.8984375).astype(jnp.bfloat16)
    norm2_bias = gaussian(streams_of[9], (D,), 0.5, 3.0, ((0, 16),))
    fc1_weight = gaussian(streams_of[10], (D, FF), D ** -0.5, 0.25, ((0, 16),))
    fc1_bias = gaussian(streams_of[11], (FF,), 0.5, 3.0, ((0, 16),))
    fc2_weight = gaussian(streams_of[12], (FF, D), FF ** -0.5, 0.125, ((0, 16),))
    fc2_bias = gaussian(streams_of[13], (D,), 0.5, 3.0, ((0, 16),))
    bias_table = gaussian(streams_of[14], (RELS, HEADS), 1.0, 4.0, (), jnp.float32)
    regions = touch_ends(jax.random.randint(streams_of[15], (HWIN, WWIN, WT), 0, 4), jax.random.fold_in(streams_of[15], 1), 0, 3).astype(jnp.int32)
    rel_index = touch_ends(jax.random.randint(streams_of[16], (WT, WT), 0, RELS), jax.random.fold_in(streams_of[16], 1), 0, RELS - 1).astype(jnp.int32)
    cotangent = heavy_noise(streams_of[17], (IMGS, HH, WW, D), 1.0, 6.0, ((0, 16), (1, 2)), (0, 3, 16, 2.0))
    return dict(images=images, norm1_gain=norm1_gain, norm1_bias=norm1_bias, qkv_weight=qkv_weight, q_bias=q_bias, v_bias=v_bias, proj_weight=proj_weight, proj_bias=proj_bias, norm2_gain=norm2_gain, norm2_bias=norm2_bias, fc1_weight=fc1_weight, fc1_bias=fc1_bias, fc2_weight=fc2_weight, fc2_bias=fc2_bias, bias_table=bias_table, regions=regions, rel_index=rel_index, cotangent=cotangent)


EPS = 1e-05
HIGHEST = lax.Precision.HIGHEST

@jax.custom_vjp
def low(v):
    return lax.optimization_barrier(v.astype(jnp.bfloat16)).astype(jnp.float32)

@jax.custom_vjp
def low_back(v):
    return v

def low_keep(v):
    return (low(v), None)

def low_pass(kept, grad):
    return (grad,)

def back_keep(v):
    return (v, None)

def back_low(kept, grad):
    return (low(grad),)
low.defvjp(low_keep, low_pass)
low_back.defvjp(back_keep, back_low)

def layer_norm(values, norm_gain, norm_bias):
    average = lax.optimization_barrier(jnp.mean(values, axis=-1, keepdims=True))
    centered = values - average
    variance = lax.optimization_barrier(jnp.mean(centered * centered, axis=-1, keepdims=True))
    return centered * lax.rsqrt(variance + EPS) * norm_gain + norm_bias

def gelu_exact(values):
    return 0.5 * values * (1.0 + jax.scipy.special.erf(values * 0.7071067811865476))

def to_windows(field_map):
    image_count = field_map.shape[0]
    feat_width = field_map.shape[-1]
    win_rows = field_map.shape[1] // WIN
    win_cols = field_map.shape[2] // WIN
    shaped = field_map.reshape(image_count, win_rows, WIN, win_cols, WIN, feat_width)
    return shaped.transpose(0, 1, 3, 2, 4, 5).reshape(image_count, win_rows * win_cols, WIN * WIN, feat_width)

def from_windows(window_rows, win_rows, win_cols):
    image_count = window_rows.shape[0]
    feat_width = window_rows.shape[-1]
    shaped = window_rows.reshape(image_count, win_rows, win_cols, WIN, WIN, feat_width)
    return shaped.transpose(0, 1, 3, 2, 4, 5).reshape(image_count, win_rows * WIN, win_cols * WIN, feat_width)

def block_forward(images, params, relative, mask_add):
    norm1_gain, norm1_bias, qkv_weight, q_bias, v_bias, proj_weight, proj_bias, norm2_gain, norm2_bias, fc1_weight, fc1_bias, fc2_weight, fc2_bias = params
    normed = low_back(low(layer_norm(images, norm1_gain, norm1_bias)))
    rolled = jnp.roll(normed, (-SHIFT, -SHIFT), axis=(1, 2))
    window_rows = to_windows(rolled)
    qkv_rows = jnp.einsum('bntd,de->bnte', window_rows, qkv_weight, precision=HIGHEST)
    queries = low_back(low(qkv_rows[..., :D] + q_bias))
    key_rows = low_back(low(qkv_rows[..., D:2 * D]))
    value_rows = low_back(low(qkv_rows[..., 2 * D:] + v_bias))
    head_shape = queries.shape[:3] + (HEADS, HD)
    scores = jnp.einsum('bnthe,bnshe->bnhts', queries.reshape(head_shape), key_rows.reshape(head_shape), precision=HIGHEST) * HD ** (-0.5)
    scores = low_back(scores + relative[None, None] + mask_add[None, :, None])
    row_peak = lax.optimization_barrier(jnp.max(scores, axis=-1, keepdims=True))
    raised = jnp.exp(scores - row_peak)
    attn_probs = raised / lax.optimization_barrier(jnp.sum(raised, axis=-1, keepdims=True))
    probs_low = low(attn_probs)
    attended = jnp.einsum('bnhts,bnshe->bnthe', probs_low, value_rows.reshape(head_shape), precision=HIGHEST)
    attended = low_back(low(attended.reshape(queries.shape)))
    merged = from_windows(attended, HWIN, WWIN)
    unrolled = jnp.roll(merged, (SHIFT, SHIFT), axis=(1, 2))
    projected = low_back(jnp.einsum('bijd,de->bije', unrolled, proj_weight, precision=HIGHEST) + proj_bias)
    middle = images + projected
    normed2 = low(layer_norm(middle, norm2_gain, norm2_bias))
    hidden = low_back(jnp.einsum('bijd,df->bijf', normed2, fc1_weight, precision=HIGHEST) + fc1_bias)
    active = low(gelu_exact(hidden))
    branch = low_back(jnp.einsum('bijf,fe->bije', active, fc2_weight, precision=HIGHEST) + fc2_bias)
    return middle + branch

def reference(images, norm1_gain, norm1_bias, qkv_weight, q_bias, v_bias, proj_weight, proj_bias, norm2_gain, norm2_bias, fc1_weight, fc1_bias, fc2_weight, fc2_bias, bias_table, regions, rel_index, cotangent):
    params = tuple((item.astype(jnp.float32) for item in (norm1_gain, norm1_bias, qkv_weight, q_bias, v_bias, proj_weight, proj_bias, norm2_gain, norm2_bias, fc1_weight, fc1_bias, fc2_weight, fc2_bias)))
    flat_regions = regions.reshape(HWIN * WWIN, WT)
    mask_add = jnp.where(flat_regions[:, :, None] == flat_regions[:, None, :], 0.0, -100.0).astype(jnp.float32)
    image_total = images.shape[0]
    group_size = math.gcd(image_total, 16)
    grouped = images.astype(jnp.float32).reshape(image_total // group_size, group_size, HH, WW, D)
    stepper = jax.checkpoint(block_forward)

    def whole_net(image_blocks, weights, table):
        relative = table[rel_index].transpose(2, 0, 1)

        def advance(carry_val, block_images):
            return (carry_val, stepper(block_images, weights, relative, mask_add))
        _, block_outs = lax.scan(advance, jnp.zeros((), jnp.float32), image_blocks)
        return block_outs
    result, pullback = jax.vjp(whole_net, grouped, params, bias_table.astype(jnp.float32))
    grad_blocks, grad_params, grad_table = pullback(cotangent.astype(jnp.float32).reshape(grouped.shape))
    return (result.reshape(images.shape).astype(jnp.bfloat16), grad_blocks.reshape(images.shape), grad_params[0], grad_params[1], grad_params[2], grad_params[3], grad_params[4], grad_params[5], grad_params[6], grad_params[7], grad_params[8], grad_params[9], grad_params[10], grad_params[11], grad_params[12], grad_table)
```

```python
import functools
import jax
import jax.numpy as jnp
import numpy as np
from jax import lax
from jax.experimental import pallas as pl
from jax.experimental.pallas import tpu as pltpu
from jax.sharding import PartitionSpec as P

HEADS = 16
HD = 32
WIN = 7
SHIFT = 3
TOK = 98
PAD = 112
LANES = 128
GROUPS = 4
NB = 8
EPS = 1e-05
FAR = -1e30
F32 = jnp.float32
BF = jnp.bfloat16
HIGHEST = lax.Precision.HIGHEST


def mm(a, b):
    return lax.dot_general(a, b, (((1,), (0,)), ((), ())), preferred_element_type=F32)


def mm_nt(a, b):
    return lax.dot_general(a, b, (((1,), (1,)), ((), ())), preferred_element_type=F32)


def mm_tn(a, b):
    return lax.dot_general(a, b, (((0,), (0,)), ((), ())), preferred_element_type=F32)


def normalized(x):
    mean = jnp.mean(x, axis=-1, keepdims=True)
    c = x - mean
    var = jnp.mean(c * c, axis=-1, keepdims=True)
    r = lax.rsqrt(var + EPS)
    return c * r, r


def norm_back(u, n, r):
    return r * (u - jnp.mean(u, axis=-1, keepdims=True) - n * jnp.mean(u * n, axis=-1, keepdims=True))


def col_sum(v):
    return jnp.sum(v, axis=0, keepdims=True)


def erf(x):
    x = jnp.clip(x, -3.7439211627767994, 3.7439211627767994)
    s = x * x
    a = (0.00022905065861350646, 0.0034082910107109506, 0.050955695062380861, 0.18520832239976145, 1.128379143519084)
    b = (-1.1791602954361697e-7, 0.000023547966471313185, 0.0010179625278914885, 0.014070470171167667, 0.11098505178285362, 0.49746925110067538, 1.0)
    p = a[0]
    for c in a[1:]:
        p = p * s + c
    q = b[0]
    for c in b[1:]:
        q = q * s + c
    return x * p / q


def head_masks():
    lane = lax.broadcasted_iota(jnp.int32, (1, LANES), 1) // HD
    return [(lane == h).astype(BF) for h in range(GROUPS)]


def attend_kernel(x_ref, g_ref, b_ref, w_ref, qb_ref, rel_ref, qkv_ref, att_ref, prob_ref, wide, joined):
    d = x_ref.shape[-1]
    n, _ = normalized(x_ref[...].astype(F32).reshape(TOK * NB, d))
    normed = (n * g_ref[...] + b_ref[...]).astype(BF)
    lanes3 = 3 * d // LANES
    chunk = 512

    @pl.when(pl.program_id(0) == 0)
    def _():
        wide[:, TOK * NB :, :] = jnp.zeros((lanes3, (PAD - TOK) * NB, LANES), F32)

    for c in range(3 * d // chunk):
        part = mm(normed, w_ref[:, c * chunk : (c + 1) * chunk]) + qb_ref[:, c * chunk : (c + 1) * chunk]
        for k in range(chunk // LANES):
            wide[c * (chunk // LANES) + k, : TOK * NB, :] = part[:, k * LANES : (k + 1) * LANES]
    masks = head_masks()
    per = d // LANES
    scale = HD ** (-0.5)

    def one(i, carry):
        for g in range(per):
            q = wide[g, pl.ds(i, PAD, stride=NB), :].astype(BF)
            k = wide[per + g, pl.ds(i, PAD, stride=NB), :].astype(BF)
            v = wide[2 * per + g, pl.ds(i, PAD, stride=NB), :].astype(BF)
            qkv_ref[i, g] = q
            qkv_ref[i, per + g] = k
            qkv_ref[i, 2 * per + g] = v
            total = None
            for h in range(GROUPS):
                s = mm_nt(q * masks[h], k) * scale + rel_ref[g * GROUPS + h][:, :PAD]
                e = jnp.exp(s - jnp.max(s, axis=-1, keepdims=True))
                p = (e / jnp.sum(e, axis=-1, keepdims=True)).astype(BF)
                prob_ref[i, g * GROUPS + h] = p
                o = mm(p, v * masks[h])
                total = o if total is None else total + o
            joined[g, pl.ds(i, PAD, stride=NB), :] = total
        return carry

    lax.fori_loop(0, NB, one, 0)
    for g in range(per):
        att_ref[:, :, g * LANES : (g + 1) * LANES] = joined[g, : TOK * NB, :].astype(BF).reshape(TOK, NB, LANES)


def attend(x, g, b, w, qb, rel):
    _, imgs, d = x.shape
    full = lambda *shape: pl.BlockSpec(shape, lambda i: (0,) * len(shape), pipeline_mode=pl.Buffered(1))
    per = d // LANES
    return pl.pallas_call(
        attend_kernel,
        grid=(imgs // NB,),
        in_specs=[
            pl.BlockSpec((TOK, NB, d), lambda i: (0, i, 0)),
            full(1, d), full(1, d), full(d, 3 * d), full(1, 3 * d), full(HEADS, PAD, LANES),
        ],
        out_specs=[
            pl.BlockSpec((NB, 3 * per, PAD, LANES), lambda i: (i, 0, 0, 0)),
            pl.BlockSpec((TOK, NB, d), lambda i: (0, i, 0)),
            pl.BlockSpec((NB, HEADS, PAD, PAD), lambda i: (i, 0, 0, 0)),
        ],
        out_shape=[
            jax.ShapeDtypeStruct((imgs, 3 * per, PAD, LANES), BF),
            jax.ShapeDtypeStruct((TOK, imgs, d), BF),
            jax.ShapeDtypeStruct((imgs, HEADS, PAD, PAD), BF),
        ],
        scratch_shapes=[
            pltpu.VMEM((3 * per, PAD * NB, LANES), F32),
            pltpu.VMEM((per, PAD * NB, LANES), F32),
        ],
        compiler_params=pltpu.CompilerParams(vmem_limit_bytes=60 << 20),
        name="attend",
    )(x, g, b, w, qb, rel)


def mlp_kernel(x_ref, att_ref, ct_ref, wp_ref, bp_ref, g_ref, b_ref, w1_ref, b1_ref, w2_ref, b2_ref,
               out_ref, gm_ref, gatt_ref, dwp_ref, dw1_ref, dw2_ref, db1_ref, small_ref,
               awp, aw1, aw2, ab1, asm):
    step = pl.program_id(0)
    d = x_ref.shape[-1]
    ff = w1_ref.shape[-1]
    chunk = 512

    @pl.when(step == 0)
    def _():
        awp[...] = jnp.zeros_like(awp)
        aw1[...] = jnp.zeros_like(aw1)
        aw2[...] = jnp.zeros_like(aw2)
        ab1[...] = jnp.zeros_like(ab1)
        asm[...] = jnp.zeros_like(asm)

    att = att_ref[...]
    gb = ct_ref[...]
    grad_out = gb.astype(F32)
    middle = x_ref[...].astype(F32) + mm(att, wp_ref[...]) + bp_ref[...]
    n, r = normalized(middle)
    normed = (n * g_ref[...] + b_ref[...]).astype(BF)
    normed_t = normed.T
    gb_t = gb.T
    out = middle + b2_ref[...]
    m = None
    for c in range(ff // chunk):
        at = slice(c * chunk, (c + 1) * chunk)
        hidden = mm(normed, w1_ref[:, at]) + b1_ref[:, at]
        cdf = 0.5 * (1.0 + erf(hidden * 0.7071067811865476))
        slope = cdf + hidden * (0.3989422804014327 * jnp.exp(-0.5 * hidden * hidden))
        active = (hidden * cdf).astype(BF)
        out = out + mm(active, w2_ref[at, :])
        gh = mm_nt(gb, w2_ref[at, :]) * slope
        ghb = gh.astype(BF)
        ab1[:, at] += col_sum(ghb.astype(F32))
        aw2[:, at] += mm(gb_t, active)
        aw1[:, at] += mm(normed_t, ghb)
        part = mm_nt(ghb, w1_ref[:, at])
        m = part if m is None else m + part
    out_ref[...] = out.astype(BF)
    grad_middle = grad_out + norm_back(m * g_ref[...], n, r)
    gm_ref[...] = grad_middle
    gp = grad_middle.astype(BF)
    gatt_ref[...] = mm_nt(gp, wp_ref[...]).astype(BF)
    awp[...] += mm_tn(att, gp)
    asm[0:1, :] += col_sum(m * n)
    asm[1:2, :] += col_sum(m)
    asm[2:3, :] += col_sum(gp.astype(F32))
    asm[3:4, :] += col_sum(grad_out)

    @pl.when(step == pl.num_programs(0) - 1)
    def _():
        dwp_ref[...] = awp[...].astype(BF)
        dw1_ref[...] = aw1[...].astype(BF)
        for c in range(ff // chunk):
            at = slice(c * chunk, (c + 1) * chunk)
            dw2_ref[at, :] = aw2[:, at].T.astype(BF)
        db1_ref[...] = ab1[...]
        small_ref[...] = asm[...]


def mlp(x, att, ct, wp, bp, g, b, w1, b1, w2, b2, tile=448):
    rows, d = x.shape
    ff = w1.shape[-1]
    full = lambda *shape: pl.BlockSpec(shape, lambda i: (0,) * len(shape), pipeline_mode=pl.Buffered(1))
    row = pl.BlockSpec((tile, d), lambda i: (i, 0))
    return pl.pallas_call(
        mlp_kernel,
        grid=(rows // tile,),
        in_specs=[row, row, row, full(d, d), full(1, d), full(1, d), full(1, d), full(d, ff), full(1, ff),
                  full(ff, d), full(1, d)],
        out_specs=[row, row, row, full(d, d), full(d, ff), full(ff, d), full(1, ff), full(8, d)],
        out_shape=[
            jax.ShapeDtypeStruct((rows, d), BF),
            jax.ShapeDtypeStruct((rows, d), F32),
            jax.ShapeDtypeStruct((rows, d), BF),
            jax.ShapeDtypeStruct((d, d), BF),
            jax.ShapeDtypeStruct((d, ff), BF),
            jax.ShapeDtypeStruct((ff, d), BF),
            jax.ShapeDtypeStruct((1, ff), F32),
            jax.ShapeDtypeStruct((8, d), F32),
        ],
        scratch_shapes=[
            pltpu.VMEM((d, d), F32), pltpu.VMEM((d, ff), F32), pltpu.VMEM((d, ff), F32),
            pltpu.VMEM((1, ff), F32), pltpu.VMEM((8, d), F32),
        ],
        compiler_params=pltpu.CompilerParams(vmem_limit_bytes=60 << 20),
        name="mlp",
    )(x, att, ct, wp, bp, g, b, w1, b1, w2, b2)


def back_kernel(x_ref, gm_ref, gatt_ref, qkv_ref, prob_ref, g_ref, b_ref, w_ref,
                gin_ref, dw_ref, small_ref, bsum_ref, rel_ref, wide, grads, aw, asm, abs_):
    step = pl.program_id(0)
    d = x_ref.shape[-1]
    per = d // LANES
    scale = HD ** (-0.5)

    @pl.when(step == 0)
    def _():
        aw[...] = jnp.zeros_like(aw)
        asm[...] = jnp.zeros_like(asm)
        abs_[...] = jnp.zeros_like(abs_)
        rel_ref[...] = jnp.zeros_like(rel_ref)
        wide[:, TOK * NB :, :] = jnp.zeros((per, (PAD - TOK) * NB, LANES), F32)

    for g in range(per):
        wide[g, : TOK * NB, :] = gatt_ref[:, :, g * LANES : (g + 1) * LANES].astype(F32).reshape(TOK * NB, LANES)
    masks = head_masks()

    def one(i, carry):
        for g in range(per):
            ga = wide[g, pl.ds(i, PAD, stride=NB), :].astype(BF)
            q = qkv_ref[i, g]
            k = qkv_ref[i, per + g]
            v = qkv_ref[i, 2 * per + g]
            dq = dk = dv = None
            for h in range(GROUPS):
                p = prob_ref[i, g * GROUPS + h]
                pf = p.astype(F32)
                gah = ga * masks[h]
                dp = mm_nt(gah, v)
                inner = jnp.sum(pf * dp, axis=-1, keepdims=True)
                ds = (pf * (dp - inner)).astype(BF)
                rel_ref[g * GROUPS + h] += ds.astype(F32)
                a, b, c = mm(ds, k * masks[h]), mm_tn(ds, q * masks[h]), mm_tn(p, gah)
                dq = a if dq is None else dq + a
                dk = b if dk is None else dk + b
                dv = c if dv is None else dv + c
            grads[g, pl.ds(i, PAD, stride=NB), :] = dq * scale
            grads[per + g, pl.ds(i, PAD, stride=NB), :] = dk * scale
            grads[2 * per + g, pl.ds(i, PAD, stride=NB), :] = dv
        return carry

    lax.fori_loop(0, NB, one, 0)
    n, r = normalized(x_ref[...].astype(F32).reshape(TOK * NB, d))
    normed = (n * g_ref[...] + b_ref[...]).astype(BF)
    normed_t = normed.T
    dn = None
    for c in range(3):
        at = slice(c * d, (c + 1) * d)
        dqkv = jnp.concatenate([grads[c * per + g, : TOK * NB, :].astype(BF) for g in range(per)], axis=-1)
        abs_[:, at] += col_sum(dqkv.astype(F32))
        aw[:, at] += mm(normed_t, dqkv)
        part = mm_nt(dqkv, w_ref[:, at])
        dn = part if dn is None else dn + part
    dn = dn.astype(BF).astype(F32)
    asm[0:1, :] += col_sum(dn * n)
    asm[1:2, :] += col_sum(dn)
    gin = gm_ref[...].reshape(TOK * NB, d) + norm_back(dn * g_ref[...], n, r)
    gin_ref[...] = gin.reshape(TOK, NB, d)

    @pl.when(step == pl.num_programs(0) - 1)
    def _():
        dw_ref[...] = aw[...].astype(BF)
        small_ref[...] = asm[...]
        bsum_ref[...] = abs_[...]


def back(x, gm, gatt, qkv, prob, g, b, w):
    _, imgs, d = x.shape
    per = d // LANES
    full = lambda *shape: pl.BlockSpec(shape, lambda i: (0,) * len(shape), pipeline_mode=pl.Buffered(1))
    tok = pl.BlockSpec((TOK, NB, d), lambda i: (0, i, 0))
    return pl.pallas_call(
        back_kernel,
        grid=(imgs // NB,),
        in_specs=[
            tok, tok, tok,
            pl.BlockSpec((NB, 3 * per, PAD, LANES), lambda i: (i, 0, 0, 0)),
            pl.BlockSpec((NB, HEADS, PAD, PAD), lambda i: (i, 0, 0, 0)),
            full(1, d), full(1, d), full(d, 3 * d),
        ],
        out_specs=[tok, full(d, 3 * d), full(8, d), full(1, 3 * d), full(HEADS, PAD, PAD)],
        out_shape=[
            jax.ShapeDtypeStruct((TOK, imgs, d), F32),
            jax.ShapeDtypeStruct((d, 3 * d), BF),
            jax.ShapeDtypeStruct((8, d), F32),
            jax.ShapeDtypeStruct((1, 3 * d), F32),
            jax.ShapeDtypeStruct((HEADS, PAD, PAD), F32),
        ],
        scratch_shapes=[
            pltpu.VMEM((per, PAD * NB, LANES), F32),
            pltpu.VMEM((3 * per, PAD * NB, LANES), F32),
            pltpu.VMEM((d, 3 * d), F32),
            pltpu.VMEM((8, d), F32),
            pltpu.VMEM((1, 3 * d), F32),
        ],
        compiler_params=pltpu.CompilerParams(vmem_limit_bytes=60 << 20),
        name="back",
    )(x, gm, gatt, qkv, prob, g, b, w)


def swap_rows(array, rows):
    incoming = lax.ppermute(array[:rows], "win", [(0, 1), (1, 0)])
    return jnp.concatenate([incoming, array[rows:]], axis=0)


def window_of_tokens():
    row, col = np.arange(TOK) // (2 * WIN), np.arange(TOK) % (2 * WIN)
    row, col = (row - SHIFT) % WIN, (col - SHIFT) % (2 * WIN)
    return col // WIN, row * WIN + col % WIN


def spread_matrix():
    _, place = window_of_tokens()
    return (place[:, None] == np.arange(WIN * WIN)[None, :]).astype(np.float32)


def relative_parts(rel_index, table):
    count = WIN * WIN
    onehot = (rel_index.reshape(count * count, 1) == jnp.arange(table.shape[0], dtype=jnp.int32)[None, :]).astype(F32)
    relative = jnp.dot(onehot, table, precision=HIGHEST).reshape(count, count, -1).transpose(2, 0, 1)
    return onehot, relative


def bias_of_pairs(relative, regions):
    side, place = window_of_tokens()
    spread = jnp.asarray(spread_matrix())
    wide = jnp.einsum("at,hts,bs->hab", spread, relative, spread, precision=HIGHEST)
    region = regions.reshape(2, WIN * WIN)
    region = jnp.concatenate(
        [jnp.roll(region[s].reshape(WIN, WIN), SHIFT, axis=0)[:, c] for s, c in ((1, slice(4, 7)), (0, slice(0, 7)), (1, slice(0, 4)))],
        axis=1,
    ).reshape(TOK)
    mask = jnp.where(region[:, None] == region[None, :], 0.0, -100.0)
    same = jnp.asarray(side[:, None] == side[None, :])
    bias = jnp.where(same[None], wide + mask[None], FAR)
    return jnp.pad(
        jnp.pad(bias, ((0, 0), (0, 0), (0, LANES - TOK)), constant_values=FAR),
        ((0, 0), (0, PAD - TOK), (0, 0)),
    )


def owner_blocks(array, count):
    return array.reshape(count, array.shape[0] // count, *array.shape[1:])


def delivered(blocks):
    mine = lax.all_to_all(blocks, "fsdp", 0, 0, tiled=True)
    mine = jnp.sum(mine.astype(F32), axis=0).astype(BF)
    other = lax.ppermute(mine, "win", [(0, 1), (1, 0)])
    return mine.astype(F32) + other.astype(F32)


def per_device(
    images, norm1_gain, norm1_bias, qkv_weight, q_bias, v_bias, proj_weight, proj_bias, norm2_gain, norm2_bias,
    fc1_weight, fc1_bias, fc2_weight, fc2_bias, bias_table, regions, rel_index, cotangent,
):
    imgs, rows, cols, d = images.shape
    top = SHIFT * cols
    owners = lax.axis_size("fsdp")
    x = swap_rows(images.transpose(1, 2, 0, 3).reshape(rows * cols, imgs, d), top)
    ct = swap_rows(cotangent.transpose(1, 2, 0, 3).reshape(rows * cols, imgs, d), top)
    vectors = (norm1_gain, norm1_bias, q_bias, v_bias, proj_bias, norm2_gain, norm2_bias, fc2_bias, fc1_bias)
    packed = lax.all_gather(jnp.concatenate(vectors), "fsdp", axis=0).astype(F32)
    at, whole = 0, []
    for v in vectors:
        whole.append(packed[:, at : at + v.shape[0]].reshape(1, -1))
        at += v.shape[0]
    g1, b1, qb, vb, bp, g2, b2, b_out, b_in = whole
    gather = functools.partial(lax.all_gather, axis_name="fsdp", axis=0, tiled=True)
    w_qkv, w_proj, w_in, w_out = gather(qkv_weight), gather(proj_weight), gather(fc1_weight), gather(fc2_weight)
    onehot, relative = relative_parts(rel_index, bias_table)
    rel = bias_of_pairs(relative, regions)
    qkv_bias = jnp.concatenate([qb, jnp.zeros_like(qb), vb], axis=1)

    qkv, att, prob = attend(x, g1, b1, w_qkv, qkv_bias, rel)
    flat = lambda v: v.reshape(rows * cols * imgs, d)
    out, gm, gatt, dwp, dw1, dw2, db_in, small2 = mlp(
        flat(x), flat(att), flat(ct), w_proj, bp, g2, b2, w_in, b_in, w_out, b_out
    )
    tall = lambda v: v.reshape(rows * cols, imgs, d)
    gin, dwq, small1, bsum, rel_sum = back(x, tall(gm), tall(gatt), qkv, prob, g1, b1, w_qkv)

    dw1, dw2, dwp, dwq = (delivered(owner_blocks(v, owners)) for v in (dw1, dw2, dwp, dwq))
    grads = (
        small1[0], small1[1], bsum[0, :d], bsum[0, 2 * d :], small2[2], small2[0], small2[1], small2[3], db_in[0],
    )
    sums = delivered(jnp.concatenate([v.reshape(owners, -1) for v in grads], axis=1).astype(BF))
    at, own = 0, []
    for v in vectors:
        own.append(sums[at : at + v.shape[0]].reshape(-1) if sums.ndim == 1 else sums[0, at : at + v.shape[0]])
        at += v.shape[0]
    dg1, db1, dqb, dvb, dbp, dg2, db2, db_out, db_in = own
    spread = jnp.asarray(spread_matrix())
    pairs = jnp.einsum("at,hab,bs->tsh", spread, rel_sum[:, :TOK, :TOK], spread, precision=HIGHEST)
    table = jnp.dot(onehot.T, pairs.reshape(WIN**4, -1), precision=HIGHEST)
    table = lax.psum(table, ("fsdp", "win"))
    back_to_images = lambda v: swap_rows(v, top).reshape(rows, cols, imgs, d).transpose(2, 0, 1, 3)
    return (
        back_to_images(tall(out)), back_to_images(gin), dg1, db1, dwq, dqb, dvb, dwp, dbp, dg2, db2, dw1, db_in, dw2,
        db_out, table,
    )


def solution(mesh):
    vec, mat, img = P("fsdp"), P("fsdp", None), P("fsdp", "win", None, None)
    in_specs = (
        img, vec, vec, mat, vec, vec, mat, vec, vec, vec, mat, vec, mat, vec, P(), P("win", None, None), P(), img,
    )
    out_specs = (img, img, vec, vec, mat, vec, vec, mat, vec, vec, vec, mat, vec, mat, vec, P())
    return jax.shard_map(per_device, mesh=mesh, in_specs=in_specs, out_specs=out_specs, check_vma=False)
```

```python
import functools
import jax
import jax.numpy as jnp
import numpy as np
from jax import lax
from jax.experimental import pallas as pl
from jax.experimental.pallas import tpu as pltpu
from jax.sharding import PartitionSpec as P

HEADS = 16
HD = 32
WIN = 7
SHIFT = 3
TOK = 98
PAD = 112
LANES = 128
GROUPS = 4
NB = 8
EPS = 1e-05
FAR = -1e30
F32 = jnp.float32
BF = jnp.bfloat16
HIGHEST = lax.Precision.HIGHEST


def mm(a, b):
    return lax.dot_general(a, b, (((1,), (0,)), ((), ())), preferred_element_type=F32)


def mm_nt(a, b):
    return lax.dot_general(a, b, (((1,), (1,)), ((), ())), preferred_element_type=F32)


def mm_tn(a, b):
    return lax.dot_general(a, b, (((0,), (0,)), ((), ())), preferred_element_type=F32)


def normalized(x):
    mean = jnp.mean(x, axis=-1, keepdims=True)
    c = x - mean
    var = jnp.mean(c * c, axis=-1, keepdims=True)
    r = lax.rsqrt(var + EPS)
    return c * r, r


def norm_back(u, n, r):
    return r * (u - jnp.mean(u, axis=-1, keepdims=True) - n * jnp.mean(u * n, axis=-1, keepdims=True))


def col_sum(v):
    return jnp.sum(v, axis=0, keepdims=True)


def erf(x):
    x = jnp.clip(x, -3.7439211627767994, 3.7439211627767994)
    s = x * x
    a = (0.00022905065861350646, 0.0034082910107109506, 0.050955695062380861, 0.18520832239976145, 1.128379143519084)
    b = (-1.1791602954361697e-7, 0.000023547966471313185, 0.0010179625278914885, 0.014070470171167667, 0.11098505178285362, 0.49746925110067538, 1.0)
    p = a[0]
    for c in a[1:]:
        p = p * s + c
    q = b[0]
    for c in b[1:]:
        q = q * s + c
    return x * p / q


def head_masks():
    lane = lax.broadcasted_iota(jnp.int32, (1, LANES), 1) // HD
    return [(lane == h).astype(BF) for h in range(GROUPS)]


def attend_kernel(x_ref, g_ref, b_ref, w_ref, qb_ref, rel_ref, qkv_ref, att_ref, prob_ref, wide, joined):
    d = x_ref.shape[-1]
    n, _ = normalized(x_ref[...].astype(F32).reshape(TOK * NB, d))
    normed = (n * g_ref[...] + b_ref[...]).astype(BF)
    lanes3 = 3 * d // LANES
    chunk = 512

    @pl.when(pl.program_id(0) == 0)
    def _():
        wide[:, TOK * NB :, :] = jnp.zeros((lanes3, (PAD - TOK) * NB, LANES), F32)

    for c in range(3 * d // chunk):
        part = mm(normed, w_ref[:, c * chunk : (c + 1) * chunk]) + qb_ref[:, c * chunk : (c + 1) * chunk]
        for k in range(chunk // LANES):
            wide[c * (chunk // LANES) + k, : TOK * NB, :] = part[:, k * LANES : (k + 1) * LANES]
    masks = head_masks()
    per = d // LANES
    scale = HD ** (-0.5)

    def one(i, carry):
        for g in range(per):
            q = wide[g, pl.ds(i, PAD, stride=NB), :].astype(BF)
            k = wide[per + g, pl.ds(i, PAD, stride=NB), :].astype(BF)
            v = wide[2 * per + g, pl.ds(i, PAD, stride=NB), :].astype(BF)
            qkv_ref[i, g] = q
            qkv_ref[i, per + g] = k
            qkv_ref[i, 2 * per + g] = v
            total = None
            for h in range(GROUPS):
                s = mm_nt(q * masks[h], k) * scale + rel_ref[g * GROUPS + h][:, :PAD]
                e = jnp.exp(s - jnp.max(s, axis=-1, keepdims=True))
                p = (e / jnp.sum(e, axis=-1, keepdims=True)).astype(BF)
                prob_ref[i, g * GROUPS + h] = p
                o = mm(p, v * masks[h])
                total = o if total is None else total + o
            joined[g, pl.ds(i, PAD, stride=NB), :] = total
        return carry

    lax.fori_loop(0, NB, one, 0)
    for g in range(per):
        att_ref[:, :, g * LANES : (g + 1) * LANES] = joined[g, : TOK * NB, :].astype(BF).reshape(TOK, NB, LANES)


def attend(x, g, b, w, qb, rel):
    _, imgs, d = x.shape
    full = lambda *shape: pl.BlockSpec(shape, lambda i: (0,) * len(shape), pipeline_mode=pl.Buffered(1))
    per = d // LANES
    return pl.pallas_call(
        attend_kernel,
        grid=(imgs // NB,),
        in_specs=[
            pl.BlockSpec((TOK, NB, d), lambda i: (0, i, 0)),
            full(1, d), full(1, d), full(d, 3 * d), full(1, 3 * d), full(HEADS, PAD, LANES),
        ],
        out_specs=[
            pl.BlockSpec((NB, 3 * per, PAD, LANES), lambda i: (i, 0, 0, 0)),
            pl.BlockSpec((TOK, NB, d), lambda i: (0, i, 0)),
            pl.BlockSpec((NB, HEADS, PAD, PAD), lambda i: (i, 0, 0, 0)),
        ],
        out_shape=[
            jax.ShapeDtypeStruct((imgs, 3 * per, PAD, LANES), BF),
            jax.ShapeDtypeStruct((TOK, imgs, d), BF),
            jax.ShapeDtypeStruct((imgs, HEADS, PAD, PAD), BF),
        ],
        scratch_shapes=[
            pltpu.VMEM((3 * per, PAD * NB, LANES), F32),
            pltpu.VMEM((per, PAD * NB, LANES), F32),
        ],
        compiler_params=pltpu.CompilerParams(vmem_limit_bytes=60 << 20),
        name="attend",
    )(x, g, b, w, qb, rel)


def mlp_kernel(x_ref, att_ref, ct_ref, wp_ref, bp_ref, g_ref, b_ref, w1_ref, b1_ref, w2_ref, b2_ref,
               out_ref, gm_ref, gatt_ref, dwp_ref, dw1_ref, dw2_ref, db1_ref, small_ref,
               awp, aw1, aw2, ab1, asm):
    step = pl.program_id(0)
    d = x_ref.shape[-1]
    ff = w1_ref.shape[-1]
    chunk = 512

    @pl.when(step == 0)
    def _():
        awp[...] = jnp.zeros_like(awp)
        aw1[...] = jnp.zeros_like(aw1)
        aw2[...] = jnp.zeros_like(aw2)
        ab1[...] = jnp.zeros_like(ab1)
        asm[...] = jnp.zeros_like(asm)

    att = att_ref[...]
    gb = ct_ref[...]
    grad_out = gb.astype(F32)
    middle = x_ref[...].astype(F32) + mm(att, wp_ref[...]) + bp_ref[...]
    n, r = normalized(middle)
    normed = (n * g_ref[...] + b_ref[...]).astype(BF)
    normed_t = normed.T
    gb_t = gb.T
    out = middle + b2_ref[...]
    m = None
    for c in range(ff // chunk):
        at = slice(c * chunk, (c + 1) * chunk)
        hidden = mm(normed, w1_ref[:, at]) + b1_ref[:, at]
        cdf = 0.5 * (1.0 + erf(hidden * 0.7071067811865476))
        slope = cdf + hidden * (0.3989422804014327 * jnp.exp(-0.5 * hidden * hidden))
        active = (hidden * cdf).astype(BF)
        out = out + mm(active, w2_ref[at, :])
        gh = mm_nt(gb, w2_ref[at, :]) * slope
        ghb = gh.astype(BF)
        ab1[:, at] += col_sum(ghb.astype(F32))
        aw2[:, at] += mm(gb_t, active)
        aw1[:, at] += mm(normed_t, ghb)
        part = mm_nt(ghb, w1_ref[:, at])
        m = part if m is None else m + part
    out_ref[...] = out.astype(BF)
    grad_middle = grad_out + norm_back(m * g_ref[...], n, r)
    gm_ref[...] = grad_middle
    gp = grad_middle.astype(BF)
    gatt_ref[...] = mm_nt(gp, wp_ref[...]).astype(BF)
    awp[...] += mm_tn(att, gp)
    asm[0:1, :] += col_sum(m * n)
    asm[1:2, :] += col_sum(m)
    asm[2:3, :] += col_sum(gp.astype(F32))
    asm[3:4, :] += col_sum(grad_out)

    @pl.when(step == pl.num_programs(0) - 1)
    def _():
        dwp_ref[...] = awp[...].astype(BF)
        dw1_ref[...] = aw1[...].astype(BF)
        for c in range(ff // chunk):
            at = slice(c * chunk, (c + 1) * chunk)
            dw2_ref[at, :] = aw2[:, at].T.astype(BF)
        db1_ref[...] = ab1[...]
        small_ref[...] = asm[...]


def mlp(x, att, ct, wp, bp, g, b, w1, b1, w2, b2, tile=448):
    rows, d = x.shape
    ff = w1.shape[-1]
    full = lambda *shape: pl.BlockSpec(shape, lambda i: (0,) * len(shape), pipeline_mode=pl.Buffered(1))
    row = pl.BlockSpec((tile, d), lambda i: (i, 0))
    return pl.pallas_call(
        mlp_kernel,
        grid=(rows // tile,),
        in_specs=[row, row, row, full(d, d), full(1, d), full(1, d), full(1, d), full(d, ff), full(1, ff),
                  full(ff, d), full(1, d)],
        out_specs=[row, row, row, full(d, d), full(d, ff), full(ff, d), full(1, ff), full(8, d)],
        out_shape=[
            jax.ShapeDtypeStruct((rows, d), BF),
            jax.ShapeDtypeStruct((rows, d), F32),
            jax.ShapeDtypeStruct((rows, d), BF),
            jax.ShapeDtypeStruct((d, d), BF),
            jax.ShapeDtypeStruct((d, ff), BF),
            jax.ShapeDtypeStruct((ff, d), BF),
            jax.ShapeDtypeStruct((1, ff), F32),
            jax.ShapeDtypeStruct((8, d), F32),
        ],
        scratch_shapes=[
            pltpu.VMEM((d, d), F32), pltpu.VMEM((d, ff), F32), pltpu.VMEM((d, ff), F32),
            pltpu.VMEM((1, ff), F32), pltpu.VMEM((8, d), F32),
        ],
        compiler_params=pltpu.CompilerParams(vmem_limit_bytes=60 << 20),
        name="mlp",
    )(x, att, ct, wp, bp, g, b, w1, b1, w2, b2)


def back_kernel(x_ref, gm_ref, gatt_ref, qkv_ref, prob_ref, g_ref, b_ref, w_ref,
                gin_ref, dw_ref, small_ref, bsum_ref, rel_ref, wide, grads, aw, asm, abs_):
    step = pl.program_id(0)
    d = x_ref.shape[-1]
    per = d // LANES
    scale = HD ** (-0.5)

    @pl.when(step == 0)
    def _():
        aw[...] = jnp.zeros_like(aw)
        asm[...] = jnp.zeros_like(asm)
        abs_[...] = jnp.zeros_like(abs_)
        rel_ref[...] = jnp.zeros_like(rel_ref)
        wide[:, TOK * NB :, :] = jnp.zeros((per, (PAD - TOK) * NB, LANES), F32)

    for g in range(per):
        wide[g, : TOK * NB, :] = gatt_ref[:, :, g * LANES : (g + 1) * LANES].astype(F32).reshape(TOK * NB, LANES)
    masks = head_masks()

    def one(i, carry):
        for g in range(per):
            ga = wide[g, pl.ds(i, PAD, stride=NB), :].astype(BF)
            q = qkv_ref[i, g]
            k = qkv_ref[i, per + g]
            v = qkv_ref[i, 2 * per + g]
            dq = dk = dv = None
            for h in range(GROUPS):
                p = prob_ref[i, g * GROUPS + h]
                pf = p.astype(F32)
                gah = ga * masks[h]
                dp = mm_nt(gah, v)
                inner = jnp.sum(pf * dp, axis=-1, keepdims=True)
                ds = (pf * (dp - inner)).astype(BF)
                rel_ref[g * GROUPS + h] += ds.astype(F32)
                a, b, c = mm(ds, k * masks[h]), mm_tn(ds, q * masks[h]), mm_tn(p, gah)
                dq = a if dq is None else dq + a
                dk = b if dk is None else dk + b
                dv = c if dv is None else dv + c
            grads[g, pl.ds(i, PAD, stride=NB), :] = dq * scale
            grads[per + g, pl.ds(i, PAD, stride=NB), :] = dk * scale
            grads[2 * per + g, pl.ds(i, PAD, stride=NB), :] = dv
        return carry

    lax.fori_loop(0, NB, one, 0)
    n, r = normalized(x_ref[...].astype(F32).reshape(TOK * NB, d))
    normed = (n * g_ref[...] + b_ref[...]).astype(BF)
    normed_t = normed.T
    dn = None
    for c in range(3):
        at = slice(c * d, (c + 1) * d)
        dqkv = jnp.concatenate([grads[c * per + g, : TOK * NB, :].astype(BF) for g in range(per)], axis=-1)
        abs_[:, at] += col_sum(dqkv.astype(F32))
        aw[:, at] += mm(normed_t, dqkv)
        part = mm_nt(dqkv, w_ref[:, at])
        dn = part if dn is None else dn + part
    dn = dn.astype(BF).astype(F32)
    asm[0:1, :] += col_sum(dn * n)
    asm[1:2, :] += col_sum(dn)
    gin = gm_ref[...].reshape(TOK * NB, d) + norm_back(dn * g_ref[...], n, r)
    gin_ref[...] = gin.reshape(TOK, NB, d)

    @pl.when(step == pl.num_programs(0) - 1)
    def _():
        dw_ref[...] = aw[...].astype(BF)
        small_ref[...] = asm[...]
        bsum_ref[...] = abs_[...]


def back(x, gm, gatt, qkv, prob, g, b, w):
    _, imgs, d = x.shape
    per = d // LANES
    full = lambda *shape: pl.BlockSpec(shape, lambda i: (0,) * len(shape), pipeline_mode=pl.Buffered(1))
    tok = pl.BlockSpec((TOK, NB, d), lambda i: (0, i, 0))
    return pl.pallas_call(
        back_kernel,
        grid=(imgs // NB,),
        in_specs=[
            tok, tok, tok,
            pl.BlockSpec((NB, 3 * per, PAD, LANES), lambda i: (i, 0, 0, 0)),
            pl.BlockSpec((NB, HEADS, PAD, PAD), lambda i: (i, 0, 0, 0)),
            full(1, d), full(1, d), full(d, 3 * d),
        ],
        out_specs=[tok, full(d, 3 * d), full(8, d), full(1, 3 * d), full(HEADS, PAD, PAD)],
        out_shape=[
            jax.ShapeDtypeStruct((TOK, imgs, d), F32),
            jax.ShapeDtypeStruct((d, 3 * d), BF),
            jax.ShapeDtypeStruct((8, d), F32),
            jax.ShapeDtypeStruct((1, 3 * d), F32),
            jax.ShapeDtypeStruct((HEADS, PAD, PAD), F32),
        ],
        scratch_shapes=[
            pltpu.VMEM((per, PAD * NB, LANES), F32),
            pltpu.VMEM((3 * per, PAD * NB, LANES), F32),
            pltpu.VMEM((d, 3 * d), F32),
            pltpu.VMEM((8, d), F32),
            pltpu.VMEM((1, 3 * d), F32),
        ],
        compiler_params=pltpu.CompilerParams(vmem_limit_bytes=60 << 20),
        name="back",
    )(x, gm, gatt, qkv, prob, g, b, w)


DEEP = 4


class Place:
    def __init__(self, inner):
        self.inner = inner
        me, core = lax.axis_index("fsdp"), lax.axis_index("win")
        self.core, self.mate = core, 1 - core
        self.z = me // (inner * inner)
        u, v = (me // inner) % inner, me % inner
        self.a = u * (1 - core) + v * core
        self.b = v * (1 - core) + u * core
        self.step_a = inner * (1 - core) + core
        self.step_b = inner * core + 1 - core

    def at(self, dz=0, da=0, db=0):
        z = (self.z + dz) % DEEP
        a = (self.a + da) % self.inner
        b = (self.b + db) % self.inner
        return z * self.inner * self.inner + a * self.step_a + b * self.step_b

    def device(self, dz=0, da=0, db=0):
        return (self.at(dz, da, db), self.core)

    def partner(self):
        return (self.at(), self.mate)

    def peers(self):
        near = [self.device(dz=d) for d in range(1, DEEP)]
        near += [self.device(da=d) for d in range(1, self.inner)]
        near += [self.device(db=d) for d in range(1, self.inner)]
        return near + [self.partner()]


def meet(place):
    barrier = pltpu.get_barrier_semaphore()
    peers = place.peers()
    for peer in peers:
        pl.semaphore_signal(barrier, inc=1, device_id=peer, device_id_type=pl.DeviceIdType.MESH)
    pl.semaphore_wait(barrier, len(peers))


def remote(src, dst, send_sem, recv_sem, device):
    return pltpu.make_async_remote_copy(
        src_ref=src, dst_ref=dst, send_sem=send_sem, recv_sem=recv_sem, device_id=device,
        device_id_type=pl.DeviceIdType.MESH,
    )


def gather_kernel(inner, kinds, *refs):
    ins, outs = refs[:kinds], refs[kinds : 2 * kinds]
    send_sem, recv_sem, own_sem = refs[2 * kinds :]
    place = Place(inner)
    meet(place)

    def piece(k, block, core):
        half = outs[k].shape[-1] // 2
        return outs[k].at[block, :, pl.ds(pl.multiple_of(core * half, LANES), half)]

    def mine(k):
        half = outs[k].shape[-1] // 2
        return ins[k].at[:, pl.ds(pl.multiple_of(place.core * half, LANES), half)]

    sent = [[] for _ in range(kinds)]

    def send(k, src, block, device):
        copy = remote(src, piece(k, block, place.core), send_sem.at[k, len(sent[k])],
                      recv_sem.at[k, place.core, block], device)
        copy.start()
        sent[k].append(copy)

    def arrive(k, core, block):
        at = piece(k, block, core)
        remote(at, at, send_sem.at[k, 0], recv_sem.at[k, core, block], place.partner()).wait_recv()

    steps = range(1, inner)
    order_z = (1, 3, 2)
    own = []
    for k in range(kinds):
        for d in order_z:
            send(k, mine(k), place.at(), place.device(dz=d))
        for d in steps:
            send(k, mine(k), place.at(), place.device(da=d))
        for d in steps:
            send(k, mine(k), place.at(), place.device(db=d))
    for k in range(kinds):
        copy = pltpu.make_async_copy(ins[k], outs[k].at[place.at()], own_sem.at[k])
        copy.start()
        own.append(copy)

    def pass_on(k, block, along_a, along_b):
        arrive(k, place.core, block)
        src = piece(k, block, place.core)
        if along_a:
            for d in steps:
                send(k, src, block, place.device(da=d))
        if along_b:
            for d in steps:
                send(k, src, block, place.device(db=d))
        send(k, src, block, place.partner())

    for k in range(kinds):
        for dz in order_z:
            pass_on(k, place.at(dz=dz), True, True)
        for da in steps:
            for dz in (0,) + order_z:
                pass_on(k, place.at(dz=dz, da=da), False, True)
    for k in range(kinds):
        for db in steps:
            for da in range(inner):
                for dz in (0,) + order_z:
                    pass_on(k, place.at(dz=dz, da=da, db=db), False, False)
    for k in range(kinds):
        for db in range(inner):
            for da in range(inner):
                for dz in range(DEEP):
                    if db or da or dz:
                        arrive(k, place.mate, place.at(dz, da, db))
        own[k].wait()
        for copy in sent[k]:
            copy.wait_send()


def inner_of(owners):
    return int(round((owners // DEEP) ** 0.5))


def gathered(shards):
    owners = lax.axis_size("fsdp")
    inner, kinds = inner_of(owners), len(shards)
    sends = (DEEP - 1) + 2 * (inner - 1) + 1 + (DEEP - 1) * (2 * inner - 1) + DEEP * (inner - 1) * inner + DEEP * inner * (inner - 1)
    anywhere = pl.BlockSpec(memory_space=pl.ANY)
    return pl.pallas_call(
        functools.partial(gather_kernel, inner, kinds),
        in_specs=[anywhere] * kinds,
        out_specs=[anywhere] * kinds,
        out_shape=[jax.ShapeDtypeStruct((owners, *s.shape), s.dtype) for s in shards],
        scratch_shapes=[
            pltpu.SemaphoreType.DMA((kinds, sends)),
            pltpu.SemaphoreType.DMA((kinds, 2, owners)),
            pltpu.SemaphoreType.DMA((kinds,)),
        ],
        compiler_params=pltpu.CompilerParams(collective_id=0, has_side_effects=True),
        name="gather",
    )(*shards)


def deliver_kernel(inner, kinds, *refs):
    ins, outs = refs[:kinds], refs[kinds : 2 * kinds]
    at = 2 * kinds
    own, from_mate, from_b, from_a, from_z, final = (refs[at + i * kinds : at + (i + 1) * kinds] for i in range(6))
    load_sem, mate_sem, b_sem, a_sem, z_sem, end_sem = refs[at + 6 * kinds :]
    owners = DEEP * inner * inner
    place = Place(inner)
    steps = range(1, inner)
    meet(place)

    def columns(k, core):
        half = outs[k].shape[-1] // 2
        return pl.ds(pl.multiple_of(core * half, LANES), half)

    loads, swaps = [], []
    for k in range(kinds):
        swap = remote(ins[k].at[:, :, columns(k, place.mate)], from_mate[k], mate_sem.at[k, 0], mate_sem.at[k, 1],
                      place.partner())
        swap.start()
        load = pltpu.make_async_copy(ins[k].at[:, :, columns(k, place.core)], own[k], load_sem.at[k])
        load.start()
        swaps.append(swap)
        loads.append(load)

    sent = []

    def add(k, block, other):
        own[k][block] = (own[k][block].astype(F32) + other[...].astype(F32)).astype(BF)

    for k in range(kinds):
        loads[k].wait()
        swaps[k].wait()
        for db in tuple(steps) + (0,):
            for da in range(inner):
                for dz in range(DEEP):
                    block = place.at(dz, da, db)
                    add(k, block, from_mate[k].at[block])
                    if db:
                        slot = (db - 1) * inner * DEEP + da * DEEP + dz
                        copy = remote(own[k].at[block], from_b[k].at[slot], b_sem.at[k, 0, slot],
                                      b_sem.at[k, 1, slot], place.device(db=db))
                        copy.start()
                        sent.append((k, copy))
    arrivals_b = list(sent)
    sent = []
    for k in range(kinds):
        for kk, copy in arrivals_b:
            if kk == k:
                copy.wait()
        for da in tuple(steps) + (0,):
            for dz in range(DEEP):
                block = place.at(dz, da)
                for db in steps:
                    add(k, block, from_b[k].at[(db - 1) * inner * DEEP + da * DEEP + dz])
                if da:
                    slot = (da - 1) * DEEP + dz
                    copy = remote(own[k].at[block], from_a[k].at[slot], a_sem.at[k, 0, slot], a_sem.at[k, 1, slot],
                                  place.device(da=da))
                    copy.start()
                    sent.append((k, copy))
    arrivals_a = list(sent)
    sent = []
    for k in range(kinds):
        for kk, copy in arrivals_a:
            if kk == k:
                copy.wait()
        for dz in (2, 1, 3, 0):
            block = place.at(dz)
            for da in steps:
                add(k, block, from_a[k].at[(da - 1) * DEEP + dz])
            if dz:
                copy = remote(own[k].at[block], from_z[k].at[dz - 1], z_sem.at[k, 0, dz - 1], z_sem.at[k, 1, dz - 1],
                              place.device(dz=dz))
                copy.start()
                sent.append((k, copy))
    ends = []
    for k in range(kinds):
        for kk, copy in sent:
            if kk == k:
                copy.wait()
        total = own[k][place.at()].astype(F32)
        for dz in range(1, DEEP):
            total = total + from_z[k][dz - 1].astype(F32)
        final[k][...] = total
        there = outs[k].at[:, columns(k, place.core)]
        far = remote(final[k], there, end_sem.at[k, 0], end_sem.at[k, 1], place.partner())
        near = pltpu.make_async_copy(final[k], there, end_sem.at[k, 2])
        far.start()
        near.start()
        ends += [far, near]
    for copy in ends:
        copy.wait()


def delivered(grads):
    owners = lax.axis_size("fsdp")
    inner, kinds = inner_of(owners), len(grads)
    anywhere = pl.BlockSpec(memory_space=pl.ANY)
    halves = [(g.shape[1], g.shape[2] // 2) for g in grads]

    def room(count, dtype=BF):
        return [pltpu.VMEM((count, *h), dtype) for h in halves]

    dma = pltpu.SemaphoreType.DMA
    return pl.pallas_call(
        functools.partial(deliver_kernel, inner, kinds),
        in_specs=[anywhere] * kinds,
        out_specs=[anywhere] * kinds,
        out_shape=[jax.ShapeDtypeStruct(g.shape[1:], F32) for g in grads],
        scratch_shapes=[
            *room(owners), *room(owners), *room((inner - 1) * inner * DEEP), *room((inner - 1) * DEEP),
            *room(DEEP - 1), *[pltpu.VMEM(h, F32) for h in halves],
            dma((kinds,)), dma((kinds, 2)), dma((kinds, 2, (inner - 1) * inner * DEEP)),
            dma((kinds, 2, (inner - 1) * DEEP)), dma((kinds, 2, DEEP - 1)), dma((kinds, 3)),
        ],
        compiler_params=pltpu.CompilerParams(collective_id=1, has_side_effects=True, vmem_limit_bytes=60 << 20),
        name="deliver",
    )(*grads)


def swap_rows(array, rows):
    incoming = lax.ppermute(array[:rows], "win", [(0, 1), (1, 0)])
    return jnp.concatenate([incoming, array[rows:]], axis=0)


def window_of_tokens():
    row, col = np.arange(TOK) // (2 * WIN), np.arange(TOK) % (2 * WIN)
    row, col = (row - SHIFT) % WIN, (col - SHIFT) % (2 * WIN)
    return col // WIN, row * WIN + col % WIN


def spread_matrix():
    _, place = window_of_tokens()
    return (place[:, None] == np.arange(WIN * WIN)[None, :]).astype(np.float32)


def relative_parts(rel_index, table):
    count = WIN * WIN
    onehot = (rel_index.reshape(count * count, 1) == jnp.arange(table.shape[0], dtype=jnp.int32)[None, :]).astype(F32)
    relative = jnp.dot(onehot, table, precision=HIGHEST).reshape(count, count, -1).transpose(2, 0, 1)
    return onehot, relative


def bias_of_pairs(relative, regions):
    side, place = window_of_tokens()
    spread = jnp.asarray(spread_matrix())
    wide = jnp.einsum("at,hts,bs->hab", spread, relative, spread, precision=HIGHEST)
    region = regions.reshape(2, WIN * WIN)
    region = jnp.concatenate(
        [jnp.roll(region[s].reshape(WIN, WIN), SHIFT, axis=0)[:, c] for s, c in ((1, slice(4, 7)), (0, slice(0, 7)), (1, slice(0, 4)))],
        axis=1,
    ).reshape(TOK)
    mask = jnp.where(region[:, None] == region[None, :], 0.0, -100.0)
    same = jnp.asarray(side[:, None] == side[None, :])
    bias = jnp.where(same[None], wide + mask[None], FAR)
    return jnp.pad(
        jnp.pad(bias, ((0, 0), (0, 0), (0, LANES - TOK)), constant_values=FAR),
        ((0, 0), (0, PAD - TOK), (0, 0)),
    )


def packed_row(parts):
    row = jnp.concatenate(parts, axis=-1)
    return jnp.pad(row, [(0, 0)] * (row.ndim - 1) + [(0, -row.shape[-1] % (2 * LANES))])


def per_device(
    images, norm1_gain, norm1_bias, qkv_weight, q_bias, v_bias, proj_weight, proj_bias, norm2_gain, norm2_bias,
    fc1_weight, fc1_bias, fc2_weight, fc2_bias, bias_table, regions, rel_index, cotangent,
):
    imgs, rows, cols, d = images.shape
    top = SHIFT * cols
    owners = lax.axis_size("fsdp")
    x = swap_rows(images.transpose(1, 2, 0, 3).reshape(rows * cols, imgs, d), top)
    ct = swap_rows(cotangent.transpose(1, 2, 0, 3).reshape(rows * cols, imgs, d), top)
    vectors = (norm1_gain, norm1_bias, q_bias, v_bias, proj_bias, norm2_gain, norm2_bias, fc2_bias, fc1_bias)
    shards = (packed_row(vectors)[None], qkv_weight, proj_weight, fc1_weight, fc2_weight)
    packed, *mats = gathered(shards)
    packed = packed[:, 0].astype(F32)
    at, whole = 0, []
    for v in vectors:
        whole.append(packed[:, at : at + v.shape[0]].reshape(1, -1))
        at += v.shape[0]
    g1, b1, qb, vb, bp, g2, b2, b_out, b_in = whole
    w_qkv, w_proj, w_in, w_out = (v.reshape(owners * v.shape[1], v.shape[2]) for v in mats)
    onehot, relative = relative_parts(rel_index, bias_table)
    rel = bias_of_pairs(relative, regions)
    qkv_bias = jnp.concatenate([qb, jnp.zeros_like(qb), vb], axis=1)

    qkv, att, prob = attend(x, g1, b1, w_qkv, qkv_bias, rel)
    flat = lambda v: v.reshape(rows * cols * imgs, d)
    out, gm, gatt, dwp, dw1, dw2, db_in, small2 = mlp(
        flat(x), flat(att), flat(ct), w_proj, bp, g2, b2, w_in, b_in, w_out, b_out
    )
    tall = lambda v: v.reshape(rows * cols, imgs, d)
    gin, dwq, small1, bsum, rel_sum = back(x, tall(gm), tall(gatt), qkv, prob, g1, b1, w_qkv)

    grads = (
        small1[0], small1[1], bsum[0, :d], bsum[0, 2 * d :], small2[2], small2[0], small2[1], small2[3], db_in[0],
    )
    row = packed_row([v.reshape(owners, 1, -1) for v in grads]).astype(BF)
    blocks = lambda v: v.reshape(owners, v.shape[0] // owners, v.shape[1])
    sums, dwp, dw1, dw2, dwq = delivered((row, blocks(dwp), blocks(dw1), blocks(dw2), blocks(dwq)))
    at, own = 0, []
    for v in vectors:
        own.append(sums[0, at : at + v.shape[0]])
        at += v.shape[0]
    dg1, db1, dqb, dvb, dbp, dg2, db2, db_out, db_in = own
    spread = jnp.asarray(spread_matrix())
    pairs = jnp.einsum("at,hab,bs->tsh", spread, rel_sum[:, :TOK, :TOK], spread, precision=HIGHEST)
    table = jnp.dot(onehot.T, pairs.reshape(WIN**4, -1), precision=HIGHEST)
    table = lax.psum(table, ("fsdp", "win"))
    back_to_images = lambda v: swap_rows(v, top).reshape(rows, cols, imgs, d).transpose(2, 0, 1, 3)
    return (
        back_to_images(tall(out)), back_to_images(gin), dg1, db1, dwq, dqb, dvb, dwp, dbp, dg2, db2, dw1, db_in, dw2,
        db_out, table,
    )


def solution(mesh):
    vec, mat, img = P("fsdp"), P("fsdp", None), P("fsdp", "win", None, None)
    in_specs = (
        img, vec, vec, mat, vec, vec, mat, vec, vec, vec, mat, vec, mat, vec, P(), P("win", None, None), P(), img,
    )
    out_specs = (img, img, vec, vec, mat, vec, vec, mat, vec, vec, vec, mat, vec, mat, vec, P())
    return jax.shard_map(per_device, mesh=mesh, in_specs=in_specs, out_specs=out_specs, check_vma=False)
```

```python
import functools
import jax
import jax.numpy as jnp
import numpy as np
from jax import lax
from jax.experimental import pallas as pl
from jax.experimental.pallas import tpu as pltpu
from jax.sharding import PartitionSpec as P

HEADS = 16
HD = 32
WIN = 7
SHIFT = 3
TOK = 98
TOP = 42
PAD = 112
LANES = 128
GROUPS = 4
NB = 8
EPS = 1e-05
FAR = -1e30
F32 = jnp.float32
BF = jnp.bfloat16
HIGHEST = lax.Precision.HIGHEST


def mm(a, b):
    return lax.dot_general(a, b, (((1,), (0,)), ((), ())), preferred_element_type=F32)


def mm_nt(a, b):
    return lax.dot_general(a, b, (((1,), (1,)), ((), ())), preferred_element_type=F32)


def mm_tn(a, b):
    return lax.dot_general(a, b, (((0,), (0,)), ((), ())), preferred_element_type=F32)


def normalized(x):
    mean = jnp.mean(x, axis=-1, keepdims=True)
    c = x - mean
    var = jnp.mean(c * c, axis=-1, keepdims=True)
    r = lax.rsqrt(var + EPS)
    return c * r, r


def norm_back(u, n, r):
    return r * (u - jnp.mean(u, axis=-1, keepdims=True) - n * jnp.mean(u * n, axis=-1, keepdims=True))


def col_sum(v):
    return jnp.sum(v, axis=0, keepdims=True)


def erf(x):
    x = jnp.clip(x, -3.7439211627767994, 3.7439211627767994)
    s = x * x
    a = (0.00022905065861350646, 0.0034082910107109506, 0.050955695062380861, 0.18520832239976145, 1.128379143519084)
    b = (-1.1791602954361697e-7, 0.000023547966471313185, 0.0010179625278914885, 0.014070470171167667, 0.11098505178285362, 0.49746925110067538, 1.0)
    p = a[0]
    for c in a[1:]:
        p = p * s + c
    q = b[0]
    for c in b[1:]:
        q = q * s + c
    return x * p / q


def head_masks():
    lane = lax.broadcasted_iota(jnp.int32, (1, LANES), 1) // HD
    return [(lane == h).astype(BF) for h in range(GROUPS)]


def shifted_rows(x_ref, halo_ref):
    x = jnp.concatenate([halo_ref[...], x_ref[TOP:]], axis=0)
    return x.astype(F32).reshape(x.shape[0] * NB, x.shape[-1])


def own_lanes(stack):
    lane = lax.broadcasted_iota(jnp.int32, (1, LANES), 1) // HD
    out = stack[:PAD]
    for h in range(1, GROUPS):
        out = jnp.where(lane == h, stack[h * PAD : (h + 1) * PAD], out)
    return out


def attend_kernel(x_ref, halo_ref, vec_ref, w_ref, rel_ref, qkv_ref, att_ref, prob_ref, wide, joined):
    d = x_ref.shape[-1]
    n, _ = normalized(shifted_rows(x_ref, halo_ref))
    normed = (n * vec_ref[0:1] + vec_ref[1:2]).astype(BF)
    lanes3 = 3 * d // LANES
    chunk = d
    biases = (vec_ref[2:3], None, vec_ref[3:4])

    @pl.when(pl.program_id(0) == 0)
    def _():
        wide[:, TOK * NB :, :] = jnp.zeros((lanes3, (PAD - TOK) * NB, LANES), F32)

    for c in range(3 * d // chunk):
        part = mm(normed, w_ref[:, c * chunk : (c + 1) * chunk])
        if biases[c] is not None:
            part = part + biases[c]
        for k in range(chunk // LANES):
            wide[c * (chunk // LANES) + k, : TOK * NB, :] = part[:, k * LANES : (k + 1) * LANES]
    masks = head_masks()
    per = d // LANES
    scale = HD ** (-0.5)

    def one(i, carry):
        for g in range(per):
            q = wide[g, pl.ds(i, PAD, stride=NB), :].astype(BF)
            k = wide[per + g, pl.ds(i, PAD, stride=NB), :].astype(BF)
            v = wide[2 * per + g, pl.ds(i, PAD, stride=NB), :].astype(BF)
            qkv_ref[i, g] = q
            qkv_ref[i, per + g] = k
            qkv_ref[i, 2 * per + g] = v
            scores = mm_nt(jnp.concatenate([k * m for m in masks], axis=0), q)
            v_t = v.T
            heads = []
            for h in range(GROUPS):
                s = scores[h * PAD : (h + 1) * PAD] * scale + rel_ref[g * GROUPS + h][:, :PAD]
                e = jnp.exp(s - jnp.max(s, axis=0, keepdims=True))
                p = (e * (1.0 / jnp.sum(e, axis=0, keepdims=True))).astype(BF)
                prob_ref[i, g * GROUPS + h] = p
                heads.append(mm(v_t[h * HD : (h + 1) * HD], p))
            joined[g, pl.ds(i, PAD, stride=NB), :] = jnp.concatenate(heads, axis=0).T
        return carry

    lax.fori_loop(0, NB, one, 0)
    for g in range(per):
        att_ref[:, :, g * LANES : (g + 1) * LANES] = joined[g, : TOK * NB, :].astype(BF).reshape(TOK, NB, LANES)


def attend(x, halo, vecs, w, rel):
    _, imgs, d = x.shape
    full = lambda *shape: pl.BlockSpec(shape, lambda i: (0,) * len(shape), pipeline_mode=pl.Buffered(1))
    per = d // LANES
    return pl.pallas_call(
        attend_kernel,
        grid=(imgs // NB,),
        in_specs=[
            pl.BlockSpec((TOK, NB, d), lambda i: (0, i, 0)),
            pl.BlockSpec((TOP, NB, d), lambda i: (0, i, 0)),
            full(8, d), full(d, 3 * d), full(HEADS, PAD, LANES),
        ],
        out_specs=[
            pl.BlockSpec((NB, 3 * per, PAD, LANES), lambda i: (i, 0, 0, 0)),
            pl.BlockSpec((TOK, NB, d), lambda i: (0, i, 0)),
            pl.BlockSpec((NB, HEADS, PAD, PAD), lambda i: (i, 0, 0, 0)),
        ],
        out_shape=[
            jax.ShapeDtypeStruct((imgs, 3 * per, PAD, LANES), BF),
            jax.ShapeDtypeStruct((TOK, imgs, d), BF),
            jax.ShapeDtypeStruct((imgs, HEADS, PAD, PAD), BF),
        ],
        scratch_shapes=[
            pltpu.VMEM((3 * per, PAD * NB, LANES), F32),
            pltpu.VMEM((per, PAD * NB, LANES), F32),
        ],
        compiler_params=pltpu.CompilerParams(vmem_limit_bytes=60 << 20),
        name="attend",
    )(x, halo, vecs, w, rel)


def mlp_kernel(tops, x_ref, halo_ref, att_ref, ct_ref, ct_halo_ref, wp_ref, vec_ref, w1_ref, b1_ref, w2_ref,
               top_ref, rest_ref, gm_ref, gatt_ref, dwp_ref, dw1_ref, dw2_ref, db1_ref, small_ref,
               awp, aw1, aw2, ab1, asm):
    step = pl.program_id(0)
    d = x_ref.shape[-1]
    ff = w1_ref.shape[-1]
    chunk = 512

    @pl.when(step == 0)
    def _():
        awp[...] = jnp.zeros_like(awp)
        aw1[...] = jnp.zeros_like(aw1)
        aw2[...] = jnp.zeros_like(aw2)
        ab1[...] = jnp.zeros_like(ab1)
        asm[...] = jnp.zeros_like(asm)

    att = att_ref[...]
    above = step < tops
    gb = jnp.where(above, ct_halo_ref[...], ct_ref[...])
    grad_out = gb.astype(F32)
    middle = jnp.where(above, halo_ref[...], x_ref[...]).astype(F32) + mm(att, wp_ref[...]) + vec_ref[4:5]
    n, r = normalized(middle)
    normed = (n * vec_ref[5:6] + vec_ref[6:7]).astype(BF)
    normed_t = normed.T
    gb_t = gb.T
    out = middle + vec_ref[7:8]
    m = None
    for c in range(ff // chunk):
        at = slice(c * chunk, (c + 1) * chunk)
        hidden = mm(normed, w1_ref[:, at]) + b1_ref[:, at]
        cdf = 0.5 * (1.0 + erf(hidden * 0.7071067811865476))
        slope = cdf + hidden * (0.3989422804014327 * jnp.exp(-0.5 * hidden * hidden))
        active = (hidden * cdf).astype(BF)
        out = out + mm(active, w2_ref[at, :])
        gh = mm_nt(gb, w2_ref[at, :]) * slope
        ghb = gh.astype(BF)
        ab1[:, at] += col_sum(ghb.astype(F32))
        aw2[:, at] += mm(gb_t, active)
        aw1[:, at] += mm(normed_t, ghb)
        part = mm_nt(ghb, w1_ref[:, at])
        m = part if m is None else m + part

    @pl.when(above)
    def _():
        top_ref[...] = out.astype(BF)

    @pl.when(jnp.logical_not(above))
    def _():
        rest_ref[...] = out.astype(BF)

    grad_middle = grad_out + norm_back(m * vec_ref[5:6], n, r)
    gm_ref[...] = grad_middle
    gp = grad_middle.astype(BF)
    gatt_ref[...] = mm_nt(gp, wp_ref[...]).astype(BF)
    awp[...] += mm_tn(att, gp)
    asm[0:1, :] += col_sum(m * n)
    asm[1:2, :] += col_sum(m)
    asm[2:3, :] += col_sum(gp.astype(F32))
    asm[3:4, :] += col_sum(grad_out)

    @pl.when(step == pl.num_programs(0) - 1)
    def _():
        dwp_ref[...] = awp[...].astype(BF)
        dw1_ref[...] = aw1[...].astype(BF)
        for c in range(ff // chunk):
            at = slice(c * chunk, (c + 1) * chunk)
            dw2_ref[at, :] = aw2[:, at].T.astype(BF)
        db1_ref[...] = ab1[...]
        small_ref[...] = asm[...]


def mlp(x, halo, att, ct, ct_halo, wp, vecs, w1, b1, w2):
    rows, d = x.shape
    tile = halo.shape[0] // 3
    tops = 3
    ff = w1.shape[-1]
    full = lambda *shape: pl.BlockSpec(shape, lambda i: (0,) * len(shape), pipeline_mode=pl.Buffered(1))
    row = pl.BlockSpec((tile, d), lambda i: (i, 0))
    own = pl.BlockSpec((tile, d), lambda i: (jnp.maximum(i, tops), 0))
    top = pl.BlockSpec((tile, d), lambda i: (jnp.minimum(i, tops - 1), 0))
    rest = pl.BlockSpec((tile, d), lambda i: (jnp.maximum(i - tops, 0), 0))
    return pl.pallas_call(
        functools.partial(mlp_kernel, tops),
        grid=(rows // tile,),
        in_specs=[own, top, row, own, top, full(d, d), full(8, d), full(d, ff), full(1, ff), full(ff, d)],
        out_specs=[top, rest, row, row, full(d, d), full(d, ff), full(ff, d), full(1, ff), full(8, d)],
        out_shape=[
            jax.ShapeDtypeStruct((tops * tile, d), BF),
            jax.ShapeDtypeStruct((rows - tops * tile, d), BF),
            jax.ShapeDtypeStruct((rows, d), F32),
            jax.ShapeDtypeStruct((rows, d), BF),
            jax.ShapeDtypeStruct((d, d), BF),
            jax.ShapeDtypeStruct((d, ff), BF),
            jax.ShapeDtypeStruct((ff, d), BF),
            jax.ShapeDtypeStruct((1, ff), F32),
            jax.ShapeDtypeStruct((8, d), F32),
        ],
        scratch_shapes=[
            pltpu.VMEM((d, d), F32), pltpu.VMEM((d, ff), F32), pltpu.VMEM((d, ff), F32),
            pltpu.VMEM((1, ff), F32), pltpu.VMEM((8, d), F32),
        ],
        compiler_params=pltpu.CompilerParams(vmem_limit_bytes=60 << 20),
        name="mlp",
    )(x, halo, att, ct, ct_halo, wp, vecs, w1, b1, w2)


def back_kernel(x_ref, halo_ref, gm_ref, gatt_ref, qkv_ref, prob_ref, vec_ref, w_ref,
                top_ref, rest_ref, dw_ref, small_ref, bsum_ref, rel_ref, wide, grads, aw, asm, abs_):
    step = pl.program_id(0)
    d = x_ref.shape[-1]
    per = d // LANES
    scale = HD ** (-0.5)

    @pl.when(step == 0)
    def _():
        aw[...] = jnp.zeros_like(aw)
        asm[...] = jnp.zeros_like(asm)
        abs_[...] = jnp.zeros_like(abs_)
        rel_ref[...] = jnp.zeros_like(rel_ref)
        wide[:, TOK * NB :, :] = jnp.zeros((per, (PAD - TOK) * NB, LANES), F32)

    for g in range(per):
        wide[g, : TOK * NB, :] = gatt_ref[:, :, g * LANES : (g + 1) * LANES].astype(F32).reshape(TOK * NB, LANES)
    masks = head_masks()

    def one(i, carry):
        for g in range(per):
            ga = wide[g, pl.ds(i, PAD, stride=NB), :].astype(BF)
            q = qkv_ref[i, g]
            k = qkv_ref[i, per + g]
            v = qkv_ref[i, 2 * per + g]
            dps = mm_nt(jnp.concatenate([v * m for m in masks], axis=0), ga)
            k_t = k.T
            probs, marks, dq = [], [], []
            for h in range(GROUPS):
                p = prob_ref[i, g * GROUPS + h]
                pf = p.astype(F32)
                dp = dps[h * PAD : (h + 1) * PAD]
                ds = (pf * (dp - jnp.sum(pf * dp, axis=0, keepdims=True))).astype(BF)
                rel_ref[g * GROUPS + h] += ds.astype(F32)
                dq.append(mm(k_t[h * HD : (h + 1) * HD], ds))
                probs.append(p)
                marks.append(ds)
            dv = own_lanes(mm(jnp.concatenate(probs, axis=0), ga))
            dk = own_lanes(mm(jnp.concatenate(marks, axis=0), q))
            grads[g, pl.ds(i, PAD, stride=NB), :] = jnp.concatenate(dq, axis=0).T * scale
            grads[per + g, pl.ds(i, PAD, stride=NB), :] = dk * scale
            grads[2 * per + g, pl.ds(i, PAD, stride=NB), :] = dv
        return carry

    lax.fori_loop(0, NB, one, 0)
    n, r = normalized(shifted_rows(x_ref, halo_ref))
    normed = (n * vec_ref[0:1] + vec_ref[1:2]).astype(BF)
    normed_t = normed.T
    dn = None
    for c in range(3):
        at = slice(c * d, (c + 1) * d)
        dqkv = jnp.concatenate([grads[c * per + g, : TOK * NB, :].astype(BF) for g in range(per)], axis=-1)
        abs_[:, at] += col_sum(dqkv.astype(F32))
        aw[:, at] += mm(normed_t, dqkv)
        part = mm_nt(dqkv, w_ref[:, at])
        dn = part if dn is None else dn + part
    dn = dn.astype(BF).astype(F32)
    asm[0:1, :] += col_sum(dn * n)
    asm[1:2, :] += col_sum(dn)
    gin = gm_ref[...].reshape(TOK * NB, d) + norm_back(dn * vec_ref[0:1], n, r)
    gin = gin.reshape(TOK, NB, d)
    top_ref[...] = gin[:TOP]
    rest_ref[...] = gin[TOP:]

    @pl.when(step == pl.num_programs(0) - 1)
    def _():
        dw_ref[...] = aw[...].astype(BF)
        small_ref[...] = asm[...]
        bsum_ref[...] = abs_[...]


def back(x, halo, gm, gatt, qkv, prob, vecs, w):
    _, imgs, d = x.shape
    per = d // LANES
    full = lambda *shape: pl.BlockSpec(shape, lambda i: (0,) * len(shape), pipeline_mode=pl.Buffered(1))
    tok = pl.BlockSpec((TOK, NB, d), lambda i: (0, i, 0))
    return pl.pallas_call(
        back_kernel,
        grid=(imgs // NB,),
        in_specs=[
            tok, pl.BlockSpec((TOP, NB, d), lambda i: (0, i, 0)), tok, tok,
            pl.BlockSpec((NB, 3 * per, PAD, LANES), lambda i: (i, 0, 0, 0)),
            pl.BlockSpec((NB, HEADS, PAD, PAD), lambda i: (i, 0, 0, 0)),
            full(8, d), full(d, 3 * d),
        ],
        out_specs=[pl.BlockSpec((TOP, NB, d), lambda i: (0, i, 0)), pl.BlockSpec((TOK - TOP, NB, d), lambda i: (0, i, 0)), full(d, 3 * d), full(8, d), full(1, 3 * d), full(HEADS, PAD, PAD)],
        out_shape=[
            jax.ShapeDtypeStruct((TOP, imgs, d), F32),
            jax.ShapeDtypeStruct((TOK - TOP, imgs, d), F32),
            jax.ShapeDtypeStruct((d, 3 * d), BF),
            jax.ShapeDtypeStruct((8, d), F32),
            jax.ShapeDtypeStruct((1, 3 * d), F32),
            jax.ShapeDtypeStruct((HEADS, PAD, PAD), F32),
        ],
        scratch_shapes=[
            pltpu.VMEM((per, PAD * NB, LANES), F32),
            pltpu.VMEM((3 * per, PAD * NB, LANES), F32),
            pltpu.VMEM((d, 3 * d), F32),
            pltpu.VMEM((8, d), F32),
            pltpu.VMEM((1, 3 * d), F32),
        ],
        compiler_params=pltpu.CompilerParams(vmem_limit_bytes=60 << 20),
        name="back",
    )(x, halo, gm, gatt, qkv, prob, vecs, w)


DEEP = 4


class Place:
    def __init__(self, inner):
        self.inner = inner
        me, core = lax.axis_index("fsdp"), lax.axis_index("win")
        self.core, self.mate = core, 1 - core
        self.z = me // (inner * inner)
        u, v = (me // inner) % inner, me % inner
        self.a = u * (1 - core) + v * core
        self.b = v * (1 - core) + u * core
        self.step_a = inner * (1 - core) + core
        self.step_b = inner * core + 1 - core

    def at(self, dz=0, da=0, db=0):
        z = (self.z + dz) % DEEP
        a = (self.a + da) % self.inner
        b = (self.b + db) % self.inner
        return z * self.inner * self.inner + a * self.step_a + b * self.step_b

    def device(self, dz=0, da=0, db=0):
        return (self.at(dz, da, db), self.core)

    def partner(self):
        return (self.at(), self.mate)

    def peers(self):
        near = [self.device(dz=d) for d in range(1, DEEP)]
        near += [self.device(da=d) for d in range(1, self.inner)]
        near += [self.device(db=d) for d in range(1, self.inner)]
        return near + [self.partner()]


def meet(place):
    barrier = pltpu.get_barrier_semaphore()
    peers = place.peers()
    for peer in peers:
        pl.semaphore_signal(barrier, inc=1, device_id=peer, device_id_type=pl.DeviceIdType.MESH)
    pl.semaphore_wait(barrier, len(peers))


def remote(src, dst, send_sem, recv_sem, device):
    return pltpu.make_async_remote_copy(
        src_ref=src, dst_ref=dst, send_sem=send_sem, recv_sem=recv_sem, device_id=device,
        device_id_type=pl.DeviceIdType.MESH,
    )


def gather_kernel(inner, kinds, fields, *refs):
    ins, maps = refs[:kinds], refs[kinds : kinds + fields]
    outs, halos = refs[kinds + fields : 2 * kinds + fields], refs[2 * kinds + fields : 2 * (kinds + fields)]
    send_sem, recv_sem, own_sem, halo_sem = refs[2 * (kinds + fields) :]
    place = Place(inner)
    meet(place)

    def piece(k, block, core):
        half = outs[k].shape[-1] // 2
        return outs[k].at[block, :, pl.ds(pl.multiple_of(core * half, LANES), half)]

    def mine(k):
        half = outs[k].shape[-1] // 2
        return ins[k].at[:, pl.ds(pl.multiple_of(place.core * half, LANES), half)]

    sent = [[] for _ in range(kinds)]

    def send(k, src, block, device):
        copy = remote(src, piece(k, block, place.core), send_sem.at[k, len(sent[k])],
                      recv_sem.at[k, place.core, block], device)
        copy.start()
        sent[k].append(copy)

    def arrive(k, core, block):
        at = piece(k, block, core)
        remote(at, at, send_sem.at[k, 0], recv_sem.at[k, core, block], place.partner()).wait_recv()

    steps = range(1, inner)
    order_z = (1, 3, 2)
    own = []
    for k in range(kinds):
        for d in order_z:
            send(k, mine(k), place.at(), place.device(dz=d))
        for d in steps:
            send(k, mine(k), place.at(), place.device(da=d))
        for d in steps:
            send(k, mine(k), place.at(), place.device(db=d))
    swaps = [remote(maps[f].at[:TOP], halos[f], halo_sem.at[f, 0], halo_sem.at[f, 1], place.partner())
             for f in range(fields)]
    for copy in swaps:
        copy.start()
    for k in range(kinds):
        copy = pltpu.make_async_copy(ins[k], outs[k].at[place.at()], own_sem.at[k])
        copy.start()
        own.append(copy)

    def pass_on(k, block, along_a, along_b):
        arrive(k, place.core, block)
        src = piece(k, block, place.core)
        if along_a:
            for d in steps:
                send(k, src, block, place.device(da=d))
        if along_b:
            for d in steps:
                send(k, src, block, place.device(db=d))
        send(k, src, block, place.partner())

    for k in range(kinds):
        for dz in order_z:
            pass_on(k, place.at(dz=dz), True, True)
        for da in steps:
            for dz in (0,) + order_z:
                pass_on(k, place.at(dz=dz, da=da), False, True)
    for k in range(kinds):
        for db in steps:
            for da in range(inner):
                for dz in (0,) + order_z:
                    pass_on(k, place.at(dz=dz, da=da, db=db), False, False)
    for k in range(kinds):
        for db in range(inner):
            for da in range(inner):
                for dz in range(DEEP):
                    if db or da or dz:
                        arrive(k, place.mate, place.at(dz, da, db))
        own[k].wait()
        for copy in sent[k]:
            copy.wait_send()
    for copy in swaps:
        copy.wait()


def inner_of(owners):
    return int(round((owners // DEEP) ** 0.5))


def gathered(shards, maps):
    owners = lax.axis_size("fsdp")
    inner, kinds, fields = inner_of(owners), len(shards), len(maps)
    sends = (DEEP - 1) + 2 * (inner - 1) + 1 + (DEEP - 1) * (2 * inner - 1) + DEEP * (inner - 1) * inner + DEEP * inner * (inner - 1)
    anywhere = pl.BlockSpec(memory_space=pl.ANY)
    return pl.pallas_call(
        functools.partial(gather_kernel, inner, kinds, fields),
        in_specs=[anywhere] * (kinds + fields),
        out_specs=[anywhere] * (kinds + fields),
        out_shape=[jax.ShapeDtypeStruct((owners, *s.shape), s.dtype) for s in shards]
        + [jax.ShapeDtypeStruct((TOP, *m.shape[1:]), m.dtype) for m in maps],
        scratch_shapes=[
            pltpu.SemaphoreType.DMA((kinds, sends)),
            pltpu.SemaphoreType.DMA((kinds, 2, owners)),
            pltpu.SemaphoreType.DMA((kinds,)),
            pltpu.SemaphoreType.DMA((fields, 2)),
        ],
        compiler_params=pltpu.CompilerParams(collective_id=0, has_side_effects=True),
        name="gather",
    )(*shards, *maps)


def deliver_kernel(inner, kinds, *refs):
    ins, table_ref, outs, sum_ref = refs[:kinds], refs[kinds], refs[kinds + 1 : 2 * kinds + 1], refs[2 * kinds + 1]
    at = 2 * kinds + 2
    own, from_mate, from_b, from_a, from_z, final = (refs[at + i * kinds : at + (i + 1) * kinds] for i in range(6))
    load_sem, mate_sem, b_sem, a_sem, z_sem, end_sem, parts, part_sem = refs[at + 6 * kinds :]
    owners = DEEP * inner * inner
    place = Place(inner)
    steps = range(1, inner)
    meet(place)

    def columns(k, core):
        half = outs[k].shape[-1] // 2
        return pl.ds(pl.multiple_of(core * half, LANES), half)

    def table_stage(stage, value, count, mine, peer):
        parts[stage, mine] = value
        copies = [remote(parts.at[stage, mine], parts.at[stage, mine], part_sem.at[stage, 0, d],
                         part_sem.at[stage, 1, d], peer(d)) for d in range(1, count)]
        for copy in copies:
            copy.start()
        return copies, stage, count

    def table_sum(begun):
        copies, stage, count = begun
        for copy in copies:
            copy.wait()
        total = parts[stage, 0]
        for i in range(1, count):
            total = total + parts[stage, i]
        return total

    u = place.a * (1 - place.core) + place.b * place.core
    v = place.b * (1 - place.core) + place.a * place.core
    along_u = lambda d: (place.at(da=d * (1 - place.core), db=d * place.core), place.core)
    along_v = lambda d: (place.at(da=d * place.core, db=d * (1 - place.core)), place.core)
    begun = table_stage(0, table_ref[...], 2, place.core, lambda d: place.partner())

    loads, swaps = [], []
    for k in range(kinds):
        swap = remote(ins[k].at[:, :, columns(k, place.mate)], from_mate[k], mate_sem.at[k, 0], mate_sem.at[k, 1],
                      place.partner())
        swap.start()
        load = pltpu.make_async_copy(ins[k].at[:, :, columns(k, place.core)], own[k], load_sem.at[k])
        load.start()
        swaps.append(swap)
        loads.append(load)

    sent = []

    def add(k, block, other):
        own[k][block] = (own[k][block].astype(F32) + other[...].astype(F32)).astype(BF)

    for k in range(kinds):
        loads[k].wait()
        swaps[k].wait()
        for db in tuple(steps) + (0,):
            for da in range(inner):
                for dz in range(DEEP):
                    block = place.at(dz, da, db)
                    add(k, block, from_mate[k].at[block])
                    if db:
                        slot = (db - 1) * inner * DEEP + da * DEEP + dz
                        copy = remote(own[k].at[block], from_b[k].at[slot], b_sem.at[k, 0, slot],
                                      b_sem.at[k, 1, slot], place.device(db=db))
                        copy.start()
                        sent.append((k, copy))
    begun = table_stage(1, table_sum(begun), inner, u, along_u)
    arrivals_b = list(sent)
    sent = []
    for k in range(kinds):
        for kk, copy in arrivals_b:
            if kk == k:
                copy.wait()
        for da in tuple(steps) + (0,):
            for dz in range(DEEP):
                block = place.at(dz, da)
                for db in steps:
                    add(k, block, from_b[k].at[(db - 1) * inner * DEEP + da * DEEP + dz])
                if da:
                    slot = (da - 1) * DEEP + dz
                    copy = remote(own[k].at[block], from_a[k].at[slot], a_sem.at[k, 0, slot], a_sem.at[k, 1, slot],
                                  place.device(da=da))
                    copy.start()
                    sent.append((k, copy))
    begun = table_stage(2, table_sum(begun), inner, v, along_v)
    arrivals_a = list(sent)
    sent = []
    for k in range(kinds):
        for kk, copy in arrivals_a:
            if kk == k:
                copy.wait()
        for dz in (2, 1, 3, 0):
            block = place.at(dz)
            for da in steps:
                add(k, block, from_a[k].at[(da - 1) * DEEP + dz])
            if dz:
                copy = remote(own[k].at[block], from_z[k].at[dz - 1], z_sem.at[k, 0, dz - 1], z_sem.at[k, 1, dz - 1],
                              place.device(dz=dz))
                copy.start()
                sent.append((k, copy))
    begun = table_stage(3, table_sum(begun), DEEP, place.z, lambda d: place.device(dz=d))
    ends = []
    for k in range(kinds):
        for kk, copy in sent:
            if kk == k:
                copy.wait()
        total = own[k][place.at()].astype(F32)
        for dz in range(1, DEEP):
            total = total + from_z[k][dz - 1].astype(F32)
        final[k][...] = total
        there = outs[k].at[:, columns(k, place.core)]
        far = remote(final[k], there, end_sem.at[k, 0], end_sem.at[k, 1], place.partner())
        near = pltpu.make_async_copy(final[k], there, end_sem.at[k, 2])
        far.start()
        near.start()
        ends += [far, near]
    sum_ref[...] = table_sum(begun)
    for copy in ends:
        copy.wait()


def delivered(grads, table):
    owners = lax.axis_size("fsdp")
    inner, kinds = inner_of(owners), len(grads)
    anywhere = pl.BlockSpec(memory_space=pl.ANY)
    halves = [(g.shape[1], g.shape[2] // 2) for g in grads]

    def room(count, dtype=BF):
        return [pltpu.VMEM((count, *h), dtype) for h in halves]

    dma = pltpu.SemaphoreType.DMA
    return pl.pallas_call(
        functools.partial(deliver_kernel, inner, kinds),
        in_specs=[anywhere] * kinds + [pl.BlockSpec(memory_space=pltpu.VMEM)],
        out_specs=[anywhere] * kinds + [pl.BlockSpec(memory_space=pltpu.VMEM)],
        out_shape=[jax.ShapeDtypeStruct(g.shape[1:], F32) for g in grads]
        + [jax.ShapeDtypeStruct(table.shape, F32)],
        scratch_shapes=[
            *room(owners), *room(owners), *room((inner - 1) * inner * DEEP), *room((inner - 1) * DEEP),
            *room(DEEP - 1), *[pltpu.VMEM(h, F32) for h in halves],
            dma((kinds,)), dma((kinds, 2)), dma((kinds, 2, (inner - 1) * inner * DEEP)),
            dma((kinds, 2, (inner - 1) * DEEP)), dma((kinds, 2, DEEP - 1)), dma((kinds, 3)),
            pltpu.VMEM((4, DEEP, *table.shape), F32), dma((4, 2, DEEP)),
        ],
        compiler_params=pltpu.CompilerParams(collective_id=1, has_side_effects=True, vmem_limit_bytes=60 << 20),
        name="deliver",
    )(*grads, table)


def window_of_tokens():
    row, col = np.arange(TOK) // (2 * WIN), np.arange(TOK) % (2 * WIN)
    row, col = (row - SHIFT) % WIN, (col - SHIFT) % (2 * WIN)
    return col // WIN, row * WIN + col % WIN


def spread_matrix():
    _, place = window_of_tokens()
    return (place[:, None] == np.arange(WIN * WIN)[None, :]).astype(np.float32)


def relative_parts(rel_index, table):
    count = WIN * WIN
    onehot = (rel_index.reshape(count * count, 1) == jnp.arange(table.shape[0], dtype=jnp.int32)[None, :]).astype(F32)
    relative = jnp.dot(onehot, table, precision=HIGHEST).reshape(count, count, -1).transpose(2, 0, 1)
    return onehot, relative


def bias_of_pairs(relative, regions):
    side, place = window_of_tokens()
    spread = jnp.asarray(spread_matrix())
    wide = jnp.einsum("at,hts,bs->hba", spread, relative, spread, precision=HIGHEST)
    region = regions.reshape(2, WIN * WIN)
    region = jnp.concatenate(
        [jnp.roll(region[s].reshape(WIN, WIN), SHIFT, axis=0)[:, c] for s, c in ((1, slice(4, 7)), (0, slice(0, 7)), (1, slice(0, 4)))],
        axis=1,
    ).reshape(TOK)
    mask = jnp.where(region[:, None] == region[None, :], 0.0, -100.0)
    same = jnp.asarray(side[:, None] == side[None, :])
    bias = jnp.where(same[None], wide + mask[None], FAR)
    return jnp.pad(
        jnp.pad(bias, ((0, 0), (0, PAD - TOK), (0, 0)), constant_values=FAR),
        ((0, 0), (0, 0), (0, LANES - TOK)),
    )


def packed_row(parts):
    row = jnp.concatenate(parts, axis=-1)
    return jnp.pad(row, [(0, 0)] * (row.ndim - 1) + [(0, -row.shape[-1] % (2 * LANES))])


def per_device(
    images, norm1_gain, norm1_bias, qkv_weight, q_bias, v_bias, proj_weight, proj_bias, norm2_gain, norm2_bias,
    fc1_weight, fc1_bias, fc2_weight, fc2_bias, bias_table, regions, rel_index, cotangent,
):
    imgs, rows, cols, d = images.shape
    owners = lax.axis_size("fsdp")
    x = images.transpose(1, 2, 0, 3).reshape(rows * cols, imgs, d)
    ct = cotangent.transpose(1, 2, 0, 3).reshape(rows * cols, imgs, d)
    vectors = (norm1_gain, norm1_bias, q_bias, v_bias, proj_bias, norm2_gain, norm2_bias, fc2_bias, fc1_bias)
    shards = (packed_row(vectors)[None], qkv_weight, proj_weight, fc1_weight, fc2_weight)
    packed, *mats, halo, ct_halo = gathered(shards, (x, ct))
    packed = packed[:, 0].astype(F32)
    part = d // owners
    vecs = packed[:, : 8 * part].reshape(owners, 8, part).transpose(1, 0, 2).reshape(8, d)
    b_in = packed[:, 8 * part : 8 * part + fc1_bias.shape[0]].reshape(1, -1)
    w_qkv, w_proj, w_in, w_out = (v.reshape(owners * v.shape[1], v.shape[2]) for v in mats)
    onehot, relative = relative_parts(rel_index, bias_table)
    rel = bias_of_pairs(relative, regions)

    qkv, att, prob = attend(x, halo, vecs, w_qkv, rel)
    flat = lambda v: v.reshape(v.shape[0] * imgs, d)
    tall = lambda v: v.reshape(v.shape[0] // imgs, imgs, d)
    out_top, out_rest, gm, gatt, dwp, dw1, dw2, db_in, small2 = mlp(
        flat(x), flat(halo), flat(att), flat(ct), flat(ct_halo), w_proj, vecs, w_in, b_in, w_out
    )
    swapped = lambda v: lax.ppermute(v, "win", [(0, 1), (1, 0)])
    out_top = swapped(out_top)
    gin_top, gin_rest, dwq, small1, bsum, rel_sum = back(x, halo, tall(gm), tall(gatt), qkv, prob, vecs, w_qkv)
    gin_top = swapped(gin_top)
    spread = jnp.asarray(spread_matrix())
    pairs = jnp.einsum("at,hba,bs->tsh", spread, rel_sum[:, :TOK, :TOK], spread, precision=HIGHEST)
    table = jnp.dot(onehot.T, pairs.reshape(WIN**4, -1), precision=HIGHEST)
    flat_table = jnp.pad(table.reshape(-1), (0, -table.size % (8 * LANES))).reshape(-1, LANES)
    grads = (
        small1[0], small1[1], bsum[0, :d], bsum[0, 2 * d :], small2[2], small2[0], small2[1], small2[3], db_in[0],
    )
    row = packed_row([v.reshape(owners, 1, -1) for v in grads]).astype(BF)
    blocks = lambda v: v.reshape(owners, v.shape[0] // owners, v.shape[1])
    sums, dwp, dw1, dw2, dwq, table_sum = delivered(
        (row, blocks(dwp), blocks(dw1), blocks(dw2), blocks(dwq)), flat_table
    )
    at, own = 0, []
    for v in vectors:
        own.append(sums[0, at : at + v.shape[0]])
        at += v.shape[0]
    dg1, db1, dqb, dvb, dbp, dg2, db2, db_out, db_in = own
    table = table_sum.reshape(-1)[: table.size].reshape(table.shape)
    joined = lambda top, rest: jnp.concatenate([top, rest], axis=0).reshape(rows, cols, imgs, d).transpose(2, 0, 1, 3)
    return (
        joined(tall(out_top), tall(out_rest)), joined(gin_top, gin_rest), dg1, db1, dwq, dqb, dvb, dwp, dbp, dg2, db2, dw1, db_in, dw2,
        db_out, table,
    )


def solution(mesh):
    vec, mat, img = P("fsdp"), P("fsdp", None), P("fsdp", "win", None, None)
    in_specs = (
        img, vec, vec, mat, vec, vec, mat, vec, vec, vec, mat, vec, mat, vec, P(), P("win", None, None), P(), img,
    )
    out_specs = (img, img, vec, vec, mat, vec, vec, mat, vec, vec, vec, mat, vec, mat, vec, P())
    return jax.shard_map(per_device, mesh=mesh, in_specs=in_specs, out_specs=out_specs, check_vma=False)
```

```python
import functools
import jax
import jax.numpy as jnp
import numpy as np
from jax import lax
from jax.experimental import pallas as pl
from jax.experimental.pallas import tpu as pltpu
from jax.sharding import PartitionSpec as P

HEADS = 16
HD = 32
WIN = 7
SHIFT = 3
TOK = 98
TOP = 42
PAD = 112
LANES = 128
GROUPS = 4
NB = 8
EPS = 1e-05
FAR = -1e30
F32 = jnp.float32
BF = jnp.bfloat16
HIGHEST = lax.Precision.HIGHEST


def mm(a, b):
    return lax.dot_general(a, b, (((1,), (0,)), ((), ())), preferred_element_type=F32)


def mm_nt(a, b):
    return lax.dot_general(a, b, (((1,), (1,)), ((), ())), preferred_element_type=F32)


def mm_tn(a, b):
    return lax.dot_general(a, b, (((0,), (0,)), ((), ())), preferred_element_type=F32)


def normalized(x):
    mean = jnp.mean(x, axis=-1, keepdims=True)
    c = x - mean
    var = jnp.mean(c * c, axis=-1, keepdims=True)
    r = lax.rsqrt(var + EPS)
    return c * r, r


def norm_back(u, n, r):
    return r * (u - jnp.mean(u, axis=-1, keepdims=True) - n * jnp.mean(u * n, axis=-1, keepdims=True))


def col_sum(v):
    return jnp.sum(v, axis=0, keepdims=True)


def erf(x):
    x = jnp.clip(x, -3.7439211627767994, 3.7439211627767994)
    s = x * x
    a = (0.00022905065861350646, 0.0034082910107109506, 0.050955695062380861, 0.18520832239976145, 1.128379143519084)
    b = (-1.1791602954361697e-7, 0.000023547966471313185, 0.0010179625278914885, 0.014070470171167667, 0.11098505178285362, 0.49746925110067538, 1.0)
    p = a[0]
    for c in a[1:]:
        p = p * s + c
    q = b[0]
    for c in b[1:]:
        q = q * s + c
    return x * p / q


def head_masks():
    lane = lax.broadcasted_iota(jnp.int32, (1, LANES), 1) // HD
    return [(lane == h).astype(BF) for h in range(GROUPS)]


def shifted_rows(x_ref, halo_ref):
    x = jnp.concatenate([halo_ref[...], x_ref[TOP:]], axis=0)
    return x.astype(F32).reshape(x.shape[0] * NB, x.shape[-1])


def own_lanes(stack):
    lane = lax.broadcasted_iota(jnp.int32, (1, LANES), 1) // HD
    out = stack[:PAD]
    for h in range(1, GROUPS):
        out = jnp.where(lane == h, stack[h * PAD : (h + 1) * PAD], out)
    return out


def at_step(step, action):
    @pl.when(pl.program_id(0) == step)
    def _():
        action()


def attend_kernel(inner, kinds, fields, x_ref, halo_ref, vec_ref, w_ref, rel_ref, *refs):
    ins, maps = refs[:kinds], refs[kinds : kinds + fields]
    qkv_ref, att_ref, prob_ref = refs[kinds + fields : kinds + fields + 3]
    outs, halos = refs[kinds + fields + 3 : 2 * kinds + fields + 3], refs[2 * kinds + fields + 3 : 2 * (kinds + fields) + 3]
    wide, joined, *sems = refs[2 * (kinds + fields) + 3 :]
    moves = Spread(inner, ins, maps, outs, halos, *sems)

    def begin():
        meet(Place(inner))
        moves.run(0)

    at_step(0, begin)
    for stage in (1, 2, 3):
        at_step(stage, functools.partial(moves.run, stage))
    d = x_ref.shape[-1]
    n, _ = normalized(shifted_rows(x_ref, halo_ref))
    normed = (n * vec_ref[0:1] + vec_ref[1:2]).astype(BF)
    lanes3 = 3 * d // LANES
    chunk = d
    biases = (vec_ref[2:3], None, vec_ref[3:4])

    @pl.when(pl.program_id(0) == 0)
    def _():
        wide[:, TOK * NB :, :] = jnp.zeros((lanes3, (PAD - TOK) * NB, LANES), F32)

    for c in range(3 * d // chunk):
        part = mm(normed, w_ref[:, c * chunk : (c + 1) * chunk])
        if biases[c] is not None:
            part = part + biases[c]
        for k in range(chunk // LANES):
            wide[c * (chunk // LANES) + k, : TOK * NB, :] = part[:, k * LANES : (k + 1) * LANES]
    masks = head_masks()
    per = d // LANES
    scale = HD ** (-0.5)

    def one(i, carry):
        for g in range(per):
            q = wide[g, pl.ds(i, PAD, stride=NB), :].astype(BF)
            k = wide[per + g, pl.ds(i, PAD, stride=NB), :].astype(BF)
            v = wide[2 * per + g, pl.ds(i, PAD, stride=NB), :].astype(BF)
            qkv_ref[i, g] = q
            qkv_ref[i, per + g] = k
            qkv_ref[i, 2 * per + g] = v
            scores = mm_nt(jnp.concatenate([k * m for m in masks], axis=0), q)
            v_t = v.T
            heads = []
            for h in range(GROUPS):
                s = scores[h * PAD : (h + 1) * PAD] * scale + rel_ref[g * GROUPS + h][:, :PAD]
                e = jnp.exp(s - jnp.max(s, axis=0, keepdims=True))
                p = (e * (1.0 / jnp.sum(e, axis=0, keepdims=True))).astype(BF)
                prob_ref[i, g * GROUPS + h] = p
                heads.append(mm(v_t[h * HD : (h + 1) * HD], p))
            joined[g, pl.ds(i, PAD, stride=NB), :] = jnp.concatenate(heads, axis=0).T
        return carry

    lax.fori_loop(0, NB, one, 0)
    for g in range(per):
        att_ref[:, :, g * LANES : (g + 1) * LANES] = joined[g, : TOK * NB, :].astype(BF).reshape(TOK, NB, LANES)
    at_step(3, moves.finish)


def attend(x, halo, vecs, w, rel, shards, maps):
    _, imgs, d = x.shape
    owners = lax.axis_size("fsdp")
    inner, kinds, fields = inner_of(owners), len(shards), len(maps)
    anywhere = [pl.BlockSpec(memory_space=pl.ANY)] * (kinds + fields)
    full = lambda *shape: pl.BlockSpec(shape, lambda i: (0,) * len(shape), pipeline_mode=pl.Buffered(1))
    per = d // LANES
    return pl.pallas_call(
        functools.partial(attend_kernel, inner, kinds, fields),
        grid=(imgs // NB,),
        in_specs=[
            pl.BlockSpec((TOK, NB, d), lambda i: (0, i, 0)),
            pl.BlockSpec((TOP, NB, d), lambda i: (0, i, 0)),
            full(8, d), full(d, 3 * d), full(HEADS, PAD, LANES), *anywhere,
        ],
        out_specs=[
            pl.BlockSpec((NB, 3 * per, PAD, LANES), lambda i: (i, 0, 0, 0)),
            pl.BlockSpec((TOK, NB, d), lambda i: (0, i, 0)),
            pl.BlockSpec((NB, HEADS, PAD, PAD), lambda i: (i, 0, 0, 0)),
            *anywhere,
        ],
        out_shape=[
            jax.ShapeDtypeStruct((imgs, 3 * per, PAD, LANES), BF),
            jax.ShapeDtypeStruct((TOK, imgs, d), BF),
            jax.ShapeDtypeStruct((imgs, HEADS, PAD, PAD), BF),
            *spread_shapes(owners, shards, maps),
        ],
        scratch_shapes=[
            pltpu.VMEM((3 * per, PAD * NB, LANES), F32),
            pltpu.VMEM((per, PAD * NB, LANES), F32),
            *spread_scratch(owners, kinds, fields),
        ],
        compiler_params=pltpu.CompilerParams(collective_id=2, has_side_effects=True, vmem_limit_bytes=60 << 20),
        name="attend",
    )(x, halo, vecs, w, rel, *shards, *maps)


def mlp_kernel(tops, x_ref, halo_ref, att_ref, ct_ref, ct_halo_ref, wp_ref, vec_ref, w1_ref, b1_ref, w2_ref,
               top_ref, rest_ref, gm_ref, gatt_ref, dwp_ref, dw1_ref, dw2_ref, db1_ref, small_ref,
               awp, aw1, aw2, ab1, asm):
    step = pl.program_id(0)
    d = x_ref.shape[-1]
    ff = w1_ref.shape[-1]
    chunk = 512

    @pl.when(step == 0)
    def _():
        awp[...] = jnp.zeros_like(awp)
        aw1[...] = jnp.zeros_like(aw1)
        aw2[...] = jnp.zeros_like(aw2)
        ab1[...] = jnp.zeros_like(ab1)
        asm[...] = jnp.zeros_like(asm)

    att = att_ref[...]
    above = step < tops
    gb = jnp.where(above, ct_halo_ref[...], ct_ref[...])
    grad_out = gb.astype(F32)
    middle = jnp.where(above, halo_ref[...], x_ref[...]).astype(F32) + mm(att, wp_ref[...]) + vec_ref[4:5]
    n, r = normalized(middle)
    normed = (n * vec_ref[5:6] + vec_ref[6:7]).astype(BF)
    normed_t = normed.T
    gb_t = gb.T
    out = middle + vec_ref[7:8]
    m = None
    for c in range(ff // chunk):
        at = slice(c * chunk, (c + 1) * chunk)
        hidden = mm(normed, w1_ref[:, at]) + b1_ref[:, at]
        cdf = 0.5 * (1.0 + erf(hidden * 0.7071067811865476))
        slope = cdf + hidden * (0.3989422804014327 * jnp.exp(-0.5 * hidden * hidden))
        active = (hidden * cdf).astype(BF)
        out = out + mm(active, w2_ref[at, :])
        gh = mm_nt(gb, w2_ref[at, :]) * slope
        ghb = gh.astype(BF)
        ab1[:, at] += col_sum(ghb.astype(F32))
        aw2[:, at] += mm(gb_t, active)
        aw1[:, at] += mm(normed_t, ghb)
        part = mm_nt(ghb, w1_ref[:, at])
        m = part if m is None else m + part

    @pl.when(above)
    def _():
        top_ref[...] = out.astype(BF)

    @pl.when(jnp.logical_not(above))
    def _():
        rest_ref[...] = out.astype(BF)

    grad_middle = grad_out + norm_back(m * vec_ref[5:6], n, r)
    gm_ref[...] = grad_middle
    gp = grad_middle.astype(BF)
    gatt_ref[...] = mm_nt(gp, wp_ref[...]).astype(BF)
    awp[...] += mm_tn(att, gp)
    asm[0:1, :] += col_sum(m * n)
    asm[1:2, :] += col_sum(m)
    asm[2:3, :] += col_sum(gp.astype(F32))
    asm[3:4, :] += col_sum(grad_out)

    @pl.when(step == pl.num_programs(0) - 1)
    def _():
        dwp_ref[...] = awp[...].astype(BF)
        dw1_ref[...] = aw1[...].astype(BF)
        for c in range(ff // chunk):
            at = slice(c * chunk, (c + 1) * chunk)
            dw2_ref[at, :] = aw2[:, at].T.astype(BF)
        db1_ref[...] = ab1[...]
        small_ref[...] = asm[...]


def mlp(x, halo, att, ct, ct_halo, wp, vecs, w1, b1, w2):
    rows, d = x.shape
    tile = halo.shape[0] // 3
    tops = 3
    ff = w1.shape[-1]
    full = lambda *shape: pl.BlockSpec(shape, lambda i: (0,) * len(shape), pipeline_mode=pl.Buffered(1))
    row = pl.BlockSpec((tile, d), lambda i: (i, 0))
    own = pl.BlockSpec((tile, d), lambda i: (jnp.maximum(i, tops), 0))
    top = pl.BlockSpec((tile, d), lambda i: (jnp.minimum(i, tops - 1), 0))
    rest = pl.BlockSpec((tile, d), lambda i: (jnp.maximum(i - tops, 0), 0))
    return pl.pallas_call(
        functools.partial(mlp_kernel, tops),
        grid=(rows // tile,),
        in_specs=[own, top, row, own, top, full(d, d), full(8, d), full(d, ff), full(1, ff), full(ff, d)],
        out_specs=[top, rest, row, row, full(d, d), full(d, ff), full(ff, d), full(1, ff), full(8, d)],
        out_shape=[
            jax.ShapeDtypeStruct((tops * tile, d), BF),
            jax.ShapeDtypeStruct((rows - tops * tile, d), BF),
            jax.ShapeDtypeStruct((rows, d), F32),
            jax.ShapeDtypeStruct((rows, d), BF),
            jax.ShapeDtypeStruct((d, d), BF),
            jax.ShapeDtypeStruct((d, ff), BF),
            jax.ShapeDtypeStruct((ff, d), BF),
            jax.ShapeDtypeStruct((1, ff), F32),
            jax.ShapeDtypeStruct((8, d), F32),
        ],
        scratch_shapes=[
            pltpu.VMEM((d, d), F32), pltpu.VMEM((d, ff), F32), pltpu.VMEM((d, ff), F32),
            pltpu.VMEM((1, ff), F32), pltpu.VMEM((8, d), F32),
        ],
        compiler_params=pltpu.CompilerParams(vmem_limit_bytes=60 << 20),
        name="mlp",
    )(x, halo, att, ct, ct_halo, wp, vecs, w1, b1, w2)


def back_kernel(inner, kinds, x_ref, halo_ref, gm_ref, gatt_ref, qkv_ref, prob_ref, vec_ref, w_ref, *refs):
    ins, (top_ref, rest_ref, dw_ref, small_ref, bsum_ref, rel_ref) = refs[:kinds], refs[kinds : kinds + 6]
    outs, (wide, grads, aw, asm, abs_), room = refs[kinds + 6 : 2 * kinds + 6], refs[2 * kinds + 6 : 2 * kinds + 11], refs[2 * kinds + 11 :]
    moves = Delivery(inner, ins, outs, room)

    def begin():
        meet(Place(inner))
        moves.start()

    at_step(0, begin)
    at_step(1, moves.pass_b)
    at_step(2, moves.pass_a)
    at_step(3, moves.pass_z)
    step = pl.program_id(0)
    d = x_ref.shape[-1]
    per = d // LANES
    scale = HD ** (-0.5)

    @pl.when(step == 0)
    def _():
        aw[...] = jnp.zeros_like(aw)
        asm[...] = jnp.zeros_like(asm)
        abs_[...] = jnp.zeros_like(abs_)
        rel_ref[...] = jnp.zeros_like(rel_ref)
        wide[:, TOK * NB :, :] = jnp.zeros((per, (PAD - TOK) * NB, LANES), F32)

    for g in range(per):
        wide[g, : TOK * NB, :] = gatt_ref[:, :, g * LANES : (g + 1) * LANES].astype(F32).reshape(TOK * NB, LANES)
    masks = head_masks()

    def one(i, carry):
        for g in range(per):
            ga = wide[g, pl.ds(i, PAD, stride=NB), :].astype(BF)
            q = qkv_ref[i, g]
            k = qkv_ref[i, per + g]
            v = qkv_ref[i, 2 * per + g]
            dps = mm_nt(jnp.concatenate([v * m for m in masks], axis=0), ga)
            k_t = k.T
            probs, marks, dq = [], [], []
            for h in range(GROUPS):
                p = prob_ref[i, g * GROUPS + h]
                pf = p.astype(F32)
                dp = dps[h * PAD : (h + 1) * PAD]
                ds = (pf * (dp - jnp.sum(pf * dp, axis=0, keepdims=True))).astype(BF)
                rel_ref[g * GROUPS + h] += ds.astype(F32)
                dq.append(mm(k_t[h * HD : (h + 1) * HD], ds))
                probs.append(p)
                marks.append(ds)
            dv = own_lanes(mm(jnp.concatenate(probs, axis=0), ga))
            dk = own_lanes(mm(jnp.concatenate(marks, axis=0), q))
            grads[g, pl.ds(i, PAD, stride=NB), :] = jnp.concatenate(dq, axis=0).T * scale
            grads[per + g, pl.ds(i, PAD, stride=NB), :] = dk * scale
            grads[2 * per + g, pl.ds(i, PAD, stride=NB), :] = dv
        return carry

    lax.fori_loop(0, NB, one, 0)
    n, r = normalized(shifted_rows(x_ref, halo_ref))
    normed = (n * vec_ref[0:1] + vec_ref[1:2]).astype(BF)
    normed_t = normed.T
    dn = None
    for c in range(3):
        at = slice(c * d, (c + 1) * d)
        dqkv = jnp.concatenate([grads[c * per + g, : TOK * NB, :].astype(BF) for g in range(per)], axis=-1)
        abs_[:, at] += col_sum(dqkv.astype(F32))
        aw[:, at] += mm(normed_t, dqkv)
        part = mm_nt(dqkv, w_ref[:, at])
        dn = part if dn is None else dn + part
    dn = dn.astype(BF).astype(F32)
    asm[0:1, :] += col_sum(dn * n)
    asm[1:2, :] += col_sum(dn)
    gin = gm_ref[...].reshape(TOK * NB, d) + norm_back(dn * vec_ref[0:1], n, r)
    gin = gin.reshape(TOK, NB, d)
    top_ref[...] = gin[:TOP]
    rest_ref[...] = gin[TOP:]

    def end():
        moves.hand_over()
        moves.finish()

    at_step(3, end)

    @pl.when(step == pl.num_programs(0) - 1)
    def _():
        dw_ref[...] = aw[...].astype(BF)
        small_ref[...] = asm[...]
        bsum_ref[...] = abs_[...]


def back(x, halo, gm, gatt, qkv, prob, vecs, w, grads):
    _, imgs, d = x.shape
    owners, kinds = lax.axis_size("fsdp"), len(grads)
    anywhere = [pl.BlockSpec(memory_space=pl.ANY)] * kinds
    per = d // LANES
    full = lambda *shape: pl.BlockSpec(shape, lambda i: (0,) * len(shape), pipeline_mode=pl.Buffered(1))
    tok = pl.BlockSpec((TOK, NB, d), lambda i: (0, i, 0))
    return pl.pallas_call(
        functools.partial(back_kernel, inner_of(owners), kinds),
        grid=(imgs // NB,),
        in_specs=[
            tok, pl.BlockSpec((TOP, NB, d), lambda i: (0, i, 0)), tok, tok,
            pl.BlockSpec((NB, 3 * per, PAD, LANES), lambda i: (i, 0, 0, 0)),
            pl.BlockSpec((NB, HEADS, PAD, PAD), lambda i: (i, 0, 0, 0)),
            full(8, d), full(d, 3 * d), *anywhere,
        ],
        out_specs=[pl.BlockSpec((TOP, NB, d), lambda i: (0, i, 0)), pl.BlockSpec((TOK - TOP, NB, d), lambda i: (0, i, 0)), full(d, 3 * d), full(8, d), full(1, 3 * d), full(HEADS, PAD, PAD), *anywhere],
        out_shape=[
            jax.ShapeDtypeStruct((TOP, imgs, d), F32),
            jax.ShapeDtypeStruct((TOK - TOP, imgs, d), F32),
            jax.ShapeDtypeStruct((d, 3 * d), BF),
            jax.ShapeDtypeStruct((8, d), F32),
            jax.ShapeDtypeStruct((1, 3 * d), F32),
            jax.ShapeDtypeStruct((HEADS, PAD, PAD), F32),
            *[jax.ShapeDtypeStruct(g.shape[1:], F32) for g in grads],
        ],
        scratch_shapes=[
            pltpu.VMEM((per, PAD * NB, LANES), F32),
            pltpu.VMEM((3 * per, PAD * NB, LANES), F32),
            pltpu.VMEM((d, 3 * d), F32),
            pltpu.VMEM((8, d), F32),
            pltpu.VMEM((1, 3 * d), F32),
            *delivery_scratch(owners, grads),
        ],
        compiler_params=pltpu.CompilerParams(collective_id=3, has_side_effects=True, vmem_limit_bytes=62 << 20),
        name="back",
    )(x, halo, gm, gatt, qkv, prob, vecs, w, *grads)


DEEP = 4


class Place:
    def __init__(self, inner):
        self.inner = inner
        me, core = lax.axis_index("fsdp"), lax.axis_index("win")
        self.core, self.mate = core, 1 - core
        self.z = me // (inner * inner)
        u, v = (me // inner) % inner, me % inner
        self.a = u * (1 - core) + v * core
        self.b = v * (1 - core) + u * core
        self.step_a = inner * (1 - core) + core
        self.step_b = inner * core + 1 - core

    def at(self, dz=0, da=0, db=0):
        z = (self.z + dz) % DEEP
        a = (self.a + da) % self.inner
        b = (self.b + db) % self.inner
        return z * self.inner * self.inner + a * self.step_a + b * self.step_b

    def device(self, dz=0, da=0, db=0):
        return (self.at(dz, da, db), self.core)

    def partner(self):
        return (self.at(), self.mate)

    def peers(self):
        near = [self.device(dz=d) for d in range(1, DEEP)]
        near += [self.device(da=d) for d in range(1, self.inner)]
        near += [self.device(db=d) for d in range(1, self.inner)]
        return near + [self.partner()]


def meet(place):
    barrier = pltpu.get_barrier_semaphore()
    peers = place.peers()
    for peer in peers:
        pl.semaphore_signal(barrier, inc=1, device_id=peer, device_id_type=pl.DeviceIdType.MESH)
    pl.semaphore_wait(barrier, len(peers))


def remote(src, dst, send_sem, recv_sem, device):
    return pltpu.make_async_remote_copy(
        src_ref=src, dst_ref=dst, send_sem=send_sem, recv_sem=recv_sem, device_id=device,
        device_id_type=pl.DeviceIdType.MESH,
    )


class Spread:
    def __init__(self, inner, ins, maps, outs, halos, send_sem, recv_sem, own_sem, halo_sem):
        self.inner, self.ins, self.maps, self.outs, self.halos = inner, ins, maps, outs, halos
        self.send_sem, self.recv_sem, self.own_sem, self.halo_sem = send_sem, recv_sem, own_sem, halo_sem
        steps = [("a", d) for d in range(1, inner)], [("b", d) for d in range(1, inner)]
        order_z, mate = (1, 3, 2), [("m", 0)]
        plan = [[((0, 0, 0), [("z", d) for d in order_z] + steps[0] + steps[1])]]
        plan.append([((dz, 0, 0), steps[0] + steps[1] + mate) for dz in order_z])
        plan.append([((dz, da, 0), steps[1] + mate) for da in range(1, inner) for dz in (0,) + order_z])
        plan.append([((dz, da, db), mate) for db in range(1, inner) for da in range(inner) for dz in (0,) + order_z])
        self.plan, count = [], 0
        for stage in plan:
            rows = []
            for block, targets in stage:
                rows.append((block, [(t, count + i) for i, t in enumerate(targets)]))
                count += len(targets)
            self.plan.append(rows)

    def piece(self, k, block, core):
        half = self.outs[k].shape[-1] // 2
        return self.outs[k].at[block, :, pl.ds(pl.multiple_of(core * half, LANES), half)]

    def copy(self, place, k, stage, block, target, index):
        (axis, d), where = target, place.at(*block)
        device = {"z": place.device(dz=d), "a": place.device(da=d), "b": place.device(db=d), "m": place.partner()}[axis]
        half = self.outs[k].shape[-1] // 2
        src = self.piece(k, where, place.core)
        if stage == 0:
            src = self.ins[k].at[:, pl.ds(pl.multiple_of(place.core * half, LANES), half)]
        return remote(src, self.piece(k, where, place.core), self.send_sem.at[k, index],
                      self.recv_sem.at[k, place.core, where], device)

    def arrive(self, place, k, block, core):
        at = self.piece(k, place.at(*block), core)
        remote(at, at, self.send_sem.at[k, 0], self.recv_sem.at[k, core, place.at(*block)], place.partner()).wait_recv()

    def local(self, place):
        copies = [remote(self.maps[f].at[:TOP], self.halos[f], self.halo_sem.at[f, 0], self.halo_sem.at[f, 1],
                         place.partner()) for f in range(len(self.maps))]
        copies += [pltpu.make_async_copy(self.ins[k], self.outs[k].at[place.at()], self.own_sem.at[k])
                   for k in range(len(self.ins))]
        return copies

    def run(self, stage, kinds=None):
        place = Place(self.inner)
        for k in range(len(self.ins)) if kinds is None else kinds:
            for block, targets in self.plan[stage]:
                if stage:
                    self.arrive(place, k, block, place.core)
                for target, index in targets:
                    self.copy(place, k, stage, block, target, index).start()
        if stage == 0:
            for copy in self.local(place):
                copy.start()

    def finish(self):
        place = Place(self.inner)
        for k in range(len(self.ins)):
            for stage in self.plan[1:]:
                for block, _ in stage:
                    self.arrive(place, k, block, place.mate)
            for stage, rows in enumerate(self.plan):
                for block, targets in rows:
                    for target, index in targets:
                        self.copy(place, k, stage, block, target, index).wait_send()
        for copy in self.local(place):
            copy.wait()


def spread_scratch(owners, kinds, fields):
    inner = inner_of(owners)
    sends = 3 + 2 * (inner - 1) + 3 * (2 * inner - 1) + 2 * DEEP * (inner - 1) * inner
    dma = pltpu.SemaphoreType.DMA
    return [dma((kinds, sends)), dma((kinds, 2, owners)), dma((kinds,)), dma((fields, 2))]


def spread_shapes(owners, shards, maps):
    return [jax.ShapeDtypeStruct((owners, *s.shape), s.dtype) for s in shards] + [
        jax.ShapeDtypeStruct((TOP, *m.shape[1:]), m.dtype) for m in maps
    ]


def gather_kernel(inner, kinds, fields, *refs):
    ins, maps = refs[:kinds], refs[kinds : kinds + fields]
    outs, halos = refs[kinds + fields : 2 * kinds + fields], refs[2 * kinds + fields : 2 * (kinds + fields)]
    meet(Place(inner))
    moves = Spread(inner, ins, maps, outs, halos, *refs[2 * (kinds + fields) :])
    moves.run(0)
    for k in range(kinds):
        moves.run(1, (k,))
        moves.run(2, (k,))
    moves.run(3)
    moves.finish()


def inner_of(owners):
    return int(round((owners // DEEP) ** 0.5))


def gathered(shards, maps):
    owners = lax.axis_size("fsdp")
    inner, kinds, fields = inner_of(owners), len(shards), len(maps)
    anywhere = pl.BlockSpec(memory_space=pl.ANY)
    return pl.pallas_call(
        functools.partial(gather_kernel, inner, kinds, fields),
        in_specs=[anywhere] * (kinds + fields),
        out_specs=[anywhere] * (kinds + fields),
        out_shape=spread_shapes(owners, shards, maps),
        scratch_shapes=spread_scratch(owners, kinds, fields),
        compiler_params=pltpu.CompilerParams(collective_id=0, has_side_effects=True),
        name="gather",
    )(*shards, *maps)


class Delivery:
    def __init__(self, inner, ins, outs, refs):
        self.inner, self.ins, self.outs, kinds = inner, ins, outs, len(ins)
        self.kinds = range(kinds)
        self.own, self.from_mate, self.from_b, self.from_a, self.from_z, self.final = (
            refs[i * kinds : (i + 1) * kinds] for i in range(6)
        )
        self.load_sem, self.mate_sem, self.b_sem, self.a_sem, self.z_sem, self.end_sem = refs[6 * kinds : 6 * kinds + 6]
        self.steps = range(1, inner)

    def columns(self, k, core):
        half = self.outs[k].shape[-1] // 2
        return pl.ds(pl.multiple_of(core * half, LANES), half)

    def add(self, k, block, other):
        self.own[k][block] = (self.own[k][block].astype(F32) + other[...].astype(F32)).astype(BF)

    def loads(self, place, k):
        return (
            remote(self.ins[k].at[:, :, self.columns(k, place.mate)], self.from_mate[k], self.mate_sem.at[k, 0],
                   self.mate_sem.at[k, 1], place.partner()),
            pltpu.make_async_copy(self.ins[k].at[:, :, self.columns(k, place.core)], self.own[k], self.load_sem.at[k]),
        )

    def to_b(self, place, k, dz, da, db):
        slot = (db - 1) * self.inner * DEEP + da * DEEP + dz
        return remote(self.own[k].at[place.at(dz, da, db)], self.from_b[k].at[slot], self.b_sem.at[k, 0, slot],
                      self.b_sem.at[k, 1, slot], place.device(db=db))

    def to_a(self, place, k, dz, da):
        slot = (da - 1) * DEEP + dz
        return remote(self.own[k].at[place.at(dz, da)], self.from_a[k].at[slot], self.a_sem.at[k, 0, slot],
                      self.a_sem.at[k, 1, slot], place.device(da=da))

    def to_z(self, place, k, dz):
        return remote(self.own[k].at[place.at(dz)], self.from_z[k].at[dz - 1], self.z_sem.at[k, 0, dz - 1],
                      self.z_sem.at[k, 1, dz - 1], place.device(dz=dz))

    def ends(self, place, k):
        there = self.outs[k].at[:, self.columns(k, place.core)]
        return (remote(self.final[k], there, self.end_sem.at[k, 0], self.end_sem.at[k, 1], place.partner()),
                pltpu.make_async_copy(self.final[k], there, self.end_sem.at[k, 2]))

    def start(self):
        place = Place(self.inner)
        for k in self.kinds:
            for copy in self.loads(place, k):
                copy.start()

    def pass_b(self):
        place = Place(self.inner)
        for k in self.kinds:
            for copy in self.loads(place, k):
                copy.wait()
            for db in tuple(self.steps) + (0,):
                for da in range(self.inner):
                    for dz in range(DEEP):
                        block = place.at(dz, da, db)
                        self.add(k, block, self.from_mate[k].at[block])
                        if db:
                            self.to_b(place, k, dz, da, db).start()

    def pass_a(self):
        place = Place(self.inner)
        for k in self.kinds:
            for db in self.steps:
                for da in range(self.inner):
                    for dz in range(DEEP):
                        self.to_b(place, k, dz, da, db).wait()
            for da in tuple(self.steps) + (0,):
                for dz in range(DEEP):
                    for db in self.steps:
                        self.add(k, place.at(dz, da), self.from_b[k].at[(db - 1) * self.inner * DEEP + da * DEEP + dz])
                    if da:
                        self.to_a(place, k, dz, da).start()

    def pass_z(self):
        place = Place(self.inner)
        for k in self.kinds:
            for da in self.steps:
                for dz in range(DEEP):
                    self.to_a(place, k, dz, da).wait()
            for dz in (2, 1, 3, 0):
                for da in self.steps:
                    self.add(k, place.at(dz), self.from_a[k].at[(da - 1) * DEEP + dz])
                if dz:
                    self.to_z(place, k, dz).start()

    def hand_over(self):
        place = Place(self.inner)
        for k in self.kinds:
            for dz in (2, 1, 3):
                self.to_z(place, k, dz).wait()
            total = self.own[k][place.at()].astype(F32)
            for dz in range(1, DEEP):
                total = total + self.from_z[k][dz - 1].astype(F32)
            self.final[k][...] = total
            for copy in self.ends(place, k):
                copy.start()

    def finish(self):
        place = Place(self.inner)
        for k in self.kinds:
            for copy in self.ends(place, k):
                copy.wait()


def delivery_scratch(owners, grads):
    inner, kinds = inner_of(owners), len(grads)
    halves = [(g.shape[1], g.shape[2] // 2) for g in grads]
    dma = pltpu.SemaphoreType.DMA

    def room(count):
        return [pltpu.VMEM((count, *h), BF) for h in halves]

    return [
        *room(owners), *room(owners), *room((inner - 1) * inner * DEEP), *room((inner - 1) * DEEP),
        *room(DEEP - 1), *[pltpu.VMEM(h, F32) for h in halves],
        dma((kinds,)), dma((kinds, 2)), dma((kinds, 2, (inner - 1) * inner * DEEP)),
        dma((kinds, 2, (inner - 1) * DEEP)), dma((kinds, 2, DEEP - 1)), dma((kinds, 3)),
    ]


def deliver_kernel(inner, kinds, *refs):
    ins, table_ref, outs, sum_ref = refs[:kinds], refs[kinds], refs[kinds + 1 : 2 * kinds + 1], refs[2 * kinds + 1]
    parts, part_sem = refs[-2:]
    place = Place(inner)
    meet(place)
    moves = Delivery(inner, ins, outs, refs[2 * kinds + 2 :])

    def table_stage(stage, value, count, mine, peer):
        parts[stage, mine] = value
        copies = [remote(parts.at[stage, mine], parts.at[stage, mine], part_sem.at[stage, 0, d],
                         part_sem.at[stage, 1, d], peer(d)) for d in range(1, count)]
        for copy in copies:
            copy.start()
        return copies, stage, count

    def table_sum(begun):
        copies, stage, count = begun
        for copy in copies:
            copy.wait()
        total = parts[stage, 0]
        for i in range(1, count):
            total = total + parts[stage, i]
        return total

    u = place.a * (1 - place.core) + place.b * place.core
    v = place.b * (1 - place.core) + place.a * place.core
    along_u = lambda d: (place.at(da=d * (1 - place.core), db=d * place.core), place.core)
    along_v = lambda d: (place.at(da=d * place.core, db=d * (1 - place.core)), place.core)
    begun = table_stage(0, table_ref[...], 2, place.core, lambda d: place.partner())
    moves.start()
    moves.pass_b()
    begun = table_stage(1, table_sum(begun), inner, u, along_u)
    moves.pass_a()
    begun = table_stage(2, table_sum(begun), inner, v, along_v)
    moves.pass_z()
    begun = table_stage(3, table_sum(begun), DEEP, place.z, lambda d: place.device(dz=d))
    moves.hand_over()
    moves.finish()
    sum_ref[...] = table_sum(begun)


def delivered(grads, table):
    owners = lax.axis_size("fsdp")
    inner, kinds = inner_of(owners), len(grads)
    anywhere = pl.BlockSpec(memory_space=pl.ANY)
    dma = pltpu.SemaphoreType.DMA
    return pl.pallas_call(
        functools.partial(deliver_kernel, inner, kinds),
        in_specs=[anywhere] * kinds + [pl.BlockSpec(memory_space=pltpu.VMEM)],
        out_specs=[anywhere] * kinds + [pl.BlockSpec(memory_space=pltpu.VMEM)],
        out_shape=[jax.ShapeDtypeStruct(g.shape[1:], F32) for g in grads]
        + [jax.ShapeDtypeStruct(table.shape, F32)],
        scratch_shapes=[
            *delivery_scratch(owners, grads), pltpu.VMEM((4, DEEP, *table.shape), F32), dma((4, 2, DEEP)),
        ],
        compiler_params=pltpu.CompilerParams(collective_id=1, has_side_effects=True, vmem_limit_bytes=60 << 20),
        name="deliver",
    )(*grads, table)


def window_of_tokens():
    row, col = np.arange(TOK) // (2 * WIN), np.arange(TOK) % (2 * WIN)
    row, col = (row - SHIFT) % WIN, (col - SHIFT) % (2 * WIN)
    return col // WIN, row * WIN + col % WIN


def spread_matrix():
    _, place = window_of_tokens()
    return (place[:, None] == np.arange(WIN * WIN)[None, :]).astype(np.float32)


def relative_parts(rel_index, table):
    count = WIN * WIN
    onehot = (rel_index.reshape(count * count, 1) == jnp.arange(table.shape[0], dtype=jnp.int32)[None, :]).astype(F32)
    relative = jnp.dot(onehot, table, precision=HIGHEST).reshape(count, count, -1).transpose(2, 0, 1)
    return onehot, relative


def bias_of_pairs(relative, regions):
    side, place = window_of_tokens()
    spread = jnp.asarray(spread_matrix())
    wide = jnp.einsum("at,hts,bs->hba", spread, relative, spread, precision=HIGHEST)
    region = regions.reshape(2, WIN * WIN)
    region = jnp.concatenate(
        [jnp.roll(region[s].reshape(WIN, WIN), SHIFT, axis=0)[:, c] for s, c in ((1, slice(4, 7)), (0, slice(0, 7)), (1, slice(0, 4)))],
        axis=1,
    ).reshape(TOK)
    mask = jnp.where(region[:, None] == region[None, :], 0.0, -100.0)
    same = jnp.asarray(side[:, None] == side[None, :])
    bias = jnp.where(same[None], wide + mask[None], FAR)
    return jnp.pad(
        jnp.pad(bias, ((0, 0), (0, PAD - TOK), (0, 0)), constant_values=FAR),
        ((0, 0), (0, 0), (0, LANES - TOK)),
    )


def packed_row(parts):
    row = jnp.concatenate(parts, axis=-1)
    return jnp.pad(row, [(0, 0)] * (row.ndim - 1) + [(0, -row.shape[-1] % (2 * LANES))])


def per_device(
    images, norm1_gain, norm1_bias, qkv_weight, q_bias, v_bias, proj_weight, proj_bias, norm2_gain, norm2_bias,
    fc1_weight, fc1_bias, fc2_weight, fc2_bias, bias_table, regions, rel_index, cotangent,
):
    imgs, rows, cols, d = images.shape
    owners = lax.axis_size("fsdp")
    x = images.transpose(1, 2, 0, 3).reshape(rows * cols, imgs, d)
    ct = cotangent.transpose(1, 2, 0, 3).reshape(rows * cols, imgs, d)
    vectors = (norm1_gain, norm1_bias, q_bias, v_bias, proj_bias, norm2_gain, norm2_bias, fc2_bias, fc1_bias)
    packed, w_qkv, halo = gathered((packed_row(vectors)[None], qkv_weight), (x,))
    packed = packed[:, 0].astype(F32)
    part = d // owners
    vecs = packed[:, : 8 * part].reshape(owners, 8, part).transpose(1, 0, 2).reshape(8, d)
    b_in = packed[:, 8 * part : 8 * part + fc1_bias.shape[0]].reshape(1, -1)
    whole = lambda v: v.reshape(owners * v.shape[1], v.shape[2])
    w_qkv = whole(w_qkv)
    onehot, relative = relative_parts(rel_index, bias_table)
    rel = bias_of_pairs(relative, regions)

    qkv, att, prob, *mats, ct_halo = attend(
        x, halo, vecs, w_qkv, rel, (proj_weight, fc1_weight, fc2_weight), (ct,)
    )
    w_proj, w_in, w_out = (whole(v) for v in mats)
    flat = lambda v: v.reshape(v.shape[0] * imgs, d)
    tall = lambda v: v.reshape(v.shape[0] // imgs, imgs, d)
    out_top, out_rest, gm, gatt, dwp, dw1, dw2, db_in, small2 = mlp(
        flat(x), flat(halo), flat(att), flat(ct), flat(ct_halo), w_proj, vecs, w_in, b_in, w_out
    )
    swapped = lambda v: lax.ppermute(v, "win", [(0, 1), (1, 0)])
    out_top = swapped(out_top)
    blocks = lambda v: v.reshape(owners, v.shape[0] // owners, v.shape[1])
    gin_top, gin_rest, dwq, small1, bsum, rel_sum, dwp, dw1, dw2 = back(
        x, halo, tall(gm), tall(gatt), qkv, prob, vecs, w_qkv, (blocks(dwp), blocks(dw1), blocks(dw2))
    )
    gin_top = swapped(gin_top)
    spread = jnp.asarray(spread_matrix())
    pairs = jnp.einsum("at,hba,bs->tsh", spread, rel_sum[:, :TOK, :TOK], spread, precision=HIGHEST)
    table = jnp.dot(onehot.T, pairs.reshape(WIN**4, -1), precision=HIGHEST)
    flat_table = jnp.pad(table.reshape(-1), (0, -table.size % (8 * LANES))).reshape(-1, LANES)
    grads = (
        small1[0], small1[1], bsum[0, :d], bsum[0, 2 * d :], small2[2], small2[0], small2[1], small2[3], db_in[0],
    )
    row = packed_row([v.reshape(owners, 1, -1) for v in grads]).astype(BF)
    sums, dwq, table_sum = delivered((row, blocks(dwq)), flat_table)
    at, own = 0, []
    for v in vectors:
        own.append(sums[0, at : at + v.shape[0]])
        at += v.shape[0]
    dg1, db1, dqb, dvb, dbp, dg2, db2, db_out, db_in = own
    table = table_sum.reshape(-1)[: table.size].reshape(table.shape)
    joined = lambda top, rest: jnp.concatenate([top, rest], axis=0).reshape(rows, cols, imgs, d).transpose(2, 0, 1, 3)
    return (
        joined(tall(out_top), tall(out_rest)), joined(gin_top, gin_rest), dg1, db1, dwq, dqb, dvb, dwp, dbp, dg2, db2, dw1, db_in, dw2,
        db_out, table,
    )


def solution(mesh):
    vec, mat, img = P("fsdp"), P("fsdp", None), P("fsdp", "win", None, None)
    in_specs = (
        img, vec, vec, mat, vec, vec, mat, vec, vec, vec, mat, vec, mat, vec, P(), P("win", None, None), P(), img,
    )
    out_specs = (img, img, vec, vec, mat, vec, vec, mat, vec, vec, vec, mat, vec, mat, vec, P())
    return jax.shard_map(per_device, mesh=mesh, in_specs=in_specs, out_specs=out_specs, check_vma=False)
```

```python
import functools
import jax
import jax.numpy as jnp
import numpy as np
from jax import lax
from jax.experimental import pallas as pl
from jax.experimental.pallas import tpu as pltpu
from jax.sharding import PartitionSpec as P

HEADS = 16
HD = 32
WIN = 7
SHIFT = 3
TOK = 98
TOP = 42
PAD = 112
LANES = 128
GROUPS = 4
NB = 8
EPS = 1e-05
FAR = -1e30
F32 = jnp.float32
BF = jnp.bfloat16
HIGHEST = lax.Precision.HIGHEST


def mm(a, b):
    return lax.dot_general(a, b, (((1,), (0,)), ((), ())), preferred_element_type=F32)


def mm_nt(a, b):
    return lax.dot_general(a, b, (((1,), (1,)), ((), ())), preferred_element_type=F32)


def mm_tn(a, b):
    return lax.dot_general(a, b, (((0,), (0,)), ((), ())), preferred_element_type=F32)


def normalized(x):
    mean = jnp.mean(x, axis=-1, keepdims=True)
    c = x - mean
    var = jnp.mean(c * c, axis=-1, keepdims=True)
    r = lax.rsqrt(var + EPS)
    return c * r, r


def norm_back(u, n, r):
    return r * (u - jnp.mean(u, axis=-1, keepdims=True) - n * jnp.mean(u * n, axis=-1, keepdims=True))


def col_sum(v):
    return jnp.sum(v, axis=0, keepdims=True)


def erf(x):
    x = jnp.clip(x, -3.7439211627767994, 3.7439211627767994)
    s = x * x
    a = (0.00022905065861350646, 0.0034082910107109506, 0.050955695062380861, 0.18520832239976145, 1.128379143519084)
    b = (-1.1791602954361697e-7, 0.000023547966471313185, 0.0010179625278914885, 0.014070470171167667, 0.11098505178285362, 0.49746925110067538, 1.0)
    p = a[0]
    for c in a[1:]:
        p = p * s + c
    q = b[0]
    for c in b[1:]:
        q = q * s + c
    return x * p / q


def head_masks():
    lane = lax.broadcasted_iota(jnp.int32, (1, LANES), 1) // HD
    return [(lane == h).astype(BF) for h in range(GROUPS)]


def shifted_rows(x_ref, halo_ref):
    x = jnp.concatenate([halo_ref[...], x_ref[TOP:]], axis=0)
    return x.astype(F32).reshape(x.shape[0] * NB, x.shape[-1])


def own_lanes(stack):
    lane = lax.broadcasted_iota(jnp.int32, (1, LANES), 1) // HD
    out = stack[:PAD]
    for h in range(1, GROUPS):
        out = jnp.where(lane == h, stack[h * PAD : (h + 1) * PAD], out)
    return out


def at_step(step, action):
    @pl.when(pl.program_id(0) == step)
    def _():
        action()


def at_images(events, i):
    images = pl.program_id(0) * NB + i
    for share, action in events:
        @pl.when(images == share)
        def _(action=action):
            action()


def whole_cuts(count):
    return tuple((i, 0, 1) for i in range(count))


def attend_kernel(inner, kinds, fields, x_ref, halo_ref, vec_ref, w_ref, rel_ref, *refs):
    ins, maps = refs[:kinds], refs[kinds : kinds + fields]
    qkv_ref, att_ref, prob_ref = refs[kinds + fields : kinds + fields + 3]
    outs, halos = refs[kinds + fields + 3 : 2 * kinds + fields + 3], refs[2 * kinds + fields + 3 : 2 * (kinds + fields) + 3]
    wide, joined, *sems = refs[2 * (kinds + fields) + 3 :]
    moves = Spread(inner, whole_cuts(kinds), ins, maps, outs, halos, *sems)

    def begin():
        meet(Place(inner))
        moves.run(0)

    at_step(0, begin)
    early, late = tuple(range(kinds - 1)), (kinds - 1,)
    events = [
        (share, functools.partial(moves.run, stage, which))
        for share, stage, which in ((8, 1, early), (13, 1, late), (15, 2, early), (19, 2, late), (23, 3, early), (28, 3, late))
    ]
    d = x_ref.shape[-1]
    n, _ = normalized(shifted_rows(x_ref, halo_ref))
    normed = (n * vec_ref[0:1] + vec_ref[1:2]).astype(BF)
    lanes3 = 3 * d // LANES
    chunk = d
    biases = (vec_ref[2:3], None, vec_ref[3:4])

    @pl.when(pl.program_id(0) == 0)
    def _():
        wide[:, TOK * NB :, :] = jnp.zeros((lanes3, (PAD - TOK) * NB, LANES), F32)

    for c in range(3 * d // chunk):
        part = mm(normed, w_ref[:, c * chunk : (c + 1) * chunk])
        if biases[c] is not None:
            part = part + biases[c]
        for k in range(chunk // LANES):
            wide[c * (chunk // LANES) + k, : TOK * NB, :] = part[:, k * LANES : (k + 1) * LANES]
    masks = head_masks()
    per = d // LANES
    scale = HD ** (-0.5)

    def one(i, carry):
        at_images(events, i)
        for g in range(per):
            q = wide[g, pl.ds(i, PAD, stride=NB), :].astype(BF)
            k = wide[per + g, pl.ds(i, PAD, stride=NB), :].astype(BF)
            v = wide[2 * per + g, pl.ds(i, PAD, stride=NB), :].astype(BF)
            qkv_ref[i, g] = q
            qkv_ref[i, per + g] = k
            qkv_ref[i, 2 * per + g] = v
            scores = mm_nt(jnp.concatenate([k * m for m in masks], axis=0), q)
            v_t = v.T
            heads = []
            for h in range(GROUPS):
                s = scores[h * PAD : (h + 1) * PAD] * scale + rel_ref[g * GROUPS + h][:, :PAD]
                e = jnp.exp(s - jnp.max(s, axis=0, keepdims=True))
                p = (e * (1.0 / jnp.sum(e, axis=0, keepdims=True))).astype(BF)
                prob_ref[i, g * GROUPS + h] = p
                heads.append(mm(v_t[h * HD : (h + 1) * HD], p))
            joined[g, pl.ds(i, PAD, stride=NB), :] = jnp.concatenate(heads, axis=0).T
        return carry

    lax.fori_loop(0, NB, one, 0)
    for g in range(per):
        att_ref[:, :, g * LANES : (g + 1) * LANES] = joined[g, : TOK * NB, :].astype(BF).reshape(TOK, NB, LANES)
    at_step(3, moves.finish)


def attend(x, halo, vecs, w, rel, shards, maps):
    _, imgs, d = x.shape
    owners = lax.axis_size("fsdp")
    inner, kinds, fields = inner_of(owners), len(shards), len(maps)
    anywhere = [pl.BlockSpec(memory_space=pl.ANY)] * (kinds + fields)
    full = lambda *shape: pl.BlockSpec(shape, lambda i: (0,) * len(shape), pipeline_mode=pl.Buffered(1))
    per = d // LANES
    return pl.pallas_call(
        functools.partial(attend_kernel, inner, kinds, fields),
        grid=(imgs // NB,),
        in_specs=[
            pl.BlockSpec((TOK, NB, d), lambda i: (0, i, 0)),
            pl.BlockSpec((TOP, NB, d), lambda i: (0, i, 0)),
            full(8, d), full(d, 3 * d), full(HEADS, PAD, LANES), *anywhere,
        ],
        out_specs=[
            pl.BlockSpec((NB, 3 * per, PAD, LANES), lambda i: (i, 0, 0, 0)),
            pl.BlockSpec((TOK, NB, d), lambda i: (0, i, 0)),
            pl.BlockSpec((NB, HEADS, PAD, PAD), lambda i: (i, 0, 0, 0)),
            *anywhere,
        ],
        out_shape=[
            jax.ShapeDtypeStruct((imgs, 3 * per, PAD, LANES), BF),
            jax.ShapeDtypeStruct((TOK, imgs, d), BF),
            jax.ShapeDtypeStruct((imgs, HEADS, PAD, PAD), BF),
            *spread_shapes(owners, shards, maps),
        ],
        scratch_shapes=[
            pltpu.VMEM((3 * per, PAD * NB, LANES), F32),
            pltpu.VMEM((per, PAD * NB, LANES), F32),
            *spread_scratch(owners, kinds, kinds, fields),
        ],
        compiler_params=pltpu.CompilerParams(collective_id=2, has_side_effects=True, vmem_limit_bytes=60 << 20),
        name="attend",
    )(x, halo, vecs, w, rel, *shards, *maps)


def mlp_kernel(tops, x_ref, halo_ref, att_ref, ct_ref, ct_halo_ref, wp_ref, vec_ref, w1_ref, b1_ref, w2_ref,
               top_ref, rest_ref, gm_ref, gatt_ref, dwp_ref, dw1_ref, dw2_ref, db1_ref, small_ref,
               awp, aw1, aw2, ab1, asm):
    step = pl.program_id(0)
    d = x_ref.shape[-1]
    ff = w1_ref.shape[-1]
    chunk = 512

    @pl.when(step == 0)
    def _():
        awp[...] = jnp.zeros_like(awp)
        aw1[...] = jnp.zeros_like(aw1)
        aw2[...] = jnp.zeros_like(aw2)
        ab1[...] = jnp.zeros_like(ab1)
        asm[...] = jnp.zeros_like(asm)

    att = att_ref[...]
    above = step < tops
    gb = jnp.where(above, ct_halo_ref[...], ct_ref[...])
    grad_out = gb.astype(F32)
    middle = jnp.where(above, halo_ref[...], x_ref[...]).astype(F32) + mm(att, wp_ref[...]) + vec_ref[4:5]
    n, r = normalized(middle)
    normed = (n * vec_ref[5:6] + vec_ref[6:7]).astype(BF)
    normed_t = normed.T
    gb_t = gb.T
    out = middle + vec_ref[7:8]
    m = None
    def begin(c):
        at = slice(c * chunk, (c + 1) * chunk)
        return mm(normed, w1_ref[:, at]), mm_nt(gb, w2_ref[at, :])

    now = begin(0)
    for c in range(ff // chunk):
        at = slice(c * chunk, (c + 1) * chunk)
        later = begin(c + 1) if c + 1 < ff // chunk else None
        hidden = now[0] + b1_ref[:, at]
        cdf = 0.5 * (1.0 + erf(hidden * 0.7071067811865476))
        slope = cdf + hidden * (0.3989422804014327 * jnp.exp(-0.5 * hidden * hidden))
        active = (hidden * cdf).astype(BF)
        gh = now[1] * slope
        ghb = gh.astype(BF)
        ab1[:, at] += col_sum(ghb.astype(F32))
        out = out + mm(active, w2_ref[at, :])
        part = mm_nt(ghb, w1_ref[:, at])
        m = part if m is None else m + part
        aw2[:, at] += mm(gb_t, active)
        aw1[:, at] += mm(normed_t, ghb)
        now = later

    @pl.when(above)
    def _():
        top_ref[...] = out.astype(BF)

    @pl.when(jnp.logical_not(above))
    def _():
        rest_ref[...] = out.astype(BF)

    grad_middle = grad_out + norm_back(m * vec_ref[5:6], n, r)
    gm_ref[...] = grad_middle
    gp = grad_middle.astype(BF)
    gatt_ref[...] = mm_nt(gp, wp_ref[...]).astype(BF)
    awp[...] += mm_tn(att, gp)
    asm[0:1, :] += col_sum(m * n)
    asm[1:2, :] += col_sum(m)
    asm[2:3, :] += col_sum(gp.astype(F32))
    asm[3:4, :] += col_sum(grad_out)

    @pl.when(step == pl.num_programs(0) - 1)
    def _():
        dwp_ref[...] = awp[...].astype(BF)
        dw1_ref[...] = aw1[...].astype(BF)
        for c in range(ff // chunk):
            at = slice(c * chunk, (c + 1) * chunk)
            dw2_ref[at, :] = aw2[:, at].T.astype(BF)
        db1_ref[...] = ab1[...]
        small_ref[...] = asm[...]


def mlp(x, halo, att, ct, ct_halo, wp, vecs, w1, b1, w2):
    rows, d = x.shape
    tile = halo.shape[0] // 3
    tops = 3
    ff = w1.shape[-1]
    full = lambda *shape: pl.BlockSpec(shape, lambda i: (0,) * len(shape), pipeline_mode=pl.Buffered(1))
    row = pl.BlockSpec((tile, d), lambda i: (i, 0))
    own = pl.BlockSpec((tile, d), lambda i: (jnp.maximum(i, tops), 0))
    top = pl.BlockSpec((tile, d), lambda i: (jnp.minimum(i, tops - 1), 0))
    rest = pl.BlockSpec((tile, d), lambda i: (jnp.maximum(i - tops, 0), 0))
    return pl.pallas_call(
        functools.partial(mlp_kernel, tops),
        grid=(rows // tile,),
        in_specs=[own, top, row, own, top, full(d, d), full(8, d), full(d, ff), full(1, ff), full(ff, d)],
        out_specs=[top, rest, row, row, full(d, d), full(d, ff), full(ff, d), full(1, ff), full(8, d)],
        out_shape=[
            jax.ShapeDtypeStruct((tops * tile, d), BF),
            jax.ShapeDtypeStruct((rows - tops * tile, d), BF),
            jax.ShapeDtypeStruct((rows, d), F32),
            jax.ShapeDtypeStruct((rows, d), BF),
            jax.ShapeDtypeStruct((d, d), BF),
            jax.ShapeDtypeStruct((d, ff), BF),
            jax.ShapeDtypeStruct((ff, d), BF),
            jax.ShapeDtypeStruct((1, ff), F32),
            jax.ShapeDtypeStruct((8, d), F32),
        ],
        scratch_shapes=[
            pltpu.VMEM((d, d), F32), pltpu.VMEM((d, ff), F32), pltpu.VMEM((d, ff), F32),
            pltpu.VMEM((1, ff), F32), pltpu.VMEM((8, d), F32),
        ],
        compiler_params=pltpu.CompilerParams(vmem_limit_bytes=60 << 20),
        name="mlp",
    )(x, halo, att, ct, ct_halo, wp, vecs, w1, b1, w2)


def back_kernel(inner, kinds, x_ref, halo_ref, gm_ref, gatt_ref, qkv_ref, prob_ref, vec_ref, w_ref, *refs):
    ins, (top_ref, rest_ref, dw_ref, small_ref, bsum_ref, rel_ref) = refs[:kinds], refs[kinds : kinds + 6]
    outs, (wide, grads, aw, asm, abs_), room = refs[kinds + 6 : 2 * kinds + 6], refs[2 * kinds + 6 : 2 * kinds + 11], refs[2 * kinds + 11 :]
    moves = Delivery(inner, whole_cuts(kinds), ins, outs, room)

    def begin():
        meet(Place(inner))
        moves.start()

    at_step(0, begin)
    events = [(6, moves.pass_b), (15, moves.pass_a), (20, moves.pass_z), (29, moves.hand_over)]
    step = pl.program_id(0)
    d = x_ref.shape[-1]
    per = d // LANES
    scale = HD ** (-0.5)

    @pl.when(step == 0)
    def _():
        aw[...] = jnp.zeros_like(aw)
        asm[...] = jnp.zeros_like(asm)
        abs_[...] = jnp.zeros_like(abs_)
        rel_ref[...] = jnp.zeros_like(rel_ref)
        wide[:, TOK * NB :, :] = jnp.zeros((per, (PAD - TOK) * NB, LANES), F32)

    for g in range(per):
        wide[g, : TOK * NB, :] = gatt_ref[:, :, g * LANES : (g + 1) * LANES].astype(F32).reshape(TOK * NB, LANES)
    masks = head_masks()

    def one(i, carry):
        at_images(events, i)
        for g in range(per):
            ga = wide[g, pl.ds(i, PAD, stride=NB), :].astype(BF)
            q = qkv_ref[i, g]
            k = qkv_ref[i, per + g]
            v = qkv_ref[i, 2 * per + g]
            dps = mm_nt(jnp.concatenate([v * m for m in masks], axis=0), ga)
            k_t = k.T
            probs, marks, dq = [], [], []
            for h in range(GROUPS):
                p = prob_ref[i, g * GROUPS + h]
                pf = p.astype(F32)
                dp = dps[h * PAD : (h + 1) * PAD]
                ds = (pf * (dp - jnp.sum(pf * dp, axis=0, keepdims=True))).astype(BF)
                rel_ref[g * GROUPS + h] += ds.astype(F32)
                dq.append(mm(k_t[h * HD : (h + 1) * HD], ds))
                probs.append(p)
                marks.append(ds)
            dv = own_lanes(mm(jnp.concatenate(probs, axis=0), ga))
            dk = own_lanes(mm(jnp.concatenate(marks, axis=0), q))
            grads[g, pl.ds(i, PAD, stride=NB), :] = jnp.concatenate(dq, axis=0).T * scale
            grads[per + g, pl.ds(i, PAD, stride=NB), :] = dk * scale
            grads[2 * per + g, pl.ds(i, PAD, stride=NB), :] = dv
        return carry

    lax.fori_loop(0, NB, one, 0)
    n, r = normalized(shifted_rows(x_ref, halo_ref))
    normed = (n * vec_ref[0:1] + vec_ref[1:2]).astype(BF)
    normed_t = normed.T
    dn = None
    for c in range(3):
        at = slice(c * d, (c + 1) * d)
        dqkv = jnp.concatenate([grads[c * per + g, : TOK * NB, :].astype(BF) for g in range(per)], axis=-1)
        abs_[:, at] += col_sum(dqkv.astype(F32))
        aw[:, at] += mm(normed_t, dqkv)
        part = mm_nt(dqkv, w_ref[:, at])
        dn = part if dn is None else dn + part
    dn = dn.astype(BF).astype(F32)
    asm[0:1, :] += col_sum(dn * n)
    asm[1:2, :] += col_sum(dn)
    gin = gm_ref[...].reshape(TOK * NB, d) + norm_back(dn * vec_ref[0:1], n, r)
    gin = gin.reshape(TOK, NB, d)
    top_ref[...] = gin[:TOP]
    rest_ref[...] = gin[TOP:]

    at_step(3, moves.finish)

    @pl.when(step == pl.num_programs(0) - 1)
    def _():
        dw_ref[...] = aw[...].astype(BF)
        small_ref[...] = asm[...]
        bsum_ref[...] = abs_[...]


def back(x, halo, gm, gatt, qkv, prob, vecs, w, grads):
    _, imgs, d = x.shape
    owners, kinds = lax.axis_size("fsdp"), len(grads)
    anywhere = [pl.BlockSpec(memory_space=pl.ANY)] * kinds
    per = d // LANES
    full = lambda *shape: pl.BlockSpec(shape, lambda i: (0,) * len(shape), pipeline_mode=pl.Buffered(1))
    tok = pl.BlockSpec((TOK, NB, d), lambda i: (0, i, 0))
    return pl.pallas_call(
        functools.partial(back_kernel, inner_of(owners), kinds),
        grid=(imgs // NB,),
        in_specs=[
            tok, pl.BlockSpec((TOP, NB, d), lambda i: (0, i, 0)), tok, tok,
            pl.BlockSpec((NB, 3 * per, PAD, LANES), lambda i: (i, 0, 0, 0)),
            pl.BlockSpec((NB, HEADS, PAD, PAD), lambda i: (i, 0, 0, 0)),
            full(8, d), full(d, 3 * d), *anywhere,
        ],
        out_specs=[pl.BlockSpec((TOP, NB, d), lambda i: (0, i, 0)), pl.BlockSpec((TOK - TOP, NB, d), lambda i: (0, i, 0)), full(d, 3 * d), full(8, d), full(1, 3 * d), full(HEADS, PAD, PAD), *anywhere],
        out_shape=[
            jax.ShapeDtypeStruct((TOP, imgs, d), F32),
            jax.ShapeDtypeStruct((TOK - TOP, imgs, d), F32),
            jax.ShapeDtypeStruct((d, 3 * d), BF),
            jax.ShapeDtypeStruct((8, d), F32),
            jax.ShapeDtypeStruct((1, 3 * d), F32),
            jax.ShapeDtypeStruct((HEADS, PAD, PAD), F32),
            *[jax.ShapeDtypeStruct(g.shape[1:], F32) for g in grads],
        ],
        scratch_shapes=[
            pltpu.VMEM((per, PAD * NB, LANES), F32),
            pltpu.VMEM((3 * per, PAD * NB, LANES), F32),
            pltpu.VMEM((d, 3 * d), F32),
            pltpu.VMEM((8, d), F32),
            pltpu.VMEM((1, 3 * d), F32),
            *delivery_scratch(owners, grads, whole_cuts(kinds)),
        ],
        compiler_params=pltpu.CompilerParams(collective_id=3, has_side_effects=True, vmem_limit_bytes=62 << 20),
        name="back",
    )(x, halo, gm, gatt, qkv, prob, vecs, w, *grads)


DEEP = 4


class Place:
    def __init__(self, inner):
        self.inner = inner
        me, core = lax.axis_index("fsdp"), lax.axis_index("win")
        self.core, self.mate = core, 1 - core
        self.z = me // (inner * inner)
        u, v = (me // inner) % inner, me % inner
        self.a = u * (1 - core) + v * core
        self.b = v * (1 - core) + u * core
        self.step_a = inner * (1 - core) + core
        self.step_b = inner * core + 1 - core

    def at(self, dz=0, da=0, db=0):
        z = (self.z + dz) % DEEP
        a = (self.a + da) % self.inner
        b = (self.b + db) % self.inner
        return z * self.inner * self.inner + a * self.step_a + b * self.step_b

    def device(self, dz=0, da=0, db=0):
        return (self.at(dz, da, db), self.core)

    def partner(self):
        return (self.at(), self.mate)

    def peers(self):
        near = [self.device(dz=d) for d in range(1, DEEP)]
        near += [self.device(da=d) for d in range(1, self.inner)]
        near += [self.device(db=d) for d in range(1, self.inner)]
        return near + [self.partner()]


def meet(place):
    barrier = pltpu.get_barrier_semaphore()
    peers = place.peers()
    for peer in peers:
        pl.semaphore_signal(barrier, inc=1, device_id=peer, device_id_type=pl.DeviceIdType.MESH)
    pl.semaphore_wait(barrier, len(peers))


def remote(src, dst, send_sem, recv_sem, device):
    return pltpu.make_async_remote_copy(
        src_ref=src, dst_ref=dst, send_sem=send_sem, recv_sem=recv_sem, device_id=device,
        device_id_type=pl.DeviceIdType.MESH,
    )


def cut_columns(array, cut, core):
    half = array.shape[-1] // 2
    width = half // cut[2]
    return pl.ds(pl.multiple_of(core * half + cut[1] * width, LANES), width)


class Spread:
    def __init__(self, inner, cuts, ins, maps, outs, halos, send_sem, recv_sem, own_sem, halo_sem):
        self.cuts = cuts
        self.inner, self.ins, self.maps, self.outs, self.halos = inner, ins, maps, outs, halos
        self.send_sem, self.recv_sem, self.own_sem, self.halo_sem = send_sem, recv_sem, own_sem, halo_sem
        steps = [("a", d) for d in range(1, inner)], [("b", d) for d in range(1, inner)]
        order_z, mate = (1, 3, 2), [("m", 0)]
        plan = [[((0, 0, 0), [("z", d) for d in order_z] + steps[0] + steps[1])]]
        plan.append([((dz, 0, 0), steps[0] + steps[1] + mate) for dz in order_z])
        plan.append([((dz, da, 0), steps[1] + mate) for da in range(1, inner) for dz in (0,) + order_z])
        plan.append([((dz, da, db), mate) for db in range(1, inner) for da in range(inner) for dz in (0,) + order_z])
        self.plan, count = [], 0
        for stage in plan:
            rows = []
            for block, targets in stage:
                rows.append((block, [(t, count + i) for i, t in enumerate(targets)]))
                count += len(targets)
            self.plan.append(rows)

    def piece(self, k, block, core):
        out = self.outs[self.cuts[k][0]]
        return out.at[block, :, cut_columns(out, self.cuts[k], core)]

    def copy(self, place, k, stage, block, target, index):
        (axis, d), where = target, place.at(*block)
        device = {"z": place.device(dz=d), "a": place.device(da=d), "b": place.device(db=d), "m": place.partner()}[axis]
        src = self.piece(k, where, place.core)
        if stage == 0:
            shard = self.ins[self.cuts[k][0]]
            src = shard.at[:, cut_columns(shard, self.cuts[k], place.core)]
        return remote(src, self.piece(k, where, place.core), self.send_sem.at[k, index],
                      self.recv_sem.at[k, place.core, where], device)

    def arrive(self, place, k, block, core):
        at = self.piece(k, place.at(*block), core)
        remote(at, at, self.send_sem.at[k, 0], self.recv_sem.at[k, core, place.at(*block)], place.partner()).wait_recv()

    def local(self, place):
        copies = [remote(self.maps[f].at[:TOP], self.halos[f], self.halo_sem.at[f, 0], self.halo_sem.at[f, 1],
                         place.partner()) for f in range(len(self.maps))]
        copies += [pltpu.make_async_copy(self.ins[k], self.outs[k].at[place.at()], self.own_sem.at[k])
                   for k in range(len(self.ins))]
        return copies

    def run(self, stage, kinds=None):
        place = Place(self.inner)
        for k in range(len(self.cuts)) if kinds is None else kinds:
            for block, targets in self.plan[stage]:
                if stage:
                    self.arrive(place, k, block, place.core)
                for target, index in targets:
                    self.copy(place, k, stage, block, target, index).start()
        if stage == 0:
            for copy in self.local(place):
                copy.start()

    def finish(self):
        place = Place(self.inner)
        for k in range(len(self.cuts)):
            for stage in self.plan[1:]:
                for block, _ in stage:
                    self.arrive(place, k, block, place.mate)
            for stage, rows in enumerate(self.plan):
                for block, targets in rows:
                    for target, index in targets:
                        self.copy(place, k, stage, block, target, index).wait_send()
        for copy in self.local(place):
            copy.wait()


def spread_scratch(owners, kinds, arrays, fields):
    inner = inner_of(owners)
    sends = 3 + 2 * (inner - 1) + 3 * (2 * inner - 1) + 2 * DEEP * (inner - 1) * inner
    dma = pltpu.SemaphoreType.DMA
    return [dma((kinds, sends)), dma((kinds, 2, owners)), dma((arrays,)), dma((fields, 2))]


def spread_shapes(owners, shards, maps):
    return [jax.ShapeDtypeStruct((owners, *s.shape), s.dtype) for s in shards] + [
        jax.ShapeDtypeStruct((TOP, *m.shape[1:]), m.dtype) for m in maps
    ]


def gather_kernel(inner, cuts, kinds, fields, *refs):
    ins, maps = refs[:kinds], refs[kinds : kinds + fields]
    outs, halos = refs[kinds + fields : 2 * kinds + fields], refs[2 * kinds + fields : 2 * (kinds + fields)]
    meet(Place(inner))
    moves = Spread(inner, cuts, ins, maps, outs, halos, *refs[2 * (kinds + fields) :])
    moves.run(0)
    for k in range(len(cuts)):
        moves.run(1, (k,))
        moves.run(2, (k,))
    moves.run(3)
    moves.finish()


def inner_of(owners):
    return int(round((owners // DEEP) ** 0.5))


def gathered(shards, maps, cuts):
    owners = lax.axis_size("fsdp")
    inner, kinds, fields = inner_of(owners), len(shards), len(maps)
    anywhere = pl.BlockSpec(memory_space=pl.ANY)
    return pl.pallas_call(
        functools.partial(gather_kernel, inner, cuts, kinds, fields),
        in_specs=[anywhere] * (kinds + fields),
        out_specs=[anywhere] * (kinds + fields),
        out_shape=spread_shapes(owners, shards, maps),
        scratch_shapes=spread_scratch(owners, len(cuts), kinds, fields),
        compiler_params=pltpu.CompilerParams(collective_id=0, has_side_effects=True),
        name="gather",
    )(*shards, *maps)


class Delivery:
    def __init__(self, inner, cuts, ins, outs, refs):
        self.inner, self.cuts, self.ins, self.outs, kinds = inner, cuts, ins, outs, len(cuts)
        self.kinds = range(kinds)
        self.own, self.from_mate, self.from_b, self.from_a, self.from_z, self.final = (
            refs[i * kinds : (i + 1) * kinds] for i in range(6)
        )
        self.load_sem, self.mate_sem, self.b_sem, self.a_sem, self.z_sem, self.end_sem = refs[6 * kinds : 6 * kinds + 6]
        self.steps = range(1, inner)

    def columns(self, k, core):
        return cut_columns(self.outs[self.cuts[k][0]], self.cuts[k], core)

    def add(self, k, block, other):
        self.own[k][block] = (self.own[k][block].astype(F32) + other[...].astype(F32)).astype(BF)

    def loads(self, place, k):
        return (
            remote(self.ins[self.cuts[k][0]].at[:, :, self.columns(k, place.mate)], self.from_mate[k], self.mate_sem.at[k, 0],
                   self.mate_sem.at[k, 1], place.partner()),
            pltpu.make_async_copy(self.ins[self.cuts[k][0]].at[:, :, self.columns(k, place.core)], self.own[k], self.load_sem.at[k]),
        )

    def to_b(self, place, k, dz, da, db):
        slot = (db - 1) * self.inner * DEEP + da * DEEP + dz
        return remote(self.own[k].at[place.at(dz, da, db)], self.from_b[k].at[slot], self.b_sem.at[k, 0, slot],
                      self.b_sem.at[k, 1, slot], place.device(db=db))

    def to_a(self, place, k, dz, da):
        slot = (da - 1) * DEEP + dz
        return remote(self.own[k].at[place.at(dz, da)], self.from_a[k].at[slot], self.a_sem.at[k, 0, slot],
                      self.a_sem.at[k, 1, slot], place.device(da=da))

    def to_z(self, place, k, dz):
        return remote(self.own[k].at[place.at(dz)], self.from_z[k].at[dz - 1], self.z_sem.at[k, 0, dz - 1],
                      self.z_sem.at[k, 1, dz - 1], place.device(dz=dz))

    def ends(self, place, k):
        there = self.outs[self.cuts[k][0]].at[:, self.columns(k, place.core)]
        return (remote(self.final[k], there, self.end_sem.at[k, 0], self.end_sem.at[k, 1], place.partner()),
                pltpu.make_async_copy(self.final[k], there, self.end_sem.at[k, 2]))

    def start(self):
        place = Place(self.inner)
        for k in self.kinds:
            for copy in self.loads(place, k):
                copy.start()

    def pass_b(self):
        place = Place(self.inner)
        for k in self.kinds:
            for copy in self.loads(place, k):
                copy.wait()
            for db in tuple(self.steps) + (0,):
                for da in range(self.inner):
                    for dz in range(DEEP):
                        block = place.at(dz, da, db)
                        self.add(k, block, self.from_mate[k].at[block])
                        if db:
                            self.to_b(place, k, dz, da, db).start()

    def pass_a(self):
        place = Place(self.inner)
        for k in self.kinds:
            for db in self.steps:
                for da in range(self.inner):
                    for dz in range(DEEP):
                        self.to_b(place, k, dz, da, db).wait()
            for da in tuple(self.steps) + (0,):
                for dz in range(DEEP):
                    for db in self.steps:
                        self.add(k, place.at(dz, da), self.from_b[k].at[(db - 1) * self.inner * DEEP + da * DEEP + dz])
                    if da:
                        self.to_a(place, k, dz, da).start()

    def pass_z(self):
        place = Place(self.inner)
        for k in self.kinds:
            for da in self.steps:
                for dz in range(DEEP):
                    self.to_a(place, k, dz, da).wait()
            for dz in (2, 1, 3, 0):
                for da in self.steps:
                    self.add(k, place.at(dz), self.from_a[k].at[(da - 1) * DEEP + dz])
                if dz:
                    self.to_z(place, k, dz).start()

    def hand_over(self):
        place = Place(self.inner)
        for k in self.kinds:
            for dz in (2, 1, 3):
                self.to_z(place, k, dz).wait()
            total = self.own[k][place.at()].astype(F32)
            for dz in range(1, DEEP):
                total = total + self.from_z[k][dz - 1].astype(F32)
            self.final[k][...] = total
            for copy in self.ends(place, k):
                copy.start()

    def finish(self):
        place = Place(self.inner)
        for k in self.kinds:
            for copy in self.ends(place, k):
                copy.wait()


def delivery_scratch(owners, grads, cuts):
    inner, kinds = inner_of(owners), len(cuts)
    halves = [(grads[i].shape[1], grads[i].shape[2] // 2 // parts) for i, _, parts in cuts]
    dma = pltpu.SemaphoreType.DMA

    def room(count):
        return [pltpu.VMEM((count, *h), BF) for h in halves]

    return [
        *room(owners), *room(owners), *room((inner - 1) * inner * DEEP), *room((inner - 1) * DEEP),
        *room(DEEP - 1), *[pltpu.VMEM(h, F32) for h in halves],
        dma((kinds,)), dma((kinds, 2)), dma((kinds, 2, (inner - 1) * inner * DEEP)),
        dma((kinds, 2, (inner - 1) * DEEP)), dma((kinds, 2, DEEP - 1)), dma((kinds, 3)),
    ]


def deliver_kernel(inner, cuts, kinds, *refs):
    ins, table_ref, outs, sum_ref = refs[:kinds], refs[kinds], refs[kinds + 1 : 2 * kinds + 1], refs[2 * kinds + 1]
    parts, part_sem = refs[-2:]
    place = Place(inner)
    meet(place)
    moves = Delivery(inner, cuts, ins, outs, refs[2 * kinds + 2 :])

    def table_stage(stage, value, count, mine, peer):
        parts[stage, mine] = value
        copies = [remote(parts.at[stage, mine], parts.at[stage, mine], part_sem.at[stage, 0, d],
                         part_sem.at[stage, 1, d], peer(d)) for d in range(1, count)]
        for copy in copies:
            copy.start()
        return copies, stage, count

    def table_sum(begun):
        copies, stage, count = begun
        for copy in copies:
            copy.wait()
        total = parts[stage, 0]
        for i in range(1, count):
            total = total + parts[stage, i]
        return total

    u = place.a * (1 - place.core) + place.b * place.core
    v = place.b * (1 - place.core) + place.a * place.core
    along_u = lambda d: (place.at(da=d * (1 - place.core), db=d * place.core), place.core)
    along_v = lambda d: (place.at(da=d * place.core, db=d * (1 - place.core)), place.core)
    begun = table_stage(0, table_ref[...], 2, place.core, lambda d: place.partner())
    moves.start()
    moves.pass_b()
    begun = table_stage(1, table_sum(begun), inner, u, along_u)
    moves.pass_a()
    begun = table_stage(2, table_sum(begun), inner, v, along_v)
    moves.pass_z()
    begun = table_stage(3, table_sum(begun), DEEP, place.z, lambda d: place.device(dz=d))
    moves.hand_over()
    moves.finish()
    sum_ref[...] = table_sum(begun)


def delivered(grads, table, cuts):
    owners = lax.axis_size("fsdp")
    inner, kinds = inner_of(owners), len(grads)
    anywhere = pl.BlockSpec(memory_space=pl.ANY)
    dma = pltpu.SemaphoreType.DMA
    return pl.pallas_call(
        functools.partial(deliver_kernel, inner, cuts, kinds),
        in_specs=[anywhere] * kinds + [pl.BlockSpec(memory_space=pltpu.VMEM)],
        out_specs=[anywhere] * kinds + [pl.BlockSpec(memory_space=pltpu.VMEM)],
        out_shape=[jax.ShapeDtypeStruct(g.shape[1:], F32) for g in grads]
        + [jax.ShapeDtypeStruct(table.shape, F32)],
        scratch_shapes=[
            *delivery_scratch(owners, grads, cuts), pltpu.VMEM((4, DEEP, *table.shape), F32), dma((4, 2, DEEP)),
        ],
        compiler_params=pltpu.CompilerParams(collective_id=1, has_side_effects=True, vmem_limit_bytes=60 << 20),
        name="deliver",
    )(*grads, table)


def window_of_tokens():
    row, col = np.arange(TOK) // (2 * WIN), np.arange(TOK) % (2 * WIN)
    row, col = (row - SHIFT) % WIN, (col - SHIFT) % (2 * WIN)
    return col // WIN, row * WIN + col % WIN


def spread_matrix():
    _, place = window_of_tokens()
    return (place[:, None] == np.arange(WIN * WIN)[None, :]).astype(np.float32)


def relative_parts(rel_index, table):
    count = WIN * WIN
    onehot = (rel_index.reshape(count * count, 1) == jnp.arange(table.shape[0], dtype=jnp.int32)[None, :]).astype(F32)
    relative = jnp.dot(onehot, table, precision=HIGHEST).reshape(count, count, -1).transpose(2, 0, 1)
    return onehot, relative


def bias_of_pairs(relative, regions):
    side, place = window_of_tokens()
    spread = jnp.asarray(spread_matrix())
    wide = jnp.einsum("at,hts,bs->hba", spread, relative, spread, precision=HIGHEST)
    region = regions.reshape(2, WIN * WIN)
    region = jnp.concatenate(
        [jnp.roll(region[s].reshape(WIN, WIN), SHIFT, axis=0)[:, c] for s, c in ((1, slice(4, 7)), (0, slice(0, 7)), (1, slice(0, 4)))],
        axis=1,
    ).reshape(TOK)
    mask = jnp.where(region[:, None] == region[None, :], 0.0, -100.0)
    same = jnp.asarray(side[:, None] == side[None, :])
    bias = jnp.where(same[None], wide + mask[None], FAR)
    return jnp.pad(
        jnp.pad(bias, ((0, 0), (0, PAD - TOK), (0, 0)), constant_values=FAR),
        ((0, 0), (0, 0), (0, LANES - TOK)),
    )


def packed_row(parts):
    width = sum(p.shape[-1] for p in parts)
    width += -width % (2 * LANES)
    at, row = 0, None
    for p in parts:
        edges = [(0, 0)] * (p.ndim - 1) + [(at, width - at - p.shape[-1])]
        row = jnp.pad(p, edges) if row is None else row + jnp.pad(p, edges)
        at += p.shape[-1]
    return row


def qkv_cuts():
    return ((0, 0, 1),) + tuple((1, part, 3) for part in range(3))


def per_device(
    images, norm1_gain, norm1_bias, qkv_weight, q_bias, v_bias, proj_weight, proj_bias, norm2_gain, norm2_bias,
    fc1_weight, fc1_bias, fc2_weight, fc2_bias, bias_table, regions, rel_index, cotangent,
):
    imgs, rows, cols, d = images.shape
    owners = lax.axis_size("fsdp")
    x = images.transpose(1, 2, 0, 3).reshape(rows * cols, imgs, d)
    ct = cotangent.transpose(1, 2, 0, 3).reshape(rows * cols, imgs, d)
    vectors = (norm1_gain, norm1_bias, q_bias, v_bias, proj_bias, norm2_gain, norm2_bias, fc2_bias, fc1_bias)
    packed, w_qkv, halo = gathered((packed_row(vectors)[None], qkv_weight), (x,), qkv_cuts())
    packed = packed[:, 0].astype(F32)
    part = d // owners
    vecs = packed[:, : 8 * part].reshape(owners, 8, part).transpose(1, 0, 2).reshape(8, d)
    b_in = packed[:, 8 * part : 8 * part + fc1_bias.shape[0]].reshape(1, -1)
    whole = lambda v: v.reshape(owners * v.shape[1], v.shape[2])
    w_qkv = whole(w_qkv)
    onehot, relative = relative_parts(rel_index, bias_table)
    rel = bias_of_pairs(relative, regions)

    qkv, att, prob, *mats, ct_halo = attend(
        x, halo, vecs, w_qkv, rel, (proj_weight, fc1_weight, fc2_weight), (ct,)
    )
    w_proj, w_in, w_out = (whole(v) for v in mats)
    flat = lambda v: v.reshape(v.shape[0] * imgs, d)
    tall = lambda v: v.reshape(v.shape[0] // imgs, imgs, d)
    out_top, out_rest, gm, gatt, dwp, dw1, dw2, db_in, small2 = mlp(
        flat(x), flat(halo), flat(att), flat(ct), flat(ct_halo), w_proj, vecs, w_in, b_in, w_out
    )
    swapped = lambda v: lax.ppermute(v, "win", [(0, 1), (1, 0)])
    out_top = swapped(out_top)
    blocks = lambda v: v.reshape(owners, v.shape[0] // owners, v.shape[1])
    gin_top, gin_rest, dwq, small1, bsum, rel_sum, dwp, dw1, dw2 = back(
        x, halo, tall(gm), tall(gatt), qkv, prob, vecs, w_qkv, (blocks(dwp), blocks(dw1), blocks(dw2))
    )
    gin_top = swapped(gin_top)
    spread = jnp.asarray(spread_matrix())
    pairs = jnp.einsum("at,hba,bs->tsh", spread, rel_sum[:, :TOK, :TOK], spread, precision=HIGHEST)
    table = jnp.dot(onehot.T, pairs.reshape(WIN**4, -1), precision=HIGHEST)
    flat_table = jnp.pad(table.reshape(-1), (0, -table.size % (8 * LANES))).reshape(-1, LANES)
    grads = (
        small1[0], small1[1], bsum[0, :d], bsum[0, 2 * d :], small2[2], small2[0], small2[1], small2[3], db_in[0],
    )
    row = packed_row([v.reshape(owners, 1, -1) for v in grads]).astype(BF)
    sums, dwq, table_sum = delivered((row, blocks(dwq)), flat_table, qkv_cuts())
    at, own = 0, []
    for v in vectors:
        own.append(sums[0, at : at + v.shape[0]])
        at += v.shape[0]
    dg1, db1, dqb, dvb, dbp, dg2, db2, db_out, db_in = own
    table = table_sum.reshape(-1)[: table.size].reshape(table.shape)
    joined = lambda top, rest: jnp.concatenate([top, rest], axis=0).reshape(rows, cols, imgs, d).transpose(2, 0, 1, 3)
    return (
        joined(tall(out_top), tall(out_rest)), joined(gin_top, gin_rest), dg1, db1, dwq, dqb, dvb, dwp, dbp, dg2, db2, dw1, db_in, dw2,
        db_out, table,
    )


def solution(mesh):
    vec, mat, img = P("fsdp"), P("fsdp", None), P("fsdp", "win", None, None)
    in_specs = (
        img, vec, vec, mat, vec, vec, mat, vec, vec, vec, mat, vec, mat, vec, P(), P("win", None, None), P(), img,
    )
    out_specs = (img, img, vec, vec, mat, vec, vec, mat, vec, vec, vec, mat, vec, mat, vec, P())
    return jax.shard_map(per_device, mesh=mesh, in_specs=in_specs, out_specs=out_specs, check_vma=False)
```

```python
import functools
import jax
import jax.numpy as jnp
import numpy as np
from jax import lax
from jax.experimental import pallas as pl
from jax.experimental.pallas import tpu as pltpu
from jax.sharding import PartitionSpec as P

HEADS = 16
HD = 32
WIN = 7
SHIFT = 3
TOK = 98
TOP = 42
PAD = 112
LANES = 128
GROUPS = 4
NB = 8
EPS = 1e-05
FAR = -1e30
F32 = jnp.float32
BF = jnp.bfloat16
HIGHEST = lax.Precision.HIGHEST


def mm(a, b):
    return lax.dot_general(a, b, (((1,), (0,)), ((), ())), preferred_element_type=F32)


def mm_nt(a, b):
    return lax.dot_general(a, b, (((1,), (1,)), ((), ())), preferred_element_type=F32)


def mm_tn(a, b):
    return lax.dot_general(a, b, (((0,), (0,)), ((), ())), preferred_element_type=F32)


def normalized(x):
    mean = jnp.mean(x, axis=-1, keepdims=True)
    c = x - mean
    var = jnp.mean(c * c, axis=-1, keepdims=True)
    r = lax.rsqrt(var + EPS)
    return c * r, r


def norm_back(u, n, r):
    return r * (u - jnp.mean(u, axis=-1, keepdims=True) - n * jnp.mean(u * n, axis=-1, keepdims=True))


def col_sum(v):
    return jnp.sum(v, axis=0, keepdims=True)


def half_erf(h):
    h = jnp.clip(h, -5.2947041, 5.2947041)
    s = h * h
    a = (0.00022905065861350646, 0.0034082910107109506, 0.050955695062380861, 0.18520832239976145, 1.128379143519084)
    b = (-1.1791602954361697e-7, 0.000023547966471313185, 0.0010179625278914885, 0.014070470171167667, 0.11098505178285362, 0.49746925110067538, 1.0)
    a = [c * 0.5 ** (4 - i) * 0.5 * 0.7071067811865476 for i, c in enumerate(a)]
    b = [c * 0.5 ** (6 - i) for i, c in enumerate(b)]
    p = a[0]
    for c in a[1:]:
        p = p * s + c
    q = b[0]
    for c in b[1:]:
        q = q * s + c
    return h * p / q


def head_masks():
    lane = lax.broadcasted_iota(jnp.int32, (1, LANES), 1) // HD
    return [(lane == h).astype(BF) for h in range(GROUPS)]


def shifted_rows(x_ref, halo_ref):
    x = jnp.concatenate([halo_ref[...], x_ref[TOP:]], axis=0)
    return x.astype(F32).reshape(x.shape[0] * NB, x.shape[-1])


def own_lanes(stack):
    lane = lax.broadcasted_iota(jnp.int32, (1, LANES), 1) // HD
    out = stack[:PAD]
    for h in range(1, GROUPS):
        out = jnp.where(lane == h, stack[h * PAD : (h + 1) * PAD], out)
    return out


def at_step(step, action):
    @pl.when(pl.program_id(0) == step)
    def _():
        action()


def at_images(events, i):
    images = pl.program_id(0) * NB + i
    for share, action in events:
        @pl.when(images == share)
        def _(action=action):
            action()


def whole_cuts(count):
    return tuple((i, 0, 1) for i in range(count))


def attend_kernel(inner, kinds, fields, x_ref, halo_ref, vec_ref, w_ref, rel_ref, *refs):
    ins, maps = refs[:kinds], refs[kinds : kinds + fields]
    qkv_ref, att_ref, prob_ref = refs[kinds + fields : kinds + fields + 3]
    outs, halos = refs[kinds + fields + 3 : 2 * kinds + fields + 3], refs[2 * kinds + fields + 3 : 2 * (kinds + fields) + 3]
    wide, joined, *sems = refs[2 * (kinds + fields) + 3 :]
    moves = ColumnSpread(inner, ins, maps, outs, halos, *sems)

    def begin():
        meet(Place(inner))
        moves.start()

    at_step(0, begin)
    early, late = tuple(range(kinds - 1)), (kinds - 1,)
    events = [
        (share, functools.partial(moves.run, stage, which))
        for share, stage, which in ((6, 0, early), (11, 0, late), (13, 1, early), (19, 1, late), (22, 2, early), (28, 2, late))
    ]
    d = x_ref.shape[-1]
    n, _ = normalized(shifted_rows(x_ref, halo_ref))
    normed = (n * vec_ref[0:1] + vec_ref[1:2]).astype(BF)
    lanes3 = 3 * d // LANES
    chunk = d
    biases = (vec_ref[2:3], None, vec_ref[3:4])

    @pl.when(pl.program_id(0) == 0)
    def _():
        wide[:, TOK * NB :, :] = jnp.zeros((lanes3, (PAD - TOK) * NB, LANES), F32)

    for c in range(3 * d // chunk):
        part = mm(normed, w_ref[:, c * chunk : (c + 1) * chunk])
        if biases[c] is not None:
            part = part + biases[c]
        for k in range(chunk // LANES):
            wide[c * (chunk // LANES) + k, : TOK * NB, :] = part[:, k * LANES : (k + 1) * LANES]
    masks = head_masks()
    per = d // LANES
    scale = HD ** (-0.5)

    def one(i, carry):
        at_images(events, i)
        for g in range(per):
            q = wide[g, pl.ds(i, PAD, stride=NB), :].astype(BF)
            k = wide[per + g, pl.ds(i, PAD, stride=NB), :].astype(BF)
            v = wide[2 * per + g, pl.ds(i, PAD, stride=NB), :].astype(BF)
            qkv_ref[i, g] = q
            qkv_ref[i, per + g] = k
            qkv_ref[i, 2 * per + g] = v
            scores = mm_nt(jnp.concatenate([k * m for m in masks], axis=0), q)
            v_t = v.T
            heads = []
            for h in range(GROUPS):
                s = scores[h * PAD : (h + 1) * PAD] * scale + rel_ref[g * GROUPS + h][:, :PAD]
                e = jnp.exp(s - jnp.max(s, axis=0, keepdims=True))
                p = (e * (1.0 / jnp.sum(e, axis=0, keepdims=True))).astype(BF)
                prob_ref[i, g * GROUPS + h] = p
                heads.append(mm(v_t[h * HD : (h + 1) * HD], p))
            joined[g, pl.ds(i, PAD, stride=NB), :] = jnp.concatenate(heads, axis=0).T
        return carry

    lax.fori_loop(0, NB, one, 0)
    for g in range(per):
        att_ref[:, :, g * LANES : (g + 1) * LANES] = joined[g, : TOK * NB, :].astype(BF).reshape(TOK, NB, LANES)
    at_step(3, moves.finish)


def attend(x, halo, vecs, w, rel, shards, maps):
    _, imgs, d = x.shape
    owners = lax.axis_size("fsdp")
    inner, kinds, fields = inner_of(owners), len(shards), len(maps)
    anywhere = [pl.BlockSpec(memory_space=pl.ANY)] * (kinds + fields)
    full = lambda *shape: pl.BlockSpec(shape, lambda i: (0,) * len(shape), pipeline_mode=pl.Buffered(1))
    per = d // LANES
    return pl.pallas_call(
        functools.partial(attend_kernel, inner, kinds, fields),
        grid=(imgs // NB,),
        in_specs=[
            pl.BlockSpec((TOK, NB, d), lambda i: (0, i, 0)),
            pl.BlockSpec((TOP, NB, d), lambda i: (0, i, 0)),
            full(8, d), full(d, 3 * d), full(HEADS, PAD, LANES), *anywhere,
        ],
        out_specs=[
            pl.BlockSpec((NB, 3 * per, PAD, LANES), lambda i: (i, 0, 0, 0)),
            pl.BlockSpec((TOK, NB, d), lambda i: (0, i, 0)),
            pl.BlockSpec((NB, HEADS, PAD, PAD), lambda i: (i, 0, 0, 0)),
            *anywhere,
        ],
        out_shape=[
            jax.ShapeDtypeStruct((imgs, 3 * per, PAD, LANES), BF),
            jax.ShapeDtypeStruct((TOK, imgs, d), BF),
            jax.ShapeDtypeStruct((imgs, HEADS, PAD, PAD), BF),
            *column_shapes(owners, shards, maps),
        ],
        scratch_shapes=[
            pltpu.VMEM((3 * per, PAD * NB, LANES), F32),
            pltpu.VMEM((per, PAD * NB, LANES), F32),
            *column_scratch(owners, kinds, fields),
        ],
        compiler_params=pltpu.CompilerParams(collective_id=2, has_side_effects=True, vmem_limit_bytes=60 << 20),
        name="attend",
    )(x, halo, vecs, w, rel, *shards, *maps)


def mlp_kernel(tops, x_ref, halo_ref, att_ref, ct_ref, ct_halo_ref, wp_ref, vec_ref, w1_ref, b1_ref, w2_ref,
               top_ref, rest_ref, gm_ref, gatt_ref, dwp_ref, dw1_ref, dw2_ref, db1_ref, small_ref,
               awp, aw1, aw2, ab1, asm):
    step = pl.program_id(0)
    d = x_ref.shape[-1]
    ff = w1_ref.shape[-1]
    chunk = 512

    @pl.when(step == 0)
    def _():
        awp[...] = jnp.zeros_like(awp)
        aw1[...] = jnp.zeros_like(aw1)
        aw2[...] = jnp.zeros_like(aw2)
        ab1[...] = jnp.zeros_like(ab1)
        asm[...] = jnp.zeros_like(asm)

    att = att_ref[...]
    above = step < tops
    gb = jnp.where(above, ct_halo_ref[...], ct_ref[...])
    grad_out = gb.astype(F32)
    middle = jnp.where(above, halo_ref[...], x_ref[...]).astype(F32) + mm(att, wp_ref[...]) + vec_ref[4:5]
    n, r = normalized(middle)
    normed = (n * vec_ref[5:6] + vec_ref[6:7]).astype(BF)
    normed_t = normed.T
    gb_t = gb.T
    out = middle + vec_ref[7:8]
    m = None
    for c in range(ff // chunk):
        at = slice(c * chunk, (c + 1) * chunk)
        hidden = mm(normed, w1_ref[:, at]) + b1_ref[:, at]
        cdf = 0.5 + half_erf(hidden)
        slope = cdf + hidden * (0.3989422804014327 * jnp.exp(-0.5 * hidden * hidden))
        active = (hidden * cdf).astype(BF)
        out = out + mm(active, w2_ref[at, :])
        gh = mm_nt(gb, w2_ref[at, :]) * slope
        ghb = gh.astype(BF)
        ab1[:, at] += col_sum(gh)
        aw2[:, at] += mm(gb_t, active)
        aw1[:, at] += mm(normed_t, ghb)
        part = mm_nt(ghb, w1_ref[:, at])
        m = part if m is None else m + part

    @pl.when(above)
    def _():
        top_ref[...] = out.astype(BF)

    @pl.when(jnp.logical_not(above))
    def _():
        rest_ref[...] = out.astype(BF)

    grad_middle = grad_out + norm_back(m * vec_ref[5:6], n, r)
    gm_ref[...] = grad_middle
    gp = grad_middle.astype(BF)
    gatt_ref[...] = mm_nt(gp, wp_ref[...]).astype(BF)
    awp[...] += mm_tn(att, gp)
    asm[0:1, :] += col_sum(m * n)
    asm[1:2, :] += col_sum(m)
    asm[2:3, :] += col_sum(gp.astype(F32))
    asm[3:4, :] += col_sum(grad_out)

    @pl.when(step == pl.num_programs(0) - 1)
    def _():
        dwp_ref[...] = awp[...].astype(BF)
        dw1_ref[...] = aw1[...].astype(BF)
        for c in range(ff // chunk):
            at = slice(c * chunk, (c + 1) * chunk)
            dw2_ref[at, :] = aw2[:, at].T.astype(BF)
        db1_ref[...] = ab1[...]
        small_ref[...] = asm[...]


def mlp(x, halo, att, ct, ct_halo, wp, vecs, w1, b1, w2):
    rows, d = x.shape
    tile = halo.shape[0] // 3
    tops = 3
    ff = w1.shape[-1]
    full = lambda *shape: pl.BlockSpec(shape, lambda i: (0,) * len(shape), pipeline_mode=pl.Buffered(1))
    row = pl.BlockSpec((tile, d), lambda i: (i, 0))
    own = pl.BlockSpec((tile, d), lambda i: (jnp.maximum(i, tops), 0))
    top = pl.BlockSpec((tile, d), lambda i: (jnp.minimum(i, tops - 1), 0))
    rest = pl.BlockSpec((tile, d), lambda i: (jnp.maximum(i - tops, 0), 0))
    return pl.pallas_call(
        functools.partial(mlp_kernel, tops),
        grid=(rows // tile,),
        in_specs=[own, top, row, own, top, full(d, d), full(8, d), full(d, ff), full(1, ff), full(ff, d)],
        out_specs=[top, rest, row, row, full(d, d), full(d, ff), full(ff, d), full(1, ff), full(8, d)],
        out_shape=[
            jax.ShapeDtypeStruct((tops * tile, d), BF),
            jax.ShapeDtypeStruct((rows - tops * tile, d), BF),
            jax.ShapeDtypeStruct((rows, d), F32),
            jax.ShapeDtypeStruct((rows, d), BF),
            jax.ShapeDtypeStruct((d, d), BF),
            jax.ShapeDtypeStruct((d, ff), BF),
            jax.ShapeDtypeStruct((ff, d), BF),
            jax.ShapeDtypeStruct((1, ff), F32),
            jax.ShapeDtypeStruct((8, d), F32),
        ],
        scratch_shapes=[
            pltpu.VMEM((d, d), F32), pltpu.VMEM((d, ff), F32), pltpu.VMEM((d, ff), F32),
            pltpu.VMEM((1, ff), F32), pltpu.VMEM((8, d), F32),
        ],
        compiler_params=pltpu.CompilerParams(vmem_limit_bytes=60 << 20),
        name="mlp",
    )(x, halo, att, ct, ct_halo, wp, vecs, w1, b1, w2)


def back_kernel(inner, kinds, x_ref, halo_ref, gm_ref, gatt_ref, qkv_ref, prob_ref, vec_ref, w_ref, *refs):
    ins, (top_ref, rest_ref, dw_ref, small_ref, bsum_ref, rel_ref) = refs[:kinds], refs[kinds : kinds + 6]
    outs, (wide, grads, aw, asm, abs_), room = refs[kinds + 6 : 2 * kinds + 6], refs[2 * kinds + 6 : 2 * kinds + 11], refs[2 * kinds + 11 :]
    moves = Delivery(inner, whole_cuts(kinds), ins, outs, room)

    def begin():
        meet(Place(inner))
        moves.start()

    at_step(0, begin)
    events = [(6, moves.pass_b), (15, moves.pass_a), (20, moves.pass_z), (29, moves.hand_over)]
    step = pl.program_id(0)
    d = x_ref.shape[-1]
    per = d // LANES
    scale = HD ** (-0.5)

    @pl.when(step == 0)
    def _():
        aw[...] = jnp.zeros_like(aw)
        asm[...] = jnp.zeros_like(asm)
        abs_[...] = jnp.zeros_like(abs_)
        rel_ref[...] = jnp.zeros_like(rel_ref)
        wide[:, TOK * NB :, :] = jnp.zeros((per, (PAD - TOK) * NB, LANES), F32)

    for g in range(per):
        wide[g, : TOK * NB, :] = gatt_ref[:, :, g * LANES : (g + 1) * LANES].astype(F32).reshape(TOK * NB, LANES)
    masks = head_masks()

    def one(i, carry):
        at_images(events, i)
        for g in range(per):
            ga = wide[g, pl.ds(i, PAD, stride=NB), :].astype(BF)
            q = qkv_ref[i, g]
            k = qkv_ref[i, per + g]
            v = qkv_ref[i, 2 * per + g]
            dps = mm_nt(jnp.concatenate([v * m for m in masks], axis=0), ga)
            k_t = k.T
            probs, marks, dq = [], [], []
            for h in range(GROUPS):
                p = prob_ref[i, g * GROUPS + h]
                pf = p.astype(F32)
                dp = dps[h * PAD : (h + 1) * PAD]
                ds = (pf * (dp - jnp.sum(pf * dp, axis=0, keepdims=True))).astype(BF)
                rel_ref[g * GROUPS + h] += ds.astype(F32)
                dq.append(mm(k_t[h * HD : (h + 1) * HD], ds))
                probs.append(p)
                marks.append(ds)
            dv = own_lanes(mm(jnp.concatenate(probs, axis=0), ga))
            dk = own_lanes(mm(jnp.concatenate(marks, axis=0), q))
            grads[g, pl.ds(i, PAD, stride=NB), :] = jnp.concatenate(dq, axis=0).T * scale
            grads[per + g, pl.ds(i, PAD, stride=NB), :] = dk * scale
            grads[2 * per + g, pl.ds(i, PAD, stride=NB), :] = dv
        return carry

    lax.fori_loop(0, NB, one, 0)
    n, r = normalized(shifted_rows(x_ref, halo_ref))
    normed = (n * vec_ref[0:1] + vec_ref[1:2]).astype(BF)
    normed_t = normed.T
    dn = None
    for c in range(3):
        at = slice(c * d, (c + 1) * d)
        dqkv = jnp.concatenate([grads[c * per + g, : TOK * NB, :].astype(BF) for g in range(per)], axis=-1)
        abs_[:, at] += col_sum(dqkv.astype(F32))
        aw[:, at] += mm(normed_t, dqkv)
        part = mm_nt(dqkv, w_ref[:, at])
        dn = part if dn is None else dn + part
    dn = dn.astype(BF).astype(F32)
    asm[0:1, :] += col_sum(dn * n)
    asm[1:2, :] += col_sum(dn)
    gin = gm_ref[...].reshape(TOK * NB, d) + norm_back(dn * vec_ref[0:1], n, r)
    gin = gin.reshape(TOK, NB, d)
    top_ref[...] = gin[:TOP]
    rest_ref[...] = gin[TOP:]

    at_step(3, moves.finish)

    @pl.when(step == pl.num_programs(0) - 1)
    def _():
        dw_ref[...] = aw[...].astype(BF)
        small_ref[...] = asm[...]
        bsum_ref[...] = abs_[...]


def back(x, halo, gm, gatt, qkv, prob, vecs, w, grads):
    _, imgs, d = x.shape
    owners, kinds = lax.axis_size("fsdp"), len(grads)
    anywhere = [pl.BlockSpec(memory_space=pl.ANY)] * kinds
    per = d // LANES
    full = lambda *shape: pl.BlockSpec(shape, lambda i: (0,) * len(shape), pipeline_mode=pl.Buffered(1))
    tok = pl.BlockSpec((TOK, NB, d), lambda i: (0, i, 0))
    return pl.pallas_call(
        functools.partial(back_kernel, inner_of(owners), kinds),
        grid=(imgs // NB,),
        in_specs=[
            tok, pl.BlockSpec((TOP, NB, d), lambda i: (0, i, 0)), tok, tok,
            pl.BlockSpec((NB, 3 * per, PAD, LANES), lambda i: (i, 0, 0, 0)),
            pl.BlockSpec((NB, HEADS, PAD, PAD), lambda i: (i, 0, 0, 0)),
            full(8, d), full(d, 3 * d), *anywhere,
        ],
        out_specs=[pl.BlockSpec((TOP, NB, d), lambda i: (0, i, 0)), pl.BlockSpec((TOK - TOP, NB, d), lambda i: (0, i, 0)), full(d, 3 * d), full(8, d), full(1, 3 * d), full(HEADS, PAD, PAD), *anywhere],
        out_shape=[
            jax.ShapeDtypeStruct((TOP, imgs, d), F32),
            jax.ShapeDtypeStruct((TOK - TOP, imgs, d), F32),
            jax.ShapeDtypeStruct((d, 3 * d), BF),
            jax.ShapeDtypeStruct((8, d), F32),
            jax.ShapeDtypeStruct((1, 3 * d), F32),
            jax.ShapeDtypeStruct((HEADS, PAD, PAD), F32),
            *[jax.ShapeDtypeStruct(g.shape[2:], F32) for g in grads],
        ],
        scratch_shapes=[
            pltpu.VMEM((per, PAD * NB, LANES), F32),
            pltpu.VMEM((3 * per, PAD * NB, LANES), F32),
            pltpu.VMEM((d, 3 * d), F32),
            pltpu.VMEM((8, d), F32),
            pltpu.VMEM((1, 3 * d), F32),
            *delivery_scratch(owners, grads, whole_cuts(kinds)),
        ],
        compiler_params=pltpu.CompilerParams(collective_id=3, has_side_effects=True, vmem_limit_bytes=62 << 20),
        name="back",
    )(x, halo, gm, gatt, qkv, prob, vecs, w, *grads)


DEEP = 4


class Place:
    def __init__(self, inner):
        self.inner = inner
        me, core = lax.axis_index("fsdp"), lax.axis_index("win")
        self.core, self.mate = core, 1 - core
        self.z = me // (inner * inner)
        u, v = (me // inner) % inner, me % inner
        self.a = u * (1 - core) + v * core
        self.b = v * (1 - core) + u * core
        self.step_a = inner * (1 - core) + core
        self.step_b = inner * core + 1 - core

    def at(self, dz=0, da=0, db=0):
        z = (self.z + dz) % DEEP
        a = (self.a + da) % self.inner
        b = (self.b + db) % self.inner
        return z * self.inner * self.inner + a * self.step_a + b * self.step_b

    def column(self, da=0, db=0):
        return ((self.a + da) % self.inner) * self.step_a + ((self.b + db) % self.inner) * self.step_b

    def depth(self, dz=0):
        return (self.z + dz) % DEEP

    def device(self, dz=0, da=0, db=0):
        return (self.at(dz, da, db), self.core)

    def partner(self):
        return (self.at(), self.mate)

    def peers(self):
        near = [self.device(dz=d) for d in range(1, DEEP)]
        near += [self.device(da=d) for d in range(1, self.inner)]
        near += [self.device(db=d) for d in range(1, self.inner)]
        return near + [self.partner()]


def meet(place):
    barrier = pltpu.get_barrier_semaphore()
    peers = place.peers()
    for peer in peers:
        pl.semaphore_signal(barrier, inc=1, device_id=peer, device_id_type=pl.DeviceIdType.MESH)
    pl.semaphore_wait(barrier, len(peers))


def remote(src, dst, send_sem, recv_sem, device):
    return pltpu.make_async_remote_copy(
        src_ref=src, dst_ref=dst, send_sem=send_sem, recv_sem=recv_sem, device_id=device,
        device_id_type=pl.DeviceIdType.MESH,
    )


def cut_columns(array, cut, core):
    half = array.shape[-1] // 2
    width = half // cut[2]
    return pl.ds(pl.multiple_of(core * half + cut[1] * width, LANES), width)


class Spread:
    def __init__(self, inner, cuts, ins, maps, outs, halos, send_sem, recv_sem, own_sem, halo_sem):
        self.cuts = cuts
        self.inner, self.ins, self.maps, self.outs, self.halos = inner, ins, maps, outs, halos
        self.send_sem, self.recv_sem, self.own_sem, self.halo_sem = send_sem, recv_sem, own_sem, halo_sem
        steps = [("a", d) for d in range(1, inner)], [("b", d) for d in range(1, inner)]
        order_z, mate = (1, 3, 2), [("m", 0)]
        plan = [[((0, 0, 0), [("z", d) for d in order_z] + steps[0] + steps[1])]]
        plan.append([((dz, 0, 0), steps[0] + steps[1] + mate) for dz in order_z])
        plan.append([((dz, da, 0), steps[1] + mate) for da in range(1, inner) for dz in (0,) + order_z])
        plan.append([((dz, da, db), mate) for db in range(1, inner) for da in range(inner) for dz in (0,) + order_z])
        self.plan, count = [], 0
        for stage in plan:
            rows = []
            for block, targets in stage:
                rows.append((block, [(t, count + i) for i, t in enumerate(targets)]))
                count += len(targets)
            self.plan.append(rows)

    def piece(self, k, block, core):
        out = self.outs[self.cuts[k][0]]
        return out.at[block, :, cut_columns(out, self.cuts[k], core)]

    def copy(self, place, k, stage, block, target, index):
        (axis, d), where = target, place.at(*block)
        device = {"z": place.device(dz=d), "a": place.device(da=d), "b": place.device(db=d), "m": place.partner()}[axis]
        src = self.piece(k, where, place.core)
        if stage == 0:
            shard = self.ins[self.cuts[k][0]]
            src = shard.at[:, cut_columns(shard, self.cuts[k], place.core)]
        return remote(src, self.piece(k, where, place.core), self.send_sem.at[k, index],
                      self.recv_sem.at[k, place.core, where], device)

    def arrive(self, place, k, block, core):
        at = self.piece(k, place.at(*block), core)
        remote(at, at, self.send_sem.at[k, 0], self.recv_sem.at[k, core, place.at(*block)], place.partner()).wait_recv()

    def local(self, place):
        copies = [remote(self.maps[f].at[:TOP], self.halos[f], self.halo_sem.at[f, 0], self.halo_sem.at[f, 1],
                         place.partner()) for f in range(len(self.maps))]
        copies += [pltpu.make_async_copy(self.ins[k], self.outs[k].at[place.at()], self.own_sem.at[k])
                   for k in range(len(self.ins))]
        return copies

    def run(self, stage, kinds=None):
        place = Place(self.inner)
        for k in range(len(self.cuts)) if kinds is None else kinds:
            for block, targets in self.plan[stage]:
                if stage:
                    self.arrive(place, k, block, place.core)
                for target, index in targets:
                    self.copy(place, k, stage, block, target, index).start()
        if stage == 0:
            for copy in self.local(place):
                copy.start()

    def finish(self):
        place = Place(self.inner)
        for k in range(len(self.cuts)):
            for stage in self.plan[1:]:
                for block, _ in stage:
                    self.arrive(place, k, block, place.mate)
            for stage, rows in enumerate(self.plan):
                for block, targets in rows:
                    for target, index in targets:
                        self.copy(place, k, stage, block, target, index).wait_send()
        for copy in self.local(place):
            copy.wait()


class ColumnSpread:
    def __init__(self, inner, ins, maps, outs, halos, send_sem, z_sem, column_sem, own_sem, halo_sem):
        self.inner, self.ins, self.maps, self.outs, self.halos = inner, ins, maps, outs, halos
        self.send_sem, self.z_sem, self.column_sem, self.own_sem, self.halo_sem = send_sem, z_sem, column_sem, own_sem, halo_sem
        steps = range(1, inner)
        along_a, along_b, mate = [("a", d) for d in steps], [("b", d) for d in steps], [("m", 0)]
        plan = [[((0, 0), along_a + along_b + mate)]]
        plan.append([((da, 0), along_b + mate) for da in steps])
        plan.append([((da, db), mate) for db in steps for da in range(inner)])
        self.plan, count = [], DEEP - 1
        for stage in plan:
            rows = []
            for block, targets in stage:
                rows.append((block, [(t, count + i) for i, t in enumerate(targets)]))
                count += len(targets)
            self.plan.append(rows)

    def cut(self, k, core):
        return cut_columns(self.outs[k], (k, 0, 1), core)

    def along_z(self, place, k, d):
        mine = self.outs[k].at[place.depth(), place.column(), :, self.cut(k, place.core)]
        return remote(self.ins[k].at[:, self.cut(k, place.core)], mine, self.send_sem.at[k, d - 1],
                      self.z_sem.at[k, d - 1], place.device(dz=d))

    def move(self, place, k, block, target, index):
        (axis, d), column = target, place.column(*block)
        device = {"a": place.device(da=d), "b": place.device(db=d), "m": place.partner()}[axis]
        part = self.outs[k].at[:, column, :, self.cut(k, place.core)]
        return remote(part, part, self.send_sem.at[k, index], self.column_sem.at[k, place.core, column], device)

    def arrive(self, place, k, block, core):
        column = place.column(*block)
        part = self.outs[k].at[:, column, :, self.cut(k, core)]
        remote(part, part, self.send_sem.at[k, 0], self.column_sem.at[k, core, column], place.partner()).wait_recv()

    def local(self, place, k):
        cut = self.cut(k, place.core)
        return pltpu.make_async_copy(self.ins[k].at[:, cut], self.outs[k].at[place.depth(), place.column(), :, cut],
                                     self.own_sem.at[k])

    def swaps(self, place):
        return [remote(self.maps[f].at[:TOP], self.halos[f], self.halo_sem.at[f, 0], self.halo_sem.at[f, 1],
                       place.partner()) for f in range(len(self.maps))]

    def start(self):
        place = Place(self.inner)
        for k in range(len(self.ins)):
            for d in (1, 3, 2):
                self.along_z(place, k, d).start()
            self.local(place, k).start()
        for copy in self.swaps(place):
            copy.start()

    def run(self, stage, kinds):
        place = Place(self.inner)
        for k in kinds:
            if stage == 0:
                self.local(place, k).wait()
                for d in (1, 3, 2):
                    self.along_z(place, k, d).wait_recv()
            for block, targets in self.plan[stage]:
                if stage:
                    self.arrive(place, k, block, place.core)
                for target, index in targets:
                    self.move(place, k, block, target, index).start()

    def finish(self):
        place = Place(self.inner)
        for k in range(len(self.ins)):
            for da in range(self.inner):
                for db in range(self.inner):
                    self.arrive(place, k, (da, db), place.mate)
            for d in range(1, DEEP):
                self.along_z(place, k, d).wait_send()
            for rows in self.plan:
                for block, targets in rows:
                    for target, index in targets:
                        self.move(place, k, block, target, index).wait_send()
        for copy in self.swaps(place):
            copy.wait()


def column_scratch(owners, kinds, fields):
    inner, dma = inner_of(owners), pltpu.SemaphoreType.DMA
    sends = DEEP - 1 + 2 * (inner - 1) + 1 + (inner - 1) * inner + (inner - 1) * inner
    return [dma((kinds, sends)), dma((kinds, DEEP - 1)), dma((kinds, 2, inner * inner)), dma((kinds,)), dma((fields, 2))]


def column_shapes(owners, shards, maps):
    return [jax.ShapeDtypeStruct((DEEP, owners // DEEP, *s.shape), s.dtype) for s in shards] + [
        jax.ShapeDtypeStruct((TOP, *m.shape[1:]), m.dtype) for m in maps
    ]


def spread_scratch(owners, kinds, arrays, fields):
    inner = inner_of(owners)
    sends = 3 + 2 * (inner - 1) + 3 * (2 * inner - 1) + 2 * DEEP * (inner - 1) * inner
    dma = pltpu.SemaphoreType.DMA
    return [dma((kinds, sends)), dma((kinds, 2, owners)), dma((arrays,)), dma((fields, 2))]


def spread_shapes(owners, shards, maps):
    return [jax.ShapeDtypeStruct((owners, *s.shape), s.dtype) for s in shards] + [
        jax.ShapeDtypeStruct((TOP, *m.shape[1:]), m.dtype) for m in maps
    ]


def gather_kernel(inner, cuts, kinds, fields, *refs):
    ins, maps = refs[:kinds], refs[kinds : kinds + fields]
    outs, halos = refs[kinds + fields : 2 * kinds + fields], refs[2 * kinds + fields : 2 * (kinds + fields)]
    meet(Place(inner))
    moves = Spread(inner, cuts, ins, maps, outs, halos, *refs[2 * (kinds + fields) :])
    moves.run(0)
    for k in range(len(cuts)):
        moves.run(1, (k,))
        moves.run(2, (k,))
    moves.run(3)
    moves.finish()


def inner_of(owners):
    return int(round((owners // DEEP) ** 0.5))


def gathered(shards, maps, cuts):
    owners = lax.axis_size("fsdp")
    inner, kinds, fields = inner_of(owners), len(shards), len(maps)
    anywhere = pl.BlockSpec(memory_space=pl.ANY)
    return pl.pallas_call(
        functools.partial(gather_kernel, inner, cuts, kinds, fields),
        in_specs=[anywhere] * (kinds + fields),
        out_specs=[anywhere] * (kinds + fields),
        out_shape=spread_shapes(owners, shards, maps),
        scratch_shapes=spread_scratch(owners, len(cuts), kinds, fields),
        compiler_params=pltpu.CompilerParams(collective_id=0, has_side_effects=True),
        name="gather",
    )(*shards, *maps)


class Delivery:
    def __init__(self, inner, cuts, ins, outs, refs):
        self.inner, self.cuts, self.ins, self.outs, kinds = inner, cuts, ins, outs, len(cuts)
        self.kinds = range(kinds)
        self.own, self.from_mate, self.from_b, self.from_a, self.from_z, self.final = (
            refs[i * kinds : (i + 1) * kinds] for i in range(6)
        )
        self.load_sem, self.mate_sem, self.b_sem, self.a_sem, self.z_sem, self.end_sem = refs[6 * kinds : 6 * kinds + 6]
        self.steps = range(1, inner)

    def columns(self, k, core):
        return cut_columns(self.outs[self.cuts[k][0]], self.cuts[k], core)

    def add(self, k, column, other):
        self.own[k][:, column] = (self.own[k][:, column].astype(F32) + other[...].astype(F32)).astype(BF)

    def loads(self, place, k):
        array = self.ins[self.cuts[k][0]]
        return (
            remote(array.at[:, :, :, self.columns(k, place.mate)], self.from_mate[k], self.mate_sem.at[k, 0],
                   self.mate_sem.at[k, 1], place.partner()),
            pltpu.make_async_copy(array.at[:, :, :, self.columns(k, place.core)], self.own[k], self.load_sem.at[k]),
        )

    def to_b(self, place, k, da, db):
        slot = (db - 1) * self.inner + da
        return remote(self.own[k].at[:, place.column(da, db)], self.from_b[k].at[slot], self.b_sem.at[k, 0, slot],
                      self.b_sem.at[k, 1, slot], place.device(db=db))

    def to_a(self, place, k, da):
        return remote(self.own[k].at[:, place.column(da)], self.from_a[k].at[da - 1], self.a_sem.at[k, 0, da - 1],
                      self.a_sem.at[k, 1, da - 1], place.device(da=da))

    def to_z(self, place, k, dz):
        return remote(self.own[k].at[place.depth(dz), place.column()], self.from_z[k].at[dz - 1],
                      self.z_sem.at[k, 0, dz - 1], self.z_sem.at[k, 1, dz - 1], place.device(dz=dz))

    def ends(self, place, k):
        there = self.outs[self.cuts[k][0]].at[:, self.columns(k, place.core)]
        return (remote(self.final[k], there, self.end_sem.at[k, 0], self.end_sem.at[k, 1], place.partner()),
                pltpu.make_async_copy(self.final[k], there, self.end_sem.at[k, 2]))

    def start(self):
        place = Place(self.inner)
        for k in self.kinds:
            for copy in self.loads(place, k):
                copy.start()

    def pass_b(self):
        place = Place(self.inner)
        for k in self.kinds:
            for copy in self.loads(place, k):
                copy.wait()
            for db in tuple(self.steps) + (0,):
                for da in range(self.inner):
                    column = place.column(da, db)
                    self.add(k, column, self.from_mate[k].at[:, column])
                    if db:
                        self.to_b(place, k, da, db).start()

    def pass_a(self):
        place = Place(self.inner)
        for k in self.kinds:
            for db in self.steps:
                for da in range(self.inner):
                    self.to_b(place, k, da, db).wait()
            for da in tuple(self.steps) + (0,):
                for db in self.steps:
                    self.add(k, place.column(da), self.from_b[k].at[(db - 1) * self.inner + da])
                if da:
                    self.to_a(place, k, da).start()

    def pass_z(self):
        place = Place(self.inner)
        for k in self.kinds:
            for da in self.steps:
                self.to_a(place, k, da).wait()
            for da in self.steps:
                self.add(k, place.column(), self.from_a[k].at[da - 1])
            for dz in (2, 1, 3):
                self.to_z(place, k, dz).start()

    def hand_over(self):
        place = Place(self.inner)
        for k in self.kinds:
            for dz in (2, 1, 3):
                self.to_z(place, k, dz).wait()
            total = self.own[k][place.depth(), place.column()].astype(F32)
            for dz in range(1, DEEP):
                total = total + self.from_z[k][dz - 1].astype(F32)
            self.final[k][...] = total
            for copy in self.ends(place, k):
                copy.start()

    def finish(self):
        place = Place(self.inner)
        for k in self.kinds:
            for copy in self.ends(place, k):
                copy.wait()


def delivery_scratch(owners, grads, cuts):
    inner, kinds = inner_of(owners), len(cuts)
    halves = [(grads[i].shape[2], grads[i].shape[3] // 2 // parts) for i, _, parts in cuts]
    dma = pltpu.SemaphoreType.DMA

    def room(*count):
        return [pltpu.VMEM((*count, *h), BF) for h in halves]

    return [
        *room(DEEP, owners // DEEP), *room(DEEP, owners // DEEP), *room((inner - 1) * inner, DEEP),
        *room(inner - 1, DEEP), *room(DEEP - 1), *[pltpu.VMEM(h, F32) for h in halves],
        dma((kinds,)), dma((kinds, 2)), dma((kinds, 2, (inner - 1) * inner)),
        dma((kinds, 2, inner - 1)), dma((kinds, 2, DEEP - 1)), dma((kinds, 3)),
    ]


def deliver_kernel(inner, cuts, kinds, *refs):
    ins, table_ref, outs, sum_ref = refs[:kinds], refs[kinds], refs[kinds + 1 : 2 * kinds + 1], refs[2 * kinds + 1]
    parts, part_sem = refs[-2:]
    place = Place(inner)
    meet(place)
    moves = Delivery(inner, cuts, ins, outs, refs[2 * kinds + 2 :])

    def table_stage(stage, value, count, mine, peer):
        parts[stage, mine] = value
        copies = [remote(parts.at[stage, mine], parts.at[stage, mine], part_sem.at[stage, 0, d],
                         part_sem.at[stage, 1, d], peer(d)) for d in range(1, count)]
        for copy in copies:
            copy.start()
        return copies, stage, count

    def table_sum(begun):
        copies, stage, count = begun
        for copy in copies:
            copy.wait()
        total = parts[stage, 0]
        for i in range(1, count):
            total = total + parts[stage, i]
        return total

    u = place.a * (1 - place.core) + place.b * place.core
    v = place.b * (1 - place.core) + place.a * place.core
    along_u = lambda d: (place.at(da=d * (1 - place.core), db=d * place.core), place.core)
    along_v = lambda d: (place.at(da=d * place.core, db=d * (1 - place.core)), place.core)
    begun = table_stage(0, table_ref[...], 2, place.core, lambda d: place.partner())
    moves.start()
    moves.pass_b()
    begun = table_stage(1, table_sum(begun), inner, u, along_u)
    moves.pass_a()
    begun = table_stage(2, table_sum(begun), inner, v, along_v)
    moves.pass_z()
    begun = table_stage(3, table_sum(begun), DEEP, place.z, lambda d: place.device(dz=d))
    moves.hand_over()
    moves.finish()
    sum_ref[...] = table_sum(begun)


def delivered(grads, table, cuts):
    owners = lax.axis_size("fsdp")
    inner, kinds = inner_of(owners), len(grads)
    anywhere = pl.BlockSpec(memory_space=pl.ANY)
    dma = pltpu.SemaphoreType.DMA
    return pl.pallas_call(
        functools.partial(deliver_kernel, inner, cuts, kinds),
        in_specs=[anywhere] * kinds + [pl.BlockSpec(memory_space=pltpu.VMEM)],
        out_specs=[anywhere] * kinds + [pl.BlockSpec(memory_space=pltpu.VMEM)],
        out_shape=[jax.ShapeDtypeStruct(g.shape[2:], F32) for g in grads]
        + [jax.ShapeDtypeStruct(table.shape, F32)],
        scratch_shapes=[
            *delivery_scratch(owners, grads, cuts), pltpu.VMEM((4, DEEP, *table.shape), F32), dma((4, 2, DEEP)),
        ],
        compiler_params=pltpu.CompilerParams(collective_id=1, has_side_effects=True, vmem_limit_bytes=60 << 20),
        name="deliver",
    )(*grads, table)


def window_of_tokens():
    row, col = np.arange(TOK) // (2 * WIN), np.arange(TOK) % (2 * WIN)
    row, col = (row - SHIFT) % WIN, (col - SHIFT) % (2 * WIN)
    return col // WIN, row * WIN + col % WIN


def spread_matrix():
    _, place = window_of_tokens()
    return (place[:, None] == np.arange(WIN * WIN)[None, :]).astype(np.float32)


def relative_parts(rel_index, table):
    count = WIN * WIN
    onehot = (rel_index.reshape(count * count, 1) == jnp.arange(table.shape[0], dtype=jnp.int32)[None, :]).astype(F32)
    relative = jnp.dot(onehot, table, precision=HIGHEST).reshape(count, count, -1).transpose(2, 0, 1)
    return onehot, relative


def bias_of_pairs(relative, regions):
    side, place = window_of_tokens()
    spread = jnp.asarray(spread_matrix())
    wide = jnp.einsum("at,hts,bs->hba", spread, relative, spread, precision=HIGHEST)
    region = regions.reshape(2, WIN * WIN)
    region = jnp.concatenate(
        [jnp.roll(region[s].reshape(WIN, WIN), SHIFT, axis=0)[:, c] for s, c in ((1, slice(4, 7)), (0, slice(0, 7)), (1, slice(0, 4)))],
        axis=1,
    ).reshape(TOK)
    mask = jnp.where(region[:, None] == region[None, :], 0.0, -100.0)
    same = jnp.asarray(side[:, None] == side[None, :])
    bias = jnp.where(same[None], wide + mask[None], FAR)
    return jnp.pad(
        jnp.pad(bias, ((0, 0), (0, PAD - TOK), (0, 0)), constant_values=FAR),
        ((0, 0), (0, 0), (0, LANES - TOK)),
    )


def packed_row(parts):
    width = sum(p.shape[-1] for p in parts)
    width += -width % (2 * LANES)
    at, row = 0, None
    for p in parts:
        edges = [(0, 0)] * (p.ndim - 1) + [(at, width - at - p.shape[-1])]
        row = jnp.pad(p, edges) if row is None else row + jnp.pad(p, edges)
        at += p.shape[-1]
    return row


def qkv_cuts():
    return ((0, 0, 1),) + tuple((1, part, 3) for part in range(3))


def per_device(
    images, norm1_gain, norm1_bias, qkv_weight, q_bias, v_bias, proj_weight, proj_bias, norm2_gain, norm2_bias,
    fc1_weight, fc1_bias, fc2_weight, fc2_bias, bias_table, regions, rel_index, cotangent,
):
    imgs, rows, cols, d = images.shape
    owners = lax.axis_size("fsdp")
    x = images.transpose(1, 2, 0, 3).reshape(rows * cols, imgs, d)
    ct = cotangent.transpose(1, 2, 0, 3).reshape(rows * cols, imgs, d)
    vectors = (norm1_gain, norm1_bias, q_bias, v_bias, proj_bias, norm2_gain, norm2_bias, fc2_bias, fc1_bias)
    packed, w_qkv, halo = gathered((packed_row(vectors)[None], qkv_weight), (x,), whole_cuts(2))
    packed = packed[:, 0].astype(F32)
    part = d // owners
    vecs = packed[:, : 8 * part].reshape(owners, 8, part).transpose(1, 0, 2).reshape(8, d)
    b_in = packed[:, 8 * part : 8 * part + fc1_bias.shape[0]].reshape(1, -1)
    whole = lambda v: v.reshape(-1, v.shape[-1])
    w_qkv = whole(w_qkv)
    onehot, relative = relative_parts(rel_index, bias_table)
    rel = bias_of_pairs(relative, regions)

    qkv, att, prob, *mats, ct_halo = attend(
        x, halo, vecs, w_qkv, rel, (proj_weight, fc1_weight, fc2_weight), (ct,)
    )
    w_proj, w_in, w_out = (whole(v) for v in mats)
    flat = lambda v: v.reshape(v.shape[0] * imgs, d)
    tall = lambda v: v.reshape(v.shape[0] // imgs, imgs, d)
    out_top, out_rest, gm, gatt, dwp, dw1, dw2, db_in, small2 = mlp(
        flat(x), flat(halo), flat(att), flat(ct), flat(ct_halo), w_proj, vecs, w_in, b_in, w_out
    )
    swapped = lambda v: lax.ppermute(v, "win", [(0, 1), (1, 0)])
    out_top = swapped(out_top)
    blocks = lambda v: v.reshape(DEEP, owners // DEEP, v.shape[0] // owners, v.shape[1])
    gin_top, gin_rest, dwq, small1, bsum, rel_sum, dwp, dw1, dw2 = back(
        x, halo, tall(gm), tall(gatt), qkv, prob, vecs, w_qkv, (blocks(dwp), blocks(dw1), blocks(dw2))
    )
    gin_top = swapped(gin_top)
    spread = jnp.asarray(spread_matrix())
    pairs = jnp.einsum("at,hba,bs->tsh", spread, rel_sum[:, :TOK, :TOK], spread, precision=HIGHEST)
    table = jnp.dot(onehot.T, pairs.reshape(WIN**4, -1), precision=HIGHEST)
    flat_table = jnp.pad(table.reshape(-1), (0, -table.size % (8 * LANES))).reshape(-1, LANES)
    grads = (
        small1[0], small1[1], bsum[0, :d], bsum[0, 2 * d :], small2[2], small2[0], small2[1], small2[3], db_in[0],
    )
    row = packed_row([v.reshape(owners, 1, -1) for v in grads]).astype(BF)
    sums, dwq, table_sum = delivered((row.reshape(DEEP, owners // DEEP, 1, -1), blocks(dwq)), flat_table, qkv_cuts())
    at, own = 0, []
    for v in vectors:
        own.append(sums[0, at : at + v.shape[0]])
        at += v.shape[0]
    dg1, db1, dqb, dvb, dbp, dg2, db2, db_out, db_in = own
    table = table_sum.reshape(-1)[: table.size].reshape(table.shape)
    joined = lambda top, rest: jnp.concatenate([top, rest], axis=0).reshape(rows, cols, imgs, d).transpose(2, 0, 1, 3)
    return (
        joined(tall(out_top), tall(out_rest)), joined(gin_top, gin_rest), dg1, db1, dwq, dqb, dvb, dwp, dbp, dg2, db2, dw1, db_in, dw2,
        db_out, table,
    )


def solution(mesh):
    vec, mat, img = P("fsdp"), P("fsdp", None), P("fsdp", "win", None, None)
    in_specs = (
        img, vec, vec, mat, vec, vec, mat, vec, vec, vec, mat, vec, mat, vec, P(), P("win", None, None), P(), img,
    )
    out_specs = (img, img, vec, vec, mat, vec, vec, mat, vec, vec, vec, mat, vec, mat, vec, P())
    return jax.shard_map(per_device, mesh=mesh, in_specs=in_specs, out_specs=out_specs, check_vma=False)
```
